128 devices in a mesh: gx: 4 (over y), gy: 8 (over z, x_lo), gz: 4 (over x_hi, core).
Axes of the slice: x: 4 (x_hi: 2, x_lo: 2; x = x_hi * 2 + x_lo), y: 4, z: 4, core: 2. Of those that a mesh axis runs over, the one named last changes fastest.
Arguments:
- node_latent: bfloat16 [64, 256, 16, 128], P('gx', 'gy', 'gz'), may hold values from -6 to 6
- edge_latent: bfloat16 [4, 8, 4, 12288, 128], P('gx', 'gy', 'gz'), may hold values from -6 to 6
- senders: int32 [4, 8, 4, 12288], P('gx', 'gy', 'gz'), may hold values from 7 to 3664, as said below
- receivers: int32 [4, 8, 4, 12288], P('gx', 'gy', 'gz'), may hold values from 0 to 2047, as said below
- w1_edge: bfloat16 [384, 128], replicated, may hold values from -0.3125 to 0.3125
- b1_edge: float32 [128], replicated, may hold values from -3 to 3
- w2_edge: bfloat16 [128, 128], replicated, may hold values from -0.5 to 0.5
- b2_edge: float32 [128], replicated, may hold values from -3 to 3
- w1_node: bfloat16 [256, 128], replicated, may hold values from -0.375 to 0.375
- b1_node: float32 [128], replicated, may hold values from -3 to 3
- w2_node: bfloat16 [128, 128], replicated, may hold values from -0.5 to 0.5
- cot_node: bfloat16 [64, 256, 16, 128], P('gx', 'gy', 'gz'), may hold values from -6 to 6
- cot_edge: bfloat16 [4, 8, 4, 12288, 128], P('gx', 'gy', 'gz'), may hold values from -8 to 8
Outputs:
- grad_node: bfloat16 [64, 256, 16, 128], P('gx', 'gy', 'gz')
- grad_edge: bfloat16 [4, 8, 4, 12288, 128], P('gx', 'gy', 'gz')
- grad_w1_edge: float32 [384, 128], replicated
- grad_w2_edge: float32 [128, 128], replicated
- grad_w1_node: float32 [256, 128], replicated
- grad_w2_node: float32 [128, 128], replicated
- grad_biases: float32 [4, 128], replicated
The draws below stay inside these ranges and needn't reach their ends.
Inputs may be any that keep to these rules, and one draw needn't show every extreme that they name: `receivers`: in every block the list is nondecreasing; entry (i * 32 + j) * 4 + l names the block's cell at local coordinates (i, j, l). `senders`: entry (p * 34 + q) * 6 + r names the cell at local coordinates (p - 1, q - 1, r - 1) of the block extended by one cell on every side, the extension being cells of the adjacent blocks around the periodic box; it is always one of the six face neighbours of the same slot's receiver.
All inputs are finite; a program needn't handle non-finite values.
Results may differ from the reference program's by a relative error of at most 0.01.
Values may be sent and summed in bfloat16 or wider, within the bound.
A program may use at most 128 MiB of HBM per device.

```python
import jax
import jax.numpy as jnp
from jax import lax

H = 128
BX = 16
BY = 32
BZ = 4
CELLS = 2048
EDGES_DEV = 12288
NX = 64
NY = 256
NZ = 16
PARAMS = 115200
N_GX = 4
N_GY = 8
N_GZ = 4


def edge_lists(key):
    base_key = jax.random.fold_in(key, 7)
    receiver_key, direction_key = jax.random.split(base_key)
    grid_shape = (N_GX, N_GY, N_GZ, EDGES_DEV)
    receiver_ids = jnp.sort(jax.random.randint(receiver_key, grid_shape, 0, BX * BY * BZ), axis=-1)
    direction = jax.random.randint(direction_key, grid_shape, 0, 6)
    along_x = receiver_ids // (BY * BZ)
    along_y = receiver_ids // BZ % BY
    along_z = receiver_ids % BZ
    step_x = (direction == 0).astype(jnp.int32) - (direction == 1).astype(jnp.int32)
    step_y = (direction == 2).astype(jnp.int32) - (direction == 3).astype(jnp.int32)
    step_z = (direction == 4).astype(jnp.int32) - (direction == 5).astype(jnp.int32)
    sender_ids = ((along_x + 1 + step_x) * (BY + 2) + along_y + 1 + step_y) * (BZ + 2) + along_z + 1 + step_z
    return (sender_ids.astype(jnp.int32), receiver_ids.astype(jnp.int32))


def draw_senders(key, part):
    return edge_lists(key)[0]


def draw_receivers(key, part):
    return edge_lists(key)[1]


def draw_cot_edge(key, part):
    base_key = jax.random.fold_in(key, 23)
    noise_key, common_key, scale_key = jax.random.split(base_key, 3)
    grid_shape = (N_GX, N_GY, N_GZ, EDGES_DEV, H)
    noise_part = jax.random.normal(noise_key, grid_shape, jnp.float32)
    values = noise_part
    return jnp.clip(values, -8.0, 8.0).astype(jnp.bfloat16)


def steps_of(rng, dims, pieces, smallest, top_value):
    def one(dim, parts):
        heights = jax.random.uniform(jax.random.fold_in(jax.random.fold_in(rng, 6), dim), (parts,), jnp.float32, smallest / len(pieces), top_value / len(pieces))
        return jnp.repeat(jnp.exp(heights), dims[dim] // parts).reshape((-1,) + (1,) * (len(dims) - dim - 1))

    loudness = one(*pieces[0])
    for cut in pieces[1:]:
        loudness = loudness * one(*cut)
    return loudness


def bell_draw(stream_key, dims, spread, reach, cuts=(), kind=jnp.bfloat16):
    array = spread * jax.random.normal(stream_key, dims, jnp.float32)
    if cuts:
        array = array * steps_of(stream_key, dims, cuts, -0.22, 0.18)
    return jnp.clip(array, -reach, reach).astype(kind)


def setup_inputs(seed: int = 0) -> dict:
    seeds = jax.random.split(jax.random.key(seed), 14)
    node_latent = bell_draw(seeds[0], (NX, NY, NZ, H), 1.0, 6.0, ((0, 4), (1, 8), (2, 4)))
    edge_latent = bell_draw(seeds[1], (N_GX, N_GY, N_GZ, EDGES_DEV, H), 1.0, 6.0, ((0, 4), (1, 8), (2, 4)))
    senders = draw_senders(jax.random.fold_in(seeds[13], 71), 0)
    receivers = draw_receivers(jax.random.fold_in(seeds[13], 71), 0)
    w1_edge = bell_draw(seeds[4], (3 * H, H), (3 * H) ** -0.5, 0.3125)
    b1_edge = bell_draw(seeds[5], (H,), 0.5, 3.0, (), jnp.float32)
    w2_edge = bell_draw(seeds[6], (H, H), H ** -0.5, 0.5)
    b2_edge = bell_draw(seeds[7], (H,), 0.5, 3.0, (), jnp.float32)
    w1_node = bell_draw(seeds[8], (2 * H, H), (2 * H) ** -0.5, 0.375)
    b1_node = bell_draw(seeds[9], (H,), 0.5, 3.0, (), jnp.float32)
    w2_node = bell_draw(seeds[10], (H, H), H ** -0.5, 0.5)
    cot_node = bell_draw(seeds[11], (NX, NY, NZ, H), 1.0, 6.0, ((0, 4), (1, 8), (2, 4)))
    cot_edge = draw_cot_edge(jax.random.fold_in(seeds[13], 71), 0)
    return dict(node_latent=node_latent, edge_latent=edge_latent, senders=senders, receivers=receivers, w1_edge=w1_edge, b1_edge=b1_edge, w2_edge=w2_edge, b2_edge=b2_edge, w1_node=w1_node, b1_node=b1_node, w2_node=w2_node, cot_node=cot_node, cot_edge=cot_edge)


def column_sums(values):
    return lax.optimization_barrier(jnp.sum(values.astype(jnp.float32), axis=0))

def silu_slope(values):
    sigma = jax.nn.sigmoid(values)
    return sigma * (1.0 + values * (1.0 - sigma))

def block_terms(padded, edge_rows, cot_rows, cot_cells, sender_ids, receiver_ids, w1_edge, b1_edge, w2_edge, b2_edge, w1_node, b1_node, w2_node):
    latent = edge_rows.shape[1]
    cell_count = cot_cells.shape[0]
    flat_pad = padded.reshape(-1, latent)
    own_rows = padded[1:-1, 1:-1, 1:-1].reshape(cell_count, latent)
    sender_rows = jnp.take(flat_pad, sender_ids, axis=0)
    receiver_rows = jnp.take(own_rows, receiver_ids, axis=0)
    x_edge = jnp.concatenate([edge_rows, sender_rows, receiver_rows], axis=1)
    z_edge = jnp.dot(x_edge, w1_edge, preferred_element_type=jnp.float32) + b1_edge
    u_edge = jax.nn.silu(z_edge).astype(jnp.bfloat16)
    edge_new = (edge_rows.astype(jnp.float32) + jnp.dot(u_edge, w2_edge, preferred_element_type=jnp.float32) + b2_edge).astype(jnp.bfloat16)
    aggregate = jax.ops.segment_sum(edge_new.astype(jnp.float32), receiver_ids, cell_count, indices_are_sorted=True).astype(jnp.bfloat16)
    x_node = jnp.concatenate([own_rows, aggregate], axis=1)
    z_node = jnp.dot(x_node, w1_node, preferred_element_type=jnp.float32) + b1_node
    u_node = jax.nn.silu(z_node).astype(jnp.bfloat16)
    dz_node = (jnp.dot(cot_cells, w2_node.T, preferred_element_type=jnp.float32) * silu_slope(z_node)).astype(jnp.bfloat16)
    dx_node = jnp.dot(dz_node, w1_node.T, preferred_element_type=jnp.float32)
    d_edge = (cot_rows.astype(jnp.float32) + jnp.take(dx_node[:, latent:], receiver_ids, axis=0)).astype(jnp.bfloat16)
    dz_edge = (jnp.dot(d_edge, w2_edge.T, preferred_element_type=jnp.float32) * silu_slope(z_edge)).astype(jnp.bfloat16)
    dx_edge = jnp.dot(dz_edge, w1_edge.T, preferred_element_type=jnp.float32)
    grad_edge = (d_edge.astype(jnp.float32) + dx_edge[:, :latent]).astype(jnp.bfloat16)
    receiver_sum = jax.ops.segment_sum(dx_edge[:, 2 * latent:], receiver_ids, cell_count, indices_are_sorted=True)
    sender_sum = jax.ops.segment_sum(dx_edge[:, latent:2 * latent], sender_ids, flat_pad.shape[0])
    local_rows = dx_node[:, :latent] + receiver_sum
    raws = (jnp.dot(x_edge.T, dz_edge, preferred_element_type=jnp.float32), column_sums(dz_edge), jnp.dot(u_edge.T, d_edge, preferred_element_type=jnp.float32), column_sums(d_edge), jnp.dot(x_node.T, dz_node, preferred_element_type=jnp.float32), column_sums(dz_node), jnp.dot(u_node.T, cot_cells, preferred_element_type=jnp.float32), column_sums(cot_cells))
    return (grad_edge, local_rows, sender_sum, raws)

def reference(node_latent, edge_latent, senders, receivers, w1_edge, b1_edge, w2_edge, b2_edge, w1_node, b1_node, w2_node, cot_node, cot_edge):
    block_total = N_GX * N_GY * N_GZ
    halo_grid = jnp.pad(node_latent, ((1, 1), (1, 1), (1, 1), (0, 0)), mode='wrap')
    edge_blocks = edge_latent.reshape(block_total, EDGES_DEV, H)
    cot_blocks = cot_edge.reshape(block_total, EDGES_DEV, H)
    sender_blocks = senders.reshape(block_total, EDGES_DEV)
    receiver_blocks = receivers.reshape(block_total, EDGES_DEV)
    zero_index = jnp.zeros((), jnp.int32)
    shapes = ((3 * H, H), (H,), (H, H), (H,), (2 * H, H), (H,), (H, H), (H,))
    totals = tuple((jnp.zeros(shape_item, jnp.float32) for shape_item in shapes))
    grad_grid = jnp.zeros((NX + 2, NY + 2, NZ + 2, H), jnp.float32)

    def block_step(running, inputs):
        grid_now, totals_now = running
        block_index, edge_rows, cot_rows, sender_ids, receiver_ids = inputs
        corner_x = (block_index // (N_GY * N_GZ) * BX).astype(jnp.int32)
        corner_y = (block_index // N_GZ % N_GY * BY).astype(jnp.int32)
        corner_z = (block_index % N_GZ * BZ).astype(jnp.int32)
        anchor = (corner_x, corner_y, corner_z, zero_index)
        padded = lax.dynamic_slice(halo_grid, anchor, (BX + 2, BY + 2, BZ + 2, H))
        cot_cells = lax.dynamic_slice(cot_node, anchor, (BX, BY, BZ, H)).reshape(CELLS, H)
        grad_edge, local_rows, sender_sum, raws = block_terms(padded, edge_rows, cot_rows, cot_cells, sender_ids, receiver_ids, w1_edge, b1_edge, w2_edge, b2_edge, w1_node, b1_node, w2_node)
        block_grad = sender_sum.reshape(BX + 2, BY + 2, BZ + 2, H)
        block_grad = block_grad.at[1:-1, 1:-1, 1:-1].add(local_rows.reshape(BX, BY, BZ, H))
        current = lax.dynamic_slice(grid_now, anchor, (BX + 2, BY + 2, BZ + 2, H))
        grid_now = lax.dynamic_update_slice(grid_now, current + block_grad, anchor)
        totals_now = tuple((older + fresh for older, fresh in zip(totals_now, raws)))
        return ((grid_now, totals_now), grad_edge)
    block_ids = jnp.arange(block_total, dtype=jnp.int32)
    (grad_grid, totals), edge_grads = lax.scan(block_step, (grad_grid, totals), (block_ids, edge_blocks, cot_blocks, sender_blocks, receiver_blocks))
    folded = grad_grid.at[1].add(grad_grid[-1]).at[-2].add(grad_grid[0])
    folded = folded.at[:, 1].add(folded[:, -1]).at[:, -2].add(folded[:, 0])
    folded = folded.at[:, :, 1].add(folded[:, :, -1]).at[:, :, -2].add(folded[:, :, 0])
    grad_node = (cot_node.astype(jnp.float32) + folded[1:-1, 1:-1, 1:-1]).astype(jnp.bfloat16)
    grad_edge = edge_grads.reshape(N_GX, N_GY, N_GZ, EDGES_DEV, H)
    squares = sum((jnp.sum(entry * entry) for entry in totals))
    factor = 1.0 / jnp.maximum(1.0, jnp.sqrt(squares / PARAMS))
    grad_w1_edge = totals[0] * factor
    grad_w2_edge = totals[2] * factor
    grad_w1_node = totals[4] * factor
    grad_w2_node = totals[6] * factor
    grad_biases = jnp.stack([totals[1], totals[3], totals[5], totals[7]]) * factor
    return (grad_node, grad_edge, grad_w1_edge, grad_w2_edge, grad_w1_node, grad_w2_node, grad_biases)
```

```python
import functools

import jax
import jax.numpy as jnp
from jax import lax
from jax.experimental import pallas as pl
from jax.experimental.pallas import tpu as pltpu
from jax.sharding import PartitionSpec as P

H = 128
PLANES = 16
ROWS = 128
CELLS = PLANES * ROWS
EDGES = 12288
TILE = 896
PADDED = EDGES + TILE
CHUNK = 512
RAW_ROWS = 904

F32 = jnp.float32
BF16 = jnp.bfloat16


def dot(a, b):
    return jnp.dot(a, b, preferred_element_type=F32)


def dot_tn(a, b):
    return lax.dot_general(a, b, (((0,), (0,)), ((), ())), preferred_element_type=F32)


def pair_dot(rows, diagonal):
    half = rows.shape[0] // 2
    both = dot(jnp.concatenate([rows[:half], rows[half:]], axis=1), diagonal)
    return jnp.concatenate([both[:, :H], both[:, H:]], axis=0)


def block_diagonal(w):
    zero = jnp.zeros_like(w)
    return jnp.concatenate(
        [jnp.concatenate([w, zero], axis=1), jnp.concatenate([zero, w], axis=1)], axis=0
    )


def slope_and_value(z):
    sigma = 0.5 * jnp.tanh(0.5 * z) + 0.5
    value = z * sigma
    return value, sigma * (1.0 + (z - value))


def local_kernel(
    bounds,
    send_ref,
    recv_ref,
    edge_hbm,
    cot_edge_hbm,
    node_ref,
    cot_node_ref,
    face_x_ref,
    face_y_ref,
    face_z_ref,
    w1e_ref,
    b1e_ref,
    w2e_ref,
    b2e_ref,
    w1n_ref,
    b1n_ref,
    w2n_ref,
    grad_edge_hbm,
    base_ref,
    out_x_ref,
    out_y_ref,
    out_z_ref,
    raw_ref,
    edge,
    cot,
    value,
    slope,
    grad,
    code_col,
    code_row,
    proj,
    proj_own,
    gathered,
    degree,
    table,
    sums,
    diag_w1,
    diag_w2t,
    diag_w1t,
    sems,
):
    copies = [
        pltpu.make_async_copy(edge_hbm, edge.at[pl.ds(0, EDGES), :], sems.at[0]),
        pltpu.make_async_copy(cot_edge_hbm, cot.at[pl.ds(0, EDGES), :], sems.at[1]),
    ]
    for item in copies:
        item.start()

    tail = jnp.zeros((TILE, H), BF16)
    edge[EDGES:, :] = tail
    cot[EDGES:, :] = tail

    recv = recv_ref[...]
    step = send_ref[...] - (
        ((recv >> 7) + 1) * 204 + (((recv >> 2) & 31) + 1) * 6 + (recv & 3) + 1
    )
    size = jnp.abs(step)
    axis = jnp.where(size == 204, 0, jnp.where(size == 6, 1, 2))
    key = (recv >> 7) * 256 + jnp.where(step < 0, 128, 0) + (recv & 127)
    code = key * 4 + axis
    code_row[0:96, :] = code
    code_row[96:, :] = jnp.full((code_row.shape[0] - 96, 128), -4, jnp.int32)
    turned = jnp.concatenate([code.astype(F32), jnp.zeros((32, 128), F32)], axis=0).T.astype(
        jnp.int32
    )
    for k in range(96):
        code_col[k * 128 : (k + 1) * 128, :] = jnp.broadcast_to(turned[:, k : k + 1], (128, 128))
    code_col[EDGES:, :] = jnp.full((TILE, 128), -4, jnp.int32)

    w1a = w1e_ref[0:H, :]
    w1b = w1e_ref[H : 2 * H, :]
    w1c = w1e_ref[2 * H :, :]
    diag_w1[...] = block_diagonal(w1a)
    diag_w2t[...] = block_diagonal(w2e_ref[...].T)
    diag_w1t[...] = block_diagonal(w1a.T)
    b1e = b1e_ref[...]

    proj[0:ROWS, :] = dot(face_x_ref[0], w1b)
    proj[ROWS * (PLANES + 1) :, :] = dot(face_x_ref[1], w1b)
    w1bc = jnp.concatenate([w1b, w1c], axis=1)

    def project(k, carry):
        rows = pl.ds(pl.multiple_of(k * CHUNK, CHUNK), CHUNK)
        both = dot(node_ref[rows, :], w1bc)
        proj[pl.ds(pl.multiple_of(k * CHUNK + ROWS, ROWS), CHUNK), :] = both[:, :H]
        proj_own[rows, :] = both[:, H:] + b1e
        return carry

    lax.fori_loop(0, CELLS // CHUNK, project, 0)

    row_id = lax.broadcasted_iota(jnp.int32, (ROWS, H), 0)
    low_z = (row_id & 3) == 0
    high_z = (row_id & 3) == 3
    low_y = row_id < 4
    high_y = row_id >= 124

    def first_row(i):
        return (bounds[i] >> 4) << 4

    def tiles_of(i):
        lo, hi = bounds[i], bounds[i + 1]
        count = (hi - first_row(i) + (TILE - 1)) // TILE
        return jnp.where(hi > lo, count, 0)

    def column_codes(start, i):
        codes = code_col[pl.ds(start, TILE), :]
        return codes & 3, (codes >> 2) - 256 * i

    def one_hot(keys):
        lane = lax.broadcasted_iota(jnp.int32, (TILE, 128), 1)
        low = jnp.where(keys == lane, 1.0, 0.0)
        high = jnp.where(keys == lane + 128, 1.0, 0.0)
        return jnp.concatenate([low, high], axis=1).astype(BF16)

    def one_hot_turned(start, i):
        q = start >> 7
        off = start & 127
        turn = (128 - off) & 127
        here = pltpu.roll(code_row[pl.ds(q, 8), :], turn, 1)
        there = pltpu.roll(code_row[pl.ds(q + 1, 8), :], turn, 1)
        lane = lax.broadcasted_iota(jnp.int32, (8, 128), 1)
        keys = (jnp.where(lane < 128 - off, here, there) >> 2) - 256 * i
        slot = lax.broadcasted_iota(jnp.int32, (256, 128), 0)
        pieces = [
            jnp.where(jnp.broadcast_to(keys[k : k + 1, :], (256, 128)) == slot, 1.0, 0.0)
            for k in range(TILE // 128)
        ]
        return pieces

    def keep_head(ref, start, new, inside):
        old = ref[pl.ds(start, 16), :].astype(F32)
        return jnp.concatenate([jnp.where(inside[:16], new[:16], old), new[16:]], axis=0)

    copies[0].wait()

    def forward_plane(i, carry):
        rows = pl.ds(pl.multiple_of(i * ROWS, ROWS), ROWS)
        own = proj_own[rows, :]
        mine = proj[pl.ds(pl.multiple_of((i + 1) * ROWS, ROWS), ROWS), :]
        above = proj[pl.ds(pl.multiple_of((i + 2) * ROWS, ROWS), ROWS), :]
        below = proj[rows, :]
        side_y = dot(face_y_ref[rows, :], w1e_ref[H : 2 * H, :])
        side_z = dot(face_z_ref[rows, :], w1e_ref[H : 2 * H, :])
        up_y = jnp.where(high_y, side_y, pltpu.roll(mine, 124, 0))
        down_y = jnp.where(low_y, side_y, pltpu.roll(mine, 4, 0))
        up_z = jnp.where(high_z, side_z, pltpu.roll(mine, 127, 0))
        down_z = jnp.where(low_z, side_z, pltpu.roll(mine, 1, 0))
        table[0:ROWS, :] = jnp.concatenate([above + own, up_y + own, up_z + own], axis=1).astype(
            BF16
        )
        table[ROWS:, :] = jnp.concatenate(
            [below + own, down_y + own, down_z + own], axis=1
        ).astype(BF16)
        gathered[rows, :] = jnp.zeros((ROWS, 2 * H), F32)
        degree[rows, :] = jnp.zeros((ROWS, H), F32)

        def tile(t, inner):
            start = pl.multiple_of(first_row(i) + t * TILE, 16)
            span = pl.ds(start, TILE)
            axis, keys = column_codes(start, i)
            picked = dot(one_hot(keys), table[...])
            latent = edge[span, :]
            z = pair_dot(latent, diag_w1[...]) + jnp.where(
                axis == 0,
                picked[:, :H],
                jnp.where(axis == 1, picked[:, H : 2 * H], picked[:, 2 * H :]),
            )
            u, sp = slope_and_value(z)
            inside = (keys >= 0) & (keys < 256)
            value[span, :] = keep_head(value, start, u, inside).astype(BF16)
            slope[span, :] = keep_head(slope, start, sp, inside).astype(BF16)
            pieces = one_hot_turned(start, i)
            spread = jnp.concatenate(pieces, axis=1)
            spread = (spread[:ROWS] + spread[ROWS:]).astype(BF16)
            gathered[rows, :] += dot(spread, jnp.concatenate([latent, u.astype(BF16)], axis=1))
            count = pieces[0]
            for piece in pieces[1:]:
                count = count + piece
            count = count[:ROWS] + count[ROWS:]
            degree[rows, :] += jnp.broadcast_to(
                jnp.sum(count, axis=1, keepdims=True), (ROWS, H)
            )
            return inner

        return lax.fori_loop(0, tiles_of(i), tile, carry)

    value[EDGES:, :] = tail
    slope[EDGES:, :] = tail
    lax.fori_loop(0, PLANES, forward_plane, 0)

    raw_ref[...] = jnp.zeros((RAW_ROWS, H), F32)
    w2nt = w2n_ref[...].T
    w1nt = w1n_ref[...].T

    def nodes(k, carry):
        rows = pl.ds(pl.multiple_of(k * CHUNK, CHUNK), CHUNK)
        packed = gathered[rows, :]
        aggregate = (
            packed[:, :H]
            + dot(packed[:, H:].astype(BF16), w2e_ref[...])
            + degree[rows, :] * b2e_ref[...]
        ).astype(BF16)
        x_node = jnp.concatenate([node_ref[rows, :], aggregate], axis=1)
        z_node = dot(x_node, w1n_ref[...]) + b1n_ref[...]
        u_node, sp_node = slope_and_value(z_node)
        cot_cells = cot_node_ref[rows, :]
        dz_node = (dot(cot_cells, w2nt) * sp_node).astype(BF16)
        dx_node = dot(dz_node, w1nt)
        base_ref[rows, :] = cot_cells.astype(F32) + dx_node[:, :H]
        gathered[rows, 0:H] = dx_node[:, H:]
        raw_ref[512:768, :] += dot_tn(x_node, dz_node)
        raw_ref[768:896, :] += dot_tn(u_node.astype(BF16), cot_cells)
        raw_ref[898:899, :] += jnp.sum(dz_node.astype(F32), axis=0, keepdims=True)
        raw_ref[899:900, :] += jnp.sum(cot_cells.astype(F32), axis=0, keepdims=True)
        return carry

    lax.fori_loop(0, CELLS // CHUNK, nodes, 0)
    copies[1].wait()

    def backward_plane(i, carry):
        rows = pl.ds(pl.multiple_of(i * ROWS, ROWS), ROWS)
        drow = gathered[rows, 0:H].astype(BF16)
        twice = jnp.concatenate([drow, drow], axis=0)
        sums[i + 1] = jnp.zeros((256, 3 * H), F32)

        def tile(t, inner):
            start = pl.multiple_of(first_row(i) + t * TILE, 16)
            span = pl.ds(start, TILE)
            axis, keys = column_codes(start, i)
            inside = (keys >= 0) & (keys < 256)
            added = dot(one_hot(keys), twice)
            d_wide = jnp.where(inside, cot[span, :].astype(F32) + added, 0.0)
            d_edge = d_wide.astype(BF16)
            dz = pair_dot(d_edge, diag_w2t[...]) * slope[span, :].astype(F32)
            dz_edge = dz.astype(BF16)
            new = d_edge.astype(F32) + pair_dot(dz_edge, diag_w1t[...])
            grad[span, :] = keep_head(grad, start, new, inside).astype(BF16)
            both = dot_tn(
                jnp.concatenate([edge[span, :], value[span, :]], axis=1),
                jnp.concatenate([dz_edge, d_edge], axis=1),
            )
            raw_ref[0:H, :] += both[:H, :H]
            raw_ref[384:512, :] += both[H:, H:]
            raw_ref[897:898, :] += jnp.sum(d_edge.astype(F32), axis=0, keepdims=True)
            spread = jnp.concatenate(one_hot_turned(start, i), axis=1).astype(BF16)
            parted = jnp.concatenate(
                [jnp.where(axis == a, dz, 0.0).astype(BF16) for a in range(3)], axis=1
            )
            sums[i + 1] += dot(spread, parted)
            return inner

        return lax.fori_loop(0, tiles_of(i), tile, carry)

    lax.fori_loop(0, PLANES, backward_plane, 0)
    grad_copy = pltpu.make_async_copy(grad.at[pl.ds(0, EDGES), :], grad_edge_hbm, sems.at[2])
    grad_copy.start()

    sums[0] = jnp.zeros((256, 3 * H), F32)
    sums[PLANES + 1] = jnp.zeros((256, 3 * H), F32)
    w1bt = w1e_ref[H : 2 * H, :].T
    w1ct = w1e_ref[2 * H :, :].T
    diag_w1[...] = block_diagonal(w1bt)
    diag_w2t[:, 0:H] = jnp.concatenate([w1bt, w1ct], axis=0)

    def cells(i, carry):
        rows = pl.ds(pl.multiple_of(i * ROWS, ROWS), ROWS)
        here = sums[i + 1]
        plus, minus = here[:ROWS], here[ROWS:]
        everything = plus + minus
        arrived = everything[:, :H] + everything[:, H : 2 * H] + everything[:, 2 * H :]
        yp, ym = plus[:, H : 2 * H], minus[:, H : 2 * H]
        zp, zm = plus[:, 2 * H :], minus[:, 2 * H :]
        left = (
            sums[i, 0:ROWS, 0:H]
            + sums[i + 2, ROWS : 2 * ROWS, 0:H]
            + jnp.where(low_y, 0.0, pltpu.roll(yp, 4, 0))
            + jnp.where(high_y, 0.0, pltpu.roll(ym, 124, 0))
            + jnp.where(low_z, 0.0, pltpu.roll(zp, 1, 0))
            + jnp.where(high_z, 0.0, pltpu.roll(zm, 127, 0))
        ).astype(BF16)
        arrived_low = arrived.astype(BF16)
        edge_y = jnp.where(high_y, yp, jnp.where(low_y, ym, 0.0)).astype(BF16)
        edge_z = jnp.where(high_z, zp, jnp.where(low_z, zm, 0.0)).astype(BF16)
        base_ref[rows, :] += dot(
            jnp.concatenate([left, arrived_low], axis=1), diag_w2t[:, 0:H]
        )
        outs = dot(jnp.concatenate([edge_y, edge_z], axis=1), diag_w1[...]).astype(BF16)
        out_y_ref[rows, :] = outs[:, :H]
        out_z_ref[rows, :] = outs[:, H:]
        cells_here = node_ref[rows, :]
        raw_ref[H : 2 * H, :] += dot_tn(
            jnp.concatenate([cells_here, face_y_ref[rows, :], face_z_ref[rows, :]], axis=0),
            jnp.concatenate([left, edge_y, edge_z], axis=0),
        )
        raw_ref[2 * H : 3 * H, :] += dot_tn(cells_here, arrived_low)
        raw_ref[896:897, :] += jnp.sum(arrived, axis=0, keepdims=True)
        return carry

    lax.fori_loop(0, PLANES, cells, 0)
    low_x = sums[1, ROWS : 2 * ROWS, 0:H].astype(BF16)
    high_x = sums[PLANES, 0:ROWS, 0:H].astype(BF16)
    out_x_ref[0] = dot(low_x, w1bt).astype(BF16)
    out_x_ref[1] = dot(high_x, w1bt).astype(BF16)
    raw_ref[H : 2 * H, :] += dot_tn(
        jnp.concatenate([face_x_ref[0], face_x_ref[1]], axis=0),
        jnp.concatenate([low_x, high_x], axis=0),
    )
    grad_copy.wait()


def local_terms(bounds, *operands):
    vmem = pl.BlockSpec(memory_space=pltpu.VMEM)
    anywhere = pl.BlockSpec(memory_space=pl.ANY)
    return pl.pallas_call(
        local_kernel,
        out_shape=(
            jax.ShapeDtypeStruct((EDGES, H), BF16),
            jax.ShapeDtypeStruct((CELLS, H), F32),
            jax.ShapeDtypeStruct((2, ROWS, H), BF16),
            jax.ShapeDtypeStruct((CELLS, H), BF16),
            jax.ShapeDtypeStruct((CELLS, H), BF16),
            jax.ShapeDtypeStruct((RAW_ROWS, H), F32),
        ),
        in_specs=[pl.BlockSpec(memory_space=pltpu.SMEM), vmem, vmem, anywhere, anywhere]
        + [vmem] * 12,
        out_specs=(anywhere, vmem, vmem, vmem, vmem, vmem),
        scratch_shapes=[
            pltpu.VMEM((PADDED, H), BF16),
            pltpu.VMEM((PADDED, H), BF16),
            pltpu.VMEM((PADDED, H), BF16),
            pltpu.VMEM((PADDED, H), BF16),
            pltpu.VMEM((PADDED, H), BF16),
            pltpu.VMEM((PADDED, 128), jnp.int32),
            pltpu.VMEM((112, 128), jnp.int32),
            pltpu.VMEM((CELLS + 2 * ROWS, H), F32),
            pltpu.VMEM((CELLS, H), F32),
            pltpu.VMEM((CELLS, 2 * H), F32),
            pltpu.VMEM((CELLS, H), F32),
            pltpu.VMEM((256, 3 * H), BF16),
            pltpu.VMEM((PLANES + 2, 256, 3 * H), F32),
            pltpu.VMEM((256, 256), BF16),
            pltpu.VMEM((256, 256), BF16),
            pltpu.VMEM((256, 256), BF16),
            pltpu.SemaphoreType.DMA((3,)),
        ],
        compiler_params=pltpu.CompilerParams(vmem_limit_bytes=62 * 1024 * 1024),
        cost_estimate=pl.CostEstimate(
            flops=10_000_000_000, bytes_accessed=20_000_000, transcendentals=2_000_000
        ),
    )(bounds, *operands)


def neighbours(axis, low, high):
    peers = lax.axis_size(axis)
    up = [(i, (i + 1) % peers) for i in range(peers)]
    down = [(b, a) for a, b in up]
    return lax.ppermute(high, axis, up), lax.ppermute(low, axis, down)


def on_device(
    node_latent,
    edge_latent,
    senders,
    receivers,
    w1_edge,
    b1_edge,
    w2_edge,
    b2_edge,
    w1_node,
    b1_node,
    w2_node,
    cot_node,
    cot_edge,
):
    side_x, side_y, side_z, latent = node_latent.shape
    x_low, x_high = neighbours("gx", node_latent[:1], node_latent[-1:])
    y_low, y_high = neighbours("gy", node_latent[:, :1], node_latent[:, -1:])
    z_low, z_high = neighbours("gz", node_latent[:, :, :1], node_latent[:, :, -1:])
    face_x = jnp.concatenate([x_low, x_high], axis=0).reshape(2, ROWS, latent)
    face_y = jnp.concatenate(
        [y_low, jnp.zeros((side_x, side_y - 2, side_z, latent), BF16), y_high], axis=1
    ).reshape(CELLS, latent)
    face_z = jnp.concatenate(
        [z_low, jnp.zeros((side_x, side_y, side_z - 2, latent), BF16), z_high], axis=2
    ).reshape(CELLS, latent)
    receiver_ids = receivers.reshape(96, 128)
    marks = jnp.arange(PLANES + 1, dtype=jnp.int32) * ROWS
    bounds = jnp.sum(
        (receivers.reshape(1, EDGES) < marks[:, None]).astype(jnp.int32), axis=1
    )
    grad_edge, base, out_x, out_y, out_z, raw = local_terms(
        bounds,
        senders.reshape(96, 128),
        receiver_ids,
        edge_latent.reshape(EDGES, latent),
        cot_edge.reshape(EDGES, latent),
        node_latent.reshape(CELLS, latent),
        cot_node.reshape(CELLS, latent),
        face_x,
        face_y,
        face_z,
        w1_edge,
        b1_edge.reshape(1, latent),
        w2_edge,
        b2_edge.reshape(1, latent),
        w1_node,
        b1_node.reshape(1, latent),
        w2_node,
    )
    total = lax.psum(raw, ("gx", "gy", "gz"))
    out_x = out_x.reshape(2, side_y, side_z, latent)
    out_y = out_y.reshape(side_x, side_y, side_z, latent)
    out_z = out_z.reshape(side_x, side_y, side_z, latent)
    from_low_x, from_high_x = neighbours("gx", out_x[:1], out_x[1:])
    from_low_y, from_high_y = neighbours("gy", out_y[:, :1], out_y[:, -1:])
    from_low_z, from_high_z = neighbours("gz", out_z[:, :, :1], out_z[:, :, -1:])
    interior = base.reshape(side_x, side_y, side_z, latent)
    interior = interior.at[:1].add(from_low_x.astype(F32)).at[-1:].add(from_high_x.astype(F32))
    interior = (
        interior.at[:, :1].add(from_low_y.astype(F32)).at[:, -1:].add(from_high_y.astype(F32))
    )
    interior = (
        interior.at[:, :, :1]
        .add(from_low_z.astype(F32))
        .at[:, :, -1:]
        .add(from_high_z.astype(F32))
    )
    grad_node = interior.astype(BF16)
    squares = jnp.sum(total * total)
    factor = 1.0 / jnp.maximum(1.0, jnp.sqrt(squares / (7 * latent * latent + 4 * latent)))
    scaled = total * factor
    return (
        grad_node,
        grad_edge.reshape(edge_latent.shape),
        scaled[:384],
        scaled[384:512],
        scaled[512:768],
        scaled[768:896],
        scaled[896:900],
    )


def solution(mesh):
    cell = P("gx", "gy", "gz", None)
    slots = P("gx", "gy", "gz", None, None)
    placed = (cell, slots, cell, cell, P(), P(), P(), P(), P(), P(), P(), cell, slots)
    return jax.shard_map(
        on_device,
        mesh=mesh,
        in_specs=placed,
        out_specs=(cell, slots, P(), P(), P(), P(), P()),
        check_vma=False,
    )
```

```python
import functools

import jax
import jax.numpy as jnp
from jax import lax
from jax.experimental import pallas as pl
from jax.experimental.pallas import tpu as pltpu
from jax.sharding import PartitionSpec as P

H = 128
PLANES = 16
ROWS = 128
CELLS = PLANES * ROWS
EDGES = 12288
TILE = 896
PADDED = EDGES + TILE
CHUNK = 512
RAW_ROWS = 1024
X_LOW, X_HIGH, Y_LOW, Y_HIGH, Z_LOW, Z_HIGH, FACES = 0, 128, 256, 320, 384, 896, 1408
SPANS = ((X_LOW, 128), (X_HIGH, 128), (Y_LOW, 64), (Y_HIGH, 64), (Z_LOW, 512), (Z_HIGH, 512))
MESH = pl.DeviceIdType.MESH

F32 = jnp.float32
BF16 = jnp.bfloat16


def dot(a, b):
    return jnp.dot(a, b, preferred_element_type=F32)


def dot_tn(a, b):
    return lax.dot_general(a, b, (((0,), (0,)), ((), ())), preferred_element_type=F32)


def pair_dot(rows, diagonal):
    half = rows.shape[0] // 2
    both = dot(jnp.concatenate([rows[:half], rows[half:]], axis=1), diagonal)
    return jnp.concatenate([both[:, :H], both[:, H:]], axis=0)


def block_diagonal(w):
    zero = jnp.zeros_like(w)
    return jnp.concatenate(
        [jnp.concatenate([w, zero], axis=1), jnp.concatenate([zero, w], axis=1)], axis=0
    )


def slope_and_value(z):
    sigma = 0.5 * jnp.tanh(0.5 * z) + 0.5
    value = z * sigma
    return value, sigma * (1.0 + (z - value))


def local_kernel(
    bounds,
    send_ref,
    recv_ref,
    edge_hbm,
    cot_edge_hbm,
    node_ref,
    cot_node_ref,
    face_ref,
    w1e_ref,
    b1e_ref,
    w2e_ref,
    b2e_ref,
    w1n_ref,
    b1n_ref,
    w2n_ref,
    grad_edge_hbm,
    base_ref,
    out_ref,
    raw_ref,
    edge,
    cot,
    value,
    slope,
    grad,
    code_col,
    code_row,
    proj,
    proj_own,
    proj_face,
    wide,
    leaving,
    gathered,
    degree,
    table,
    sums,
    diag_w1,
    diag_w2t,
    diag_w1t,
    sems,
):
    copies = [
        pltpu.make_async_copy(edge_hbm, edge.at[pl.ds(0, EDGES), :], sems.at[0]),
        pltpu.make_async_copy(cot_edge_hbm, cot.at[pl.ds(0, EDGES), :], sems.at[1]),
    ]
    for item in copies:
        item.start()

    tail = jnp.zeros((TILE, H), BF16)
    edge[EDGES:, :] = tail
    cot[EDGES:, :] = tail

    recv = recv_ref[...]
    step = send_ref[...] - (
        ((recv >> 7) + 1) * 204 + (((recv >> 2) & 31) + 1) * 6 + (recv & 3) + 1
    )
    size = jnp.abs(step)
    axis = jnp.where(size == 204, 0, jnp.where(size == 6, 1, 2))
    key = (recv >> 7) * 256 + jnp.where(step < 0, 128, 0) + (recv & 127)
    code = key * 4 + axis
    code_row[0:96, :] = code
    code_row[96:, :] = jnp.full((code_row.shape[0] - 96, 128), -4, jnp.int32)
    turned = jnp.concatenate([code.astype(F32), jnp.zeros((32, 128), F32)], axis=0).T.astype(
        jnp.int32
    )
    for k in range(96):
        code_col[k * 128 : (k + 1) * 128, :] = jnp.broadcast_to(turned[:, k : k + 1], (128, 128))
    code_col[EDGES:, :] = jnp.full((TILE, 128), -4, jnp.int32)

    w1a = w1e_ref[0:H, :]
    w1b = w1e_ref[H : 2 * H, :]
    w1c = w1e_ref[2 * H :, :]
    diag_w1[...] = block_diagonal(w1a)
    diag_w2t[...] = block_diagonal(w2e_ref[...].T)
    diag_w1t[...] = block_diagonal(w1a.T)
    b1e = b1e_ref[...]

    proj_face[...] = dot(face_ref[...], w1b)
    proj[0:ROWS, :] = proj_face[X_LOW : X_LOW + ROWS, :]
    proj[ROWS * (PLANES + 1) :, :] = proj_face[X_HIGH : X_HIGH + ROWS, :]
    wide[...] = jnp.zeros((2 * ROWS, H), F32)
    w1bc = jnp.concatenate([w1b, w1c], axis=1)

    def project(k, carry):
        rows = pl.ds(pl.multiple_of(k * CHUNK, CHUNK), CHUNK)
        both = dot(node_ref[rows, :], w1bc)
        proj[pl.ds(pl.multiple_of(k * CHUNK + ROWS, ROWS), CHUNK), :] = both[:, :H]
        proj_own[rows, :] = both[:, H:] + b1e
        return carry

    lax.fori_loop(0, CELLS // CHUNK, project, 0)

    row_id = lax.broadcasted_iota(jnp.int32, (ROWS, H), 0)
    low_z = (row_id & 3) == 0
    high_z = (row_id & 3) == 3
    low_y = row_id < 4
    high_y = row_id >= 124

    def first_row(i):
        return (bounds[i] >> 4) << 4

    def tiles_of(i):
        lo, hi = bounds[i], bounds[i + 1]
        count = (hi - first_row(i) + (TILE - 1)) // TILE
        return jnp.where(hi > lo, count, 0)

    def column_codes(start, i):
        codes = code_col[pl.ds(start, TILE), :]
        return codes & 3, (codes >> 2) - 256 * i

    def one_hot(keys):
        lane = lax.broadcasted_iota(jnp.int32, (TILE, 128), 1)
        low = jnp.where(keys == lane, 1.0, 0.0)
        high = jnp.where(keys == lane + 128, 1.0, 0.0)
        return jnp.concatenate([low, high], axis=1).astype(BF16)

    def one_hot_turned(start, i):
        q = start >> 7
        off = start & 127
        turn = (128 - off) & 127
        here = pltpu.roll(code_row[pl.ds(q, 8), :], turn, 1)
        there = pltpu.roll(code_row[pl.ds(q + 1, 8), :], turn, 1)
        lane = lax.broadcasted_iota(jnp.int32, (8, 128), 1)
        keys = (jnp.where(lane < 128 - off, here, there) >> 2) - 256 * i
        slot = lax.broadcasted_iota(jnp.int32, (256, 128), 0)
        pieces = [
            jnp.where(jnp.broadcast_to(keys[k : k + 1, :], (256, 128)) == slot, 1.0, 0.0)
            for k in range(TILE // 128)
        ]
        return pieces

    def keep_head(ref, start, new, inside):
        old = ref[pl.ds(start, 16), :].astype(F32)
        return jnp.concatenate([jnp.where(inside[:16], new[:16], old), new[16:]], axis=0)

    copies[0].wait()

    def forward_plane(i, carry):
        rows = pl.ds(pl.multiple_of(i * ROWS, ROWS), ROWS)
        own = proj_own[rows, :]
        mine = proj[pl.ds(pl.multiple_of((i + 1) * ROWS, ROWS), ROWS), :]
        above = proj[pl.ds(pl.multiple_of((i + 2) * ROWS, ROWS), ROWS), :]
        below = proj[rows, :]
        wide[0:4, :] = proj_face[pl.ds(Y_LOW + 4 * i, 4), :]
        wide[124:128, :] = proj_face[pl.ds(Y_HIGH + 4 * i, 4), :]
        wide[pl.ds(ROWS, 32, stride=4), :] = proj_face[pl.ds(Z_LOW + 32 * i, 32), :]
        wide[pl.ds(ROWS + 3, 32, stride=4), :] = proj_face[pl.ds(Z_HIGH + 32 * i, 32), :]
        side_y = wide[:ROWS, :]
        side_z = wide[ROWS:, :]
        up_y = jnp.where(high_y, side_y, pltpu.roll(mine, 124, 0))
        down_y = jnp.where(low_y, side_y, pltpu.roll(mine, 4, 0))
        up_z = jnp.where(high_z, side_z, pltpu.roll(mine, 127, 0))
        down_z = jnp.where(low_z, side_z, pltpu.roll(mine, 1, 0))
        table[0:ROWS, :] = jnp.concatenate([above + own, up_y + own, up_z + own], axis=1).astype(
            BF16
        )
        table[ROWS:, :] = jnp.concatenate(
            [below + own, down_y + own, down_z + own], axis=1
        ).astype(BF16)
        gathered[rows, :] = jnp.zeros((ROWS, 2 * H), F32)
        degree[rows, :] = jnp.zeros((ROWS, H), F32)

        def tile(t, inner):
            start = pl.multiple_of(first_row(i) + t * TILE, 16)
            span = pl.ds(start, TILE)
            axis, keys = column_codes(start, i)
            picked = dot(one_hot(keys), table[...])
            latent = edge[span, :]
            z = pair_dot(latent, diag_w1[...]) + jnp.where(
                axis == 0,
                picked[:, :H],
                jnp.where(axis == 1, picked[:, H : 2 * H], picked[:, 2 * H :]),
            )
            u, sp = slope_and_value(z)
            inside = (keys >= 0) & (keys < 256)
            value[span, :] = keep_head(value, start, u, inside).astype(BF16)
            slope[span, :] = keep_head(slope, start, sp, inside).astype(BF16)
            pieces = one_hot_turned(start, i)
            spread = jnp.concatenate(pieces, axis=1)
            spread = (spread[:ROWS] + spread[ROWS:]).astype(BF16)
            gathered[rows, :] += dot(spread, jnp.concatenate([latent, u.astype(BF16)], axis=1))
            count = pieces[0]
            for piece in pieces[1:]:
                count = count + piece
            count = count[:ROWS] + count[ROWS:]
            degree[rows, :] += jnp.broadcast_to(
                jnp.sum(count, axis=1, keepdims=True), (ROWS, H)
            )
            return inner

        return lax.fori_loop(0, tiles_of(i), tile, carry)

    value[EDGES:, :] = tail
    slope[EDGES:, :] = tail
    lax.fori_loop(0, PLANES, forward_plane, 0)

    raw_ref[...] = jnp.zeros((RAW_ROWS, H), F32)
    w2nt = w2n_ref[...].T
    w1nt = w1n_ref[...].T

    def nodes(k, carry):
        rows = pl.ds(pl.multiple_of(k * CHUNK, CHUNK), CHUNK)
        packed = gathered[rows, :]
        aggregate = (
            packed[:, :H]
            + dot(packed[:, H:].astype(BF16), w2e_ref[...])
            + degree[rows, :] * b2e_ref[...]
        ).astype(BF16)
        x_node = jnp.concatenate([node_ref[rows, :], aggregate], axis=1)
        z_node = dot(x_node, w1n_ref[...]) + b1n_ref[...]
        u_node, sp_node = slope_and_value(z_node)
        cot_cells = cot_node_ref[rows, :]
        dz_node = (dot(cot_cells, w2nt) * sp_node).astype(BF16)
        dx_node = dot(dz_node, w1nt)
        base_ref[rows, :] = cot_cells.astype(F32) + dx_node[:, :H]
        gathered[rows, 0:H] = dx_node[:, H:]
        raw_ref[512:768, :] += dot_tn(x_node, dz_node)
        raw_ref[768:896, :] += dot_tn(u_node.astype(BF16), cot_cells)
        raw_ref[898:899, :] += jnp.sum(dz_node.astype(F32), axis=0, keepdims=True)
        raw_ref[899:900, :] += jnp.sum(cot_cells.astype(F32), axis=0, keepdims=True)
        return carry

    lax.fori_loop(0, CELLS // CHUNK, nodes, 0)
    copies[1].wait()

    def backward_plane(i, carry):
        rows = pl.ds(pl.multiple_of(i * ROWS, ROWS), ROWS)
        drow = gathered[rows, 0:H].astype(BF16)
        twice = jnp.concatenate([drow, drow], axis=0)
        sums[i + 1] = jnp.zeros((256, 3 * H), F32)

        def tile(t, inner):
            start = pl.multiple_of(first_row(i) + t * TILE, 16)
            span = pl.ds(start, TILE)
            axis, keys = column_codes(start, i)
            inside = (keys >= 0) & (keys < 256)
            added = dot(one_hot(keys), twice)
            d_wide = jnp.where(inside, cot[span, :].astype(F32) + added, 0.0)
            d_edge = d_wide.astype(BF16)
            dz = pair_dot(d_edge, diag_w2t[...]) * slope[span, :].astype(F32)
            dz_edge = dz.astype(BF16)
            new = d_edge.astype(F32) + pair_dot(dz_edge, diag_w1t[...])
            grad[span, :] = keep_head(grad, start, new, inside).astype(BF16)
            both = dot_tn(
                jnp.concatenate([edge[span, :], value[span, :]], axis=1),
                jnp.concatenate([dz_edge, d_edge], axis=1),
            )
            raw_ref[0:H, :] += both[:H, :H]
            raw_ref[384:512, :] += both[H:, H:]
            raw_ref[897:898, :] += jnp.sum(d_edge.astype(F32), axis=0, keepdims=True)
            spread = jnp.concatenate(one_hot_turned(start, i), axis=1).astype(BF16)
            parted = jnp.concatenate(
                [jnp.where(axis == a, dz, 0.0).astype(BF16) for a in range(3)], axis=1
            )
            sums[i + 1] += dot(spread, parted)
            return inner

        return lax.fori_loop(0, tiles_of(i), tile, carry)

    lax.fori_loop(0, PLANES, backward_plane, 0)
    grad_copy = pltpu.make_async_copy(grad.at[pl.ds(0, EDGES), :], grad_edge_hbm, sems.at[2])
    grad_copy.start()

    sums[0] = jnp.zeros((256, 3 * H), F32)
    sums[PLANES + 1] = jnp.zeros((256, 3 * H), F32)
    w1bt = w1e_ref[H : 2 * H, :].T
    w1ct = w1e_ref[2 * H :, :].T
    diag_w2t[:, 0:H] = jnp.concatenate([w1bt, w1ct], axis=0)

    def cells(i, carry):
        rows = pl.ds(pl.multiple_of(i * ROWS, ROWS), ROWS)
        here = sums[i + 1]
        plus, minus = here[:ROWS], here[ROWS:]
        everything = plus + minus
        arrived = everything[:, :H] + everything[:, H : 2 * H] + everything[:, 2 * H :]
        yp, ym = plus[:, H : 2 * H], minus[:, H : 2 * H]
        zp, zm = plus[:, 2 * H :], minus[:, 2 * H :]
        left = (
            sums[i, 0:ROWS, 0:H]
            + sums[i + 2, ROWS : 2 * ROWS, 0:H]
            + jnp.where(low_y, 0.0, pltpu.roll(yp, 4, 0))
            + jnp.where(high_y, 0.0, pltpu.roll(ym, 124, 0))
            + jnp.where(low_z, 0.0, pltpu.roll(zp, 1, 0))
            + jnp.where(high_z, 0.0, pltpu.roll(zm, 127, 0))
        ).astype(BF16)
        arrived_low = arrived.astype(BF16)
        leaving[pl.ds(Y_LOW + 4 * i, 4), :] = ym[:4]
        leaving[pl.ds(Y_HIGH + 4 * i, 4), :] = yp[124:]
        wide[0:ROWS, :] = zm
        wide[ROWS:, :] = zp
        leaving[pl.ds(Z_LOW + 32 * i, 32), :] = wide[pl.ds(0, 32, stride=4), :]
        leaving[pl.ds(Z_HIGH + 32 * i, 32), :] = wide[pl.ds(ROWS + 3, 32, stride=4), :]
        base_ref[rows, :] += dot(
            jnp.concatenate([left, arrived_low], axis=1), diag_w2t[:, 0:H]
        )
        cells_here = node_ref[rows, :]
        raw_ref[H : 2 * H, :] += dot_tn(cells_here, left)
        raw_ref[2 * H : 3 * H, :] += dot_tn(cells_here, arrived_low)
        raw_ref[896:897, :] += jnp.sum(arrived, axis=0, keepdims=True)
        return carry

    lax.fori_loop(0, PLANES, cells, 0)
    leaving[X_LOW : X_LOW + ROWS, :] = sums[1, ROWS : 2 * ROWS, 0:H]
    leaving[X_HIGH : X_HIGH + ROWS, :] = sums[PLANES, 0:ROWS, 0:H]
    gone = leaving[...].astype(BF16)
    out_ref[...] = dot(gone, w1bt).astype(BF16)
    raw_ref[H : 2 * H, :] += dot_tn(face_ref[...], gone)
    grad_copy.wait()


def local_terms(bounds, *operands):
    vmem = pl.BlockSpec(memory_space=pltpu.VMEM)
    anywhere = pl.BlockSpec(memory_space=pl.ANY)
    return pl.pallas_call(
        local_kernel,
        out_shape=(
            jax.ShapeDtypeStruct((EDGES, H), BF16),
            jax.ShapeDtypeStruct((CELLS, H), F32),
            jax.ShapeDtypeStruct((FACES, H), BF16),
            jax.ShapeDtypeStruct((RAW_ROWS, H), F32),
        ),
        in_specs=[pl.BlockSpec(memory_space=pltpu.SMEM), vmem, vmem, anywhere, anywhere]
        + [vmem] * 10,
        out_specs=(anywhere, vmem, vmem, vmem),
        scratch_shapes=[
            pltpu.VMEM((PADDED, H), BF16),
            pltpu.VMEM((PADDED, H), BF16),
            pltpu.VMEM((PADDED, H), BF16),
            pltpu.VMEM((PADDED, H), BF16),
            pltpu.VMEM((PADDED, H), BF16),
            pltpu.VMEM((PADDED, 128), jnp.int32),
            pltpu.VMEM((112, 128), jnp.int32),
            pltpu.VMEM((CELLS + 2 * ROWS, H), F32),
            pltpu.VMEM((CELLS, H), F32),
            pltpu.VMEM((FACES, H), F32),
            pltpu.VMEM((2 * ROWS, H), F32),
            pltpu.VMEM((FACES, H), F32),
            pltpu.VMEM((CELLS, 2 * H), F32),
            pltpu.VMEM((CELLS, H), F32),
            pltpu.VMEM((256, 3 * H), BF16),
            pltpu.VMEM((PLANES + 2, 256, 3 * H), F32),
            pltpu.VMEM((256, 256), BF16),
            pltpu.VMEM((256, 256), BF16),
            pltpu.VMEM((256, 256), BF16),
            pltpu.SemaphoreType.DMA((3,)),
        ],
        compiler_params=pltpu.CompilerParams(vmem_limit_bytes=62 * 1024 * 1024),
        cost_estimate=pl.CostEstimate(
            flops=10_000_000_000, bytes_accessed=20_000_000, transcendentals=2_000_000
        ),
    )(bounds, *operands)


def place():
    return tuple(lax.axis_index(name) for name in ("gx", "gy", "gz"))


def sizes():
    return tuple(lax.axis_size(name) for name in ("gx", "gy", "gz"))


def across(side):
    dim, up = side // 2, side % 2
    here, count = place(), sizes()
    beyond = list(here)
    beyond[dim] = lax.rem(here[dim] + (1 if up else count[dim] - 1), count[dim])
    return tuple(beyond)


def face_copies(source, target, send_sems, recv_sems):
    copies = []
    for side, (first, rows) in enumerate(SPANS):
        opposite = SPANS[side ^ 1][0]
        copies.append(
            pltpu.make_async_remote_copy(
                src_ref=source.at[pl.ds(first, rows), :],
                dst_ref=target.at[pl.ds(opposite, rows), :],
                send_sem=send_sems.at[side],
                recv_sem=recv_sems.at[side],
                device_id=across(side),
                device_id_type=MESH,
            )
        )
    return copies


def halo_kernel(node_ref, recv_ref, face_ref, bounds_ref, cells, packed, send_sems, recv_sems):
    barrier = pltpu.get_barrier_semaphore()
    for side in range(6):
        pl.semaphore_signal(barrier, inc=1, device_id=across(side), device_id_type=MESH)
    cells[...] = node_ref[...].astype(F32)
    packed[X_LOW : X_LOW + ROWS, :] = node_ref[0:ROWS, :]
    packed[X_HIGH : X_HIGH + ROWS, :] = node_ref[CELLS - ROWS :, :]
    for first, at in ((Y_LOW, 0), (Y_HIGH, 124)):
        strips = [cells[ROWS * i + at : ROWS * i + at + 4, :] for i in range(PLANES)]
        packed[first : first + 64, :] = jnp.concatenate(strips, axis=0).astype(BF16)
    packed[Z_LOW : Z_LOW + 512, :] = cells[pl.ds(0, 512, stride=4), :].astype(BF16)
    packed[Z_HIGH : Z_HIGH + 512, :] = cells[pl.ds(3, 512, stride=4), :].astype(BF16)
    pl.semaphore_wait(barrier, 6)
    copies = face_copies(packed, face_ref, send_sems, recv_sems)
    for side in (5, 4, 1, 0, 3, 2):
        copies[side].start()
    recv = recv_ref[...]
    for i in range(PLANES + 1):
        below = jnp.where(recv < ROWS * i, 1.0, 0.0)
        bounds_ref[i] = jnp.sum(below).astype(jnp.int32)
    for item in copies:
        item.wait()


def halo(node, recv):
    vmem = pl.BlockSpec(memory_space=pltpu.VMEM)
    return pl.pallas_call(
        halo_kernel,
        out_shape=(
            jax.ShapeDtypeStruct((FACES, H), BF16),
            jax.ShapeDtypeStruct((PLANES + 1,), jnp.int32),
        ),
        in_specs=[vmem, vmem],
        out_specs=(vmem, pl.BlockSpec(memory_space=pltpu.SMEM)),
        scratch_shapes=[
            pltpu.VMEM((CELLS, H), F32),
            pltpu.VMEM((FACES, H), BF16),
            pltpu.SemaphoreType.DMA((6,)),
            pltpu.SemaphoreType.DMA((6,)),
        ],
        compiler_params=pltpu.CompilerParams(
            collective_id=0, has_side_effects=True, vmem_limit_bytes=16 * 1024 * 1024
        ),
    )(node, recv)


def finish_kernel(
    base_ref,
    out_ref,
    raw_ref,
    grad_ref,
    w1e_ref,
    w2e_ref,
    w1n_ref,
    w2n_ref,
    bias_ref,
    faces,
    cells,
    partner_part,
    half,
    parts,
    mine,
    full,
    send_sems,
    recv_sems,
    pair_send,
    pair_recv,
    all_send,
    all_recv,
):
    (ga, gb, gc), (na, nb, nc) = place(), sizes()
    nz = nc // 2
    chips = na * nb * nz
    chip_z, core = lax.div(gc, 2), lax.rem(gc, 2)
    chip = (ga * nb + gb) * nz + chip_z
    partner = (ga, gb, 2 * chip_z + 1 - core)

    def peer(d):
        da, rest = lax.div(d, nb * nz), lax.rem(d, nb * nz)
        db, dz = lax.div(rest, nz), lax.rem(rest, nz)
        pa, pb = lax.rem(ga + da, na), lax.rem(gb + db, nb)
        pz = lax.rem(chip_z + dz, nz)
        return (pa, pb, 2 * pz + core), (pa * nb + pb) * nz + pz

    barrier = pltpu.get_barrier_semaphore()

    def greet(d, carry):
        pl.semaphore_signal(barrier, inc=1, device_id=peer(d)[0], device_id_type=MESH)
        return carry

    pl.semaphore_signal(barrier, inc=1, device_id=partner, device_id_type=MESH)
    lax.fori_loop(1, chips, greet, 0)
    for side in (4, 5):
        pl.semaphore_signal(barrier, inc=1, device_id=across(side), device_id_type=MESH)
    pl.semaphore_wait(barrier, chips + 2)

    def to_partner(source, target, k):
        return pltpu.make_async_remote_copy(
            src_ref=source,
            dst_ref=target,
            send_sem=pair_send.at[k],
            recv_sem=pair_recv.at[k],
            device_id=partner,
            device_id_type=MESH,
        )

    first = to_partner(raw_ref.at[pl.ds((1 - core) * chips, chips)], partner_part, 0)
    first.start()
    halos = face_copies(out_ref, faces, send_sems, recv_sems)
    for side in (0, 1, 2, 3):
        halos[side].start()
    first.wait()
    half[...] = raw_ref[pl.ds(core * chips, chips)] + partner_part[...]

    def scatter(d, carry):
        where, other = peer(d)
        pltpu.make_async_remote_copy(
            src_ref=half.at[other],
            dst_ref=parts.at[chip],
            send_sem=all_send.at[0],
            recv_sem=all_recv.at[0],
            device_id=where,
            device_id_type=MESH,
        ).start()
        return carry

    lax.fori_loop(1, chips, scatter, 0)
    for side in (4, 5):
        halos[side].start()
    parts[chip] = half[chip]

    def settle(buffer, sem):
        span = buffer.at[pl.ds(0, chips - 1)]
        pltpu.make_async_copy(span, span, sem).wait()

    settle(parts, all_recv.at[0])
    mine[...] = jnp.sum(parts[...], axis=0)

    def gather(d, carry):
        where, _ = peer(d)
        pltpu.make_async_remote_copy(
            src_ref=mine,
            dst_ref=full.at[core * chips + chip],
            send_sem=all_send.at[1],
            recv_sem=all_recv.at[1],
            device_id=where,
            device_id_type=MESH,
        ).start()
        return carry

    lax.fori_loop(1, chips, gather, 0)
    full[core * chips + chip] = mine[...]
    for item in halos:
        item.wait()
    cells[...] = base_ref[...]
    cells[0:ROWS, :] += faces[X_LOW : X_LOW + ROWS, :].astype(F32)
    cells[CELLS - ROWS :, :] += faces[X_HIGH : X_HIGH + ROWS, :].astype(F32)
    for start, at in ((Y_LOW, 0), (Y_HIGH, 124)):
        strip = faces[start : start + 64, :].astype(F32)
        for i in range(PLANES):
            cells[ROWS * i + at : ROWS * i + at + 4, :] += strip[4 * i : 4 * i + 4]
    cells[pl.ds(0, 512, stride=4), :] += faces[Z_LOW : Z_LOW + 512, :].astype(F32)
    cells[pl.ds(3, 512, stride=4), :] += faces[Z_HIGH : Z_HIGH + 512, :].astype(F32)
    grad_ref[...] = cells[...].astype(BF16)
    settle(full, all_recv.at[1])
    held = pl.ds(core * chips, chips)
    last = to_partner(full.at[held], full.at[held], 1)
    last.start()
    settle(half, all_send.at[0])
    settle(half, all_send.at[1])
    last.wait()
    total = full[...].reshape(RAW_ROWS, H)
    squares = jnp.sum(total * total, axis=0, keepdims=True)
    squares = jnp.sum(squares, axis=1, keepdims=True)
    factor = 1.0 / jnp.maximum(1.0, jnp.sqrt(squares / (7 * H * H + 4 * H)))
    scaled = total * factor
    w1e_ref[...] = scaled[:384]
    w2e_ref[...] = scaled[384:512]
    w1n_ref[...] = scaled[512:768]
    w2n_ref[...] = scaled[768:896]
    bias_ref[...] = scaled[896:900]


def finish(base, out, raw):
    chips = lax.axis_size("gx") * lax.axis_size("gy") * lax.axis_size("gz") // 2
    block = RAW_ROWS // (2 * chips)
    vmem = pl.BlockSpec(memory_space=pltpu.VMEM)
    return pl.pallas_call(
        finish_kernel,
        out_shape=(
            jax.ShapeDtypeStruct((CELLS, H), BF16),
            jax.ShapeDtypeStruct((384, H), F32),
            jax.ShapeDtypeStruct((128, H), F32),
            jax.ShapeDtypeStruct((256, H), F32),
            jax.ShapeDtypeStruct((128, H), F32),
            jax.ShapeDtypeStruct((4, H), F32),
        ),
        in_specs=[vmem] * 3,
        out_specs=(vmem,) * 6,
        scratch_shapes=[
            pltpu.VMEM((FACES, H), BF16),
            pltpu.VMEM((CELLS, H), F32),
            pltpu.VMEM((chips, block, H), F32),
            pltpu.VMEM((chips, block, H), F32),
            pltpu.VMEM((chips, block, H), F32),
            pltpu.VMEM((block, H), F32),
            pltpu.VMEM((2 * chips, block, H), F32),
            pltpu.SemaphoreType.DMA((6,)),
            pltpu.SemaphoreType.DMA((6,)),
            pltpu.SemaphoreType.DMA((2,)),
            pltpu.SemaphoreType.DMA((2,)),
            pltpu.SemaphoreType.DMA((2,)),
            pltpu.SemaphoreType.DMA((2,)),
        ],
        compiler_params=pltpu.CompilerParams(
            collective_id=1, has_side_effects=True, vmem_limit_bytes=24 * 1024 * 1024
        ),
    )(base, out, raw.reshape(2 * chips, block, H))


def on_device(
    node_latent,
    edge_latent,
    senders,
    receivers,
    w1_edge,
    b1_edge,
    w2_edge,
    b2_edge,
    w1_node,
    b1_node,
    w2_node,
    cot_node,
    cot_edge,
):
    cells = node_latent.reshape(CELLS, H)
    receiver_ids = receivers.reshape(96, 128)
    faces, bounds = halo(cells, receiver_ids)
    grad_edge, base, out, raw = local_terms(
        bounds,
        senders.reshape(96, 128),
        receiver_ids,
        edge_latent.reshape(EDGES, H),
        cot_edge.reshape(EDGES, H),
        cells,
        cot_node.reshape(CELLS, H),
        faces,
        w1_edge,
        b1_edge.reshape(1, H),
        w2_edge,
        b2_edge.reshape(1, H),
        w1_node,
        b1_node.reshape(1, H),
        w2_node,
    )
    grad_node, *grads = finish(base, out, raw)
    return (grad_node.reshape(node_latent.shape), grad_edge.reshape(edge_latent.shape), *grads)


def solution(mesh):
    cell = P("gx", "gy", "gz", None)
    slots = P("gx", "gy", "gz", None, None)
    placed = (cell, slots, cell, cell, P(), P(), P(), P(), P(), P(), P(), cell, slots)
    return jax.shard_map(
        on_device,
        mesh=mesh,
        in_specs=placed,
        out_specs=(cell, slots, P(), P(), P(), P(), P()),
        check_vma=False,
    )
```

```python
import functools

import jax
import jax.numpy as jnp
from jax import lax
from jax.experimental import pallas as pl
from jax.experimental.pallas import tpu as pltpu
from jax.sharding import PartitionSpec as P

H = 128
PLANES = 16
ROWS = 128
CELLS = PLANES * ROWS
EDGES = 12288
TILE = 896
LOCAL_VMEM = 42 * 1024 * 1024
PADDED = EDGES + TILE
CHUNK = 512
RAW_ROWS = 1024
X_LOW, X_HIGH, Y_LOW, Y_HIGH, Z_LOW, Z_HIGH, FACES = 0, 128, 256, 320, 384, 896, 1408
SPANS = ((X_LOW, 128), (X_HIGH, 128), (Y_LOW, 64), (Y_HIGH, 64), (Z_LOW, 512), (Z_HIGH, 512))
MESH = pl.DeviceIdType.MESH

F32 = jnp.float32
BF16 = jnp.bfloat16


def dot(a, b):
    return jnp.dot(a, b, preferred_element_type=F32)


def dot_tn(a, b):
    return lax.dot_general(a, b, (((0,), (0,)), ((), ())), preferred_element_type=F32)


def pair_dot(rows, diagonal):
    half = rows.shape[0] // 2
    both = dot(jnp.concatenate([rows[:half], rows[half:]], axis=1), diagonal)
    return jnp.concatenate([both[:, :H], both[:, H:]], axis=0)


def block_diagonal(w):
    zero = jnp.zeros_like(w)
    return jnp.concatenate(
        [jnp.concatenate([w, zero], axis=1), jnp.concatenate([zero, w], axis=1)], axis=0
    )


def slope_and_value(z):
    sigma = 0.5 * jnp.tanh(0.5 * z) + 0.5
    value = z * sigma
    return value, sigma * (1.0 + (z - value))


def steps_of(send, recv):
    step = send - (((recv >> 7) + 1) * 204 + (((recv >> 2) & 31) + 1) * 6 + (recv & 3) + 1)
    size = jnp.abs(step)
    return step, jnp.where(size == 204, 0, jnp.where(size == 6, 1, 2))


def local_kernel(
    bounds,
    send_ref,
    recv_ref,
    edge_hbm,
    cot_edge_hbm,
    node_ref,
    cot_node_ref,
    face_ref,
    key_col,
    kind_col,
    w1e_ref,
    b1e_ref,
    w2e_ref,
    b2e_ref,
    w1n_ref,
    b1n_ref,
    w2n_ref,
    grad_edge_hbm,
    base_ref,
    out_ref,
    raw_ref,
    edge,
    cot,
    value,
    slope,
    grad,
    code_row,
    proj,
    proj_own,
    proj_face,
    wide,
    leaving,
    gathered,
    degree,
    tables,
    sums,
    diag_w1,
    diag_w2t,
    diag_w1t,
    z_a,
    z_b,
    d_a,
    d_b,
    starts,
    planes,
    sems,
):
    copies = [
        pltpu.make_async_copy(edge_hbm, edge.at[pl.ds(0, EDGES), :], sems.at[0]),
        pltpu.make_async_copy(cot_edge_hbm, cot.at[pl.ds(0, EDGES), :], sems.at[1]),
    ]
    for item in copies:
        item.start()

    tail = jnp.zeros((TILE, H), BF16)
    for ref in (edge, cot, value, slope):
        ref[EDGES:, :] = tail

    def list_plane(i, n):
        lo, hi = bounds[i], bounds[i + 1]
        first = (lo >> 4) << 4
        count = jnp.where(hi > lo, (hi - first + (TILE - 1)) // TILE, 0)

        def put(t, n):
            starts[n] = first + t * TILE
            planes[n] = i
            return n + 1

        return lax.fori_loop(0, count, put, n)

    starts[0] = EDGES
    planes[0] = 0
    last = lax.fori_loop(0, PLANES, list_plane, 1)
    rounds = last // 2
    starts[last] = EDGES
    planes[last] = 0

    recv, step, axis = recv_ref[...], *steps_of(send_ref[...], recv_ref[...])
    code = recv * 8 + jnp.where(step < 0, 4, 0) + axis
    code_row[0:96, :] = code
    code_row[96:, :] = jnp.full((code_row.shape[0] - 96, 128), -8, jnp.int32)
    w1a = w1e_ref[0:H, :]
    w1b = w1e_ref[H : 2 * H, :]
    w1c = w1e_ref[2 * H :, :]
    diag_w1[...] = block_diagonal(w1a)
    diag_w2t[...] = block_diagonal(w2e_ref[...].T)
    diag_w1t[...] = block_diagonal(w1a.T)
    b1e = b1e_ref[...]

    proj_face[...] = dot(face_ref[...], w1b)
    proj[0:ROWS, :] = proj_face[X_LOW : X_LOW + ROWS, :]
    proj[ROWS * (PLANES + 1) :, :] = proj_face[X_HIGH : X_HIGH + ROWS, :]
    wide[...] = jnp.zeros((2 * ROWS, H), F32)
    w1bc = jnp.concatenate([w1b, w1c], axis=1)

    def project(k, carry):
        rows = pl.ds(pl.multiple_of(k * CHUNK, CHUNK), CHUNK)
        both = dot(node_ref[rows, :], w1bc)
        proj[pl.ds(pl.multiple_of(k * CHUNK + ROWS, ROWS), CHUNK), :] = both[:, :H]
        proj_own[rows, :] = both[:, H:] + b1e
        gathered[rows, :] = jnp.zeros((CHUNK, 2 * H), F32)
        degree[rows, :] = jnp.zeros((CHUNK, H), F32)
        return carry

    lax.fori_loop(0, CELLS // CHUNK, project, 0)

    row_id = lax.broadcasted_iota(jnp.int32, (ROWS, H), 0)
    low_z = (row_id & 3) == 0
    high_z = (row_id & 3) == 3
    low_y = row_id < 4
    high_y = row_id >= 124

    def plane_rows(i):
        return pl.ds(pl.multiple_of(i * ROWS, ROWS), ROWS)

    def build_table(i, carry):
        own = proj_own[plane_rows(i), :]
        mine = proj[plane_rows(i + 1), :]
        above = proj[plane_rows(i + 2), :]
        below = proj[plane_rows(i), :]
        wide[0:4, :] = proj_face[pl.ds(Y_LOW + 4 * i, 4), :]
        wide[124:128, :] = proj_face[pl.ds(Y_HIGH + 4 * i, 4), :]
        wide[pl.ds(ROWS, 32, stride=4), :] = proj_face[pl.ds(Z_LOW + 32 * i, 32), :]
        wide[pl.ds(ROWS + 3, 32, stride=4), :] = proj_face[pl.ds(Z_HIGH + 32 * i, 32), :]
        side_y = wide[:ROWS, :]
        side_z = wide[ROWS:, :]
        up_y = jnp.where(high_y, side_y, pltpu.roll(mine, 124, 0))
        down_y = jnp.where(low_y, side_y, pltpu.roll(mine, 4, 0))
        up_z = jnp.where(high_z, side_z, pltpu.roll(mine, 127, 0))
        down_z = jnp.where(low_z, side_z, pltpu.roll(mine, 1, 0))
        tables[i, 0:ROWS, :] = jnp.concatenate(
            [above + own, up_y + own, up_z + own], axis=1
        ).astype(BF16)
        tables[i, ROWS : 2 * ROWS, :] = jnp.concatenate(
            [below + own, down_y + own, down_z + own], axis=1
        ).astype(BF16)
        return carry

    lax.fori_loop(0, PLANES, build_table, 0)

    def tile_at(j):
        start = pl.multiple_of(starts[j], 16)
        return start, pl.ds(start, TILE), planes[j]

    lane = lax.broadcasted_iota(jnp.int32, (1, 128), 1).astype(F32)
    lane_low, lane_high = lane.astype(BF16), (lane + 128.0).astype(BF16)

    one, zero = jnp.ones((TILE, 128), BF16), jnp.zeros((TILE, 128), BF16)

    def kinds(i, count):
        first = jnp.full((1, 128), 4 * i, jnp.int32).astype(F32)
        return [first + float(k) for k in range(count)]

    def head_inside(start, i):
        kind = kind_col[pl.ds(start, 16), :].astype(F32)
        low, _, high = kinds(i, 3)
        return (kind >= low) & (kind <= high)

    def row_codes(start):
        q = start >> 7
        off = start & 127
        turn = (128 - off) & 127
        here = pltpu.roll(code_row[pl.ds(q, 8), :], turn, 1)
        there = pltpu.roll(code_row[pl.ds(q + 1, 8), :], turn, 1)
        spot = lax.broadcasted_iota(jnp.int32, (8, 128), 1)
        return jnp.where(spot < 128 - off, here, there)

    def one_hot_turned(keys, slots):
        slot = lax.broadcasted_iota(jnp.int32, (slots, 128), 0)
        return [
            jnp.where(jnp.broadcast_to(keys[k : k + 1, :], (slots, 128)) == slot, 1.0, 0.0)
            for k in range(TILE // 128)
        ]

    def keep_head(ref, start, new, inside):
        old = ref[pl.ds(start, 16), :].astype(F32)
        return jnp.concatenate([jnp.where(inside, new[:16], old), new[16:]], axis=0)

    copies[0].wait()

    def forward_sums(j, z_buffer):
        start, span, i = tile_at(j)
        u, sp = slope_and_value(z_buffer[...])
        inside = head_inside(start, i)
        u = keep_head(value, start, u, inside).astype(BF16)
        value[span, :] = u
        slope[span, :] = keep_head(slope, start, sp, inside).astype(BF16)
        pieces = one_hot_turned((row_codes(start) >> 3) - 128 * i, ROWS)
        count = pieces[0]
        for piece in pieces[1:]:
            count = count + piece
        degree[plane_rows(i), :] += count
        spread = jnp.concatenate(pieces, axis=1).astype(BF16)
        gathered[plane_rows(i), :] += dot(spread, jnp.concatenate([edge[span, :], u], axis=1))

    def forward_values(j, z_buffer):
        start, span, i = tile_at(j)
        keys = key_col[span, :]
        hot = jnp.concatenate(
            [jnp.where(keys == lane_low, one, zero), jnp.where(keys == lane_high, one, zero)],
            axis=1,
        )
        picked = dot(hot, tables[i])
        kind = kind_col[span, :].astype(F32)
        first, second = kinds(i, 2)
        z_buffer[...] = pair_dot(edge[span, :], diag_w1[...]) + jnp.where(
            kind == first,
            picked[:, :H],
            jnp.where(kind == second, picked[:, H : 2 * H], picked[:, 2 * H :]),
        )

    def forward(m, carry):
        forward_values(2 * m + 1, z_a)
        forward_sums(2 * m, z_b)
        forward_values(2 * m + 2, z_b)
        forward_sums(2 * m + 1, z_a)
        return carry

    z_b[...] = jnp.zeros((TILE, H), F32)
    lax.fori_loop(0, rounds, forward, 0)
    forward_sums(2 * rounds, z_b)

    raw_ref[...] = jnp.zeros((RAW_ROWS, H), F32)
    w2nt = w2n_ref[...].T
    w1nt = w1n_ref[...].T

    def nodes(k, carry):
        rows = pl.ds(pl.multiple_of(k * CHUNK, CHUNK), CHUNK)
        packed = gathered[rows, :]
        count = jnp.sum(degree[rows, :], axis=1, keepdims=True)
        aggregate = (
            packed[:, :H]
            + dot(packed[:, H:].astype(BF16), w2e_ref[...])
            + count * b2e_ref[...]
        ).astype(BF16)
        x_node = jnp.concatenate([node_ref[rows, :], aggregate], axis=1)
        z_node = dot(x_node, w1n_ref[...]) + b1n_ref[...]
        u_node, sp_node = slope_and_value(z_node)
        cot_cells = cot_node_ref[rows, :]
        dz_node = (dot(cot_cells, w2nt) * sp_node).astype(BF16)
        dx_node = dot(dz_node, w1nt)
        base_ref[rows, :] = cot_cells.astype(F32) + dx_node[:, :H]
        gathered[rows, 0:H] = dx_node[:, H:]
        raw_ref[512:768, :] += dot_tn(x_node, dz_node)
        raw_ref[768:896, :] += dot_tn(u_node.astype(BF16), cot_cells)
        raw_ref[898:899, :] += jnp.sum(dz_node.astype(F32), axis=0, keepdims=True)
        raw_ref[899:900, :] += jnp.sum(cot_cells.astype(F32), axis=0, keepdims=True)
        return carry

    lax.fori_loop(0, CELLS // CHUNK, nodes, 0)
    copies[1].wait()

    def clear(i, carry):
        sums[i] = jnp.zeros((256, 3 * H), F32)
        return carry

    lax.fori_loop(0, PLANES + 2, clear, 0)
    ones = jnp.ones((16, TILE), BF16)

    def backward_sums(j, d_buffer):
        start, span, i = tile_at(j)
        dz_edge = d_buffer[:, :H]
        both = dot(
            jnp.concatenate([edge[span, :].T, value[span, :].T, ones], axis=0), d_buffer[...]
        )
        raw_ref[0:H, :] += both[:H, :H]
        raw_ref[384:512, :] += both[H : 2 * H, H:]
        raw_ref[897:898, :] += both[2 * H : 2 * H + 1, H:]
        codes = row_codes(start)
        keys = (codes >> 3) - 128 * i + ((codes >> 2) & 1) * 128
        keys = jnp.where((codes >> 10) == i, keys, -1)
        spread = jnp.concatenate(one_hot_turned(keys, 2 * ROWS), axis=1).astype(BF16)
        kind = kind_col[span, :]
        first, second = (number.astype(BF16) for number in kinds(i, 2))
        parted = jnp.concatenate(
            [
                jnp.where(kind == first, dz_edge, zero),
                jnp.where(kind == second, dz_edge, zero),
                dz_edge,
            ],
            axis=1,
        )
        sums[i + 1] += dot(spread, parted)

    def backward_values(j, d_buffer):
        start, span, i = tile_at(j)
        keys, kind = key_col[span, :], kind_col[span, :]
        hot = jnp.where((keys == lane_low) | (keys == lane_high), one, zero)
        added = pair_dot(hot, block_diagonal(gathered[plane_rows(i), 0:H].astype(BF16)))
        d_wide = cot[span, :].astype(F32) + added
        low, _, high = (number.astype(BF16) for number in kinds(i, 3))
        d_edge = jnp.where((kind >= low) & (kind <= high), d_wide.astype(BF16), zero)
        dz_edge = (pair_dot(d_edge, diag_w2t[...]) * slope[span, :].astype(F32)).astype(BF16)
        d_buffer[...] = jnp.concatenate([dz_edge, d_edge], axis=1)
        new = d_wide + pair_dot(dz_edge, diag_w1t[...])
        grad[span, :] = keep_head(grad, start, new, head_inside(start, i)).astype(BF16)

    def backward(m, carry):
        backward_values(2 * m + 1, d_a)
        backward_sums(2 * m, d_b)
        backward_values(2 * m + 2, d_b)
        backward_sums(2 * m + 1, d_a)
        return carry

    d_b[...] = jnp.zeros((TILE, 2 * H), BF16)
    lax.fori_loop(0, rounds, backward, 0)
    backward_sums(2 * rounds, d_b)
    grad_copy = pltpu.make_async_copy(grad.at[pl.ds(0, EDGES), :], grad_edge_hbm, sems.at[2])
    grad_copy.start()

    w1bt = w1e_ref[H : 2 * H, :].T
    w1ct = w1e_ref[2 * H :, :].T
    diag_w2t[:, 0:H] = jnp.concatenate([w1bt, w1ct], axis=0)

    def cells(i, carry):
        rows = plane_rows(i)
        here = sums[i + 1]
        third = here[:, 2 * H :] - here[:, :H] - here[:, H : 2 * H]
        arrived = here[:ROWS, 2 * H :] + here[ROWS:, 2 * H :]
        yp, ym = here[:ROWS, H : 2 * H], here[ROWS:, H : 2 * H]
        zp, zm = third[:ROWS], third[ROWS:]
        left = (
            sums[i, 0:ROWS, 0:H]
            + sums[i + 2, ROWS : 2 * ROWS, 0:H]
            + jnp.where(low_y, 0.0, pltpu.roll(yp, 4, 0))
            + jnp.where(high_y, 0.0, pltpu.roll(ym, 124, 0))
            + jnp.where(low_z, 0.0, pltpu.roll(zp, 1, 0))
            + jnp.where(high_z, 0.0, pltpu.roll(zm, 127, 0))
        ).astype(BF16)
        arrived_low = arrived.astype(BF16)
        leaving[pl.ds(Y_LOW + 4 * i, 4), :] = ym[:4]
        leaving[pl.ds(Y_HIGH + 4 * i, 4), :] = yp[124:]
        wide[0:ROWS, :] = zm
        wide[ROWS:, :] = zp
        leaving[pl.ds(Z_LOW + 32 * i, 32), :] = wide[pl.ds(0, 32, stride=4), :]
        leaving[pl.ds(Z_HIGH + 32 * i, 32), :] = wide[pl.ds(ROWS + 3, 32, stride=4), :]
        base_ref[rows, :] += dot(jnp.concatenate([left, arrived_low], axis=1), diag_w2t[:, 0:H])
        both = dot_tn(node_ref[rows, :], jnp.concatenate([left, arrived_low], axis=1))
        raw_ref[H : 2 * H, :] += both[:, :H]
        raw_ref[2 * H : 3 * H, :] += both[:, H:]
        raw_ref[896:897, :] += jnp.sum(arrived, axis=0, keepdims=True)
        return carry

    lax.fori_loop(0, PLANES, cells, 0)
    leaving[X_LOW : X_LOW + ROWS, :] = sums[1, ROWS : 2 * ROWS, 0:H]
    leaving[X_HIGH : X_HIGH + ROWS, :] = sums[PLANES, 0:ROWS, 0:H]
    gone = leaving[...].astype(BF16)
    out_ref[...] = dot(gone, w1bt).astype(BF16)
    raw_ref[H : 2 * H, :] += dot_tn(face_ref[...], gone)
    grad_copy.wait()


def local_terms(bounds, *operands):
    vmem = pl.BlockSpec(memory_space=pltpu.VMEM)
    anywhere = pl.BlockSpec(memory_space=pltpu.MemorySpace.HBM)
    return pl.pallas_call(
        local_kernel,
        out_shape=(
            jax.ShapeDtypeStruct((EDGES, H), BF16),
            jax.ShapeDtypeStruct((CELLS, H), F32),
            jax.ShapeDtypeStruct((FACES, H), BF16),
            jax.ShapeDtypeStruct((RAW_ROWS, H), F32),
        ),
        in_specs=[pl.BlockSpec(memory_space=pltpu.SMEM), vmem, vmem, anywhere, anywhere]
        + [vmem] * 12,
        out_specs=(anywhere, vmem, vmem, vmem),
        scratch_shapes=[pltpu.VMEM((PADDED, H), BF16)] * 5
        + [
            pltpu.VMEM((112, 128), jnp.int32),
            pltpu.VMEM((CELLS + 2 * ROWS, H), F32),
            pltpu.VMEM((CELLS, H), F32),
            pltpu.VMEM((FACES, H), F32),
            pltpu.VMEM((2 * ROWS, H), F32),
            pltpu.VMEM((FACES, H), F32),
            pltpu.VMEM((CELLS, 2 * H), F32),
            pltpu.VMEM((CELLS, H), F32),
            pltpu.VMEM((PLANES, 256, 3 * H), BF16),
            pltpu.VMEM((PLANES + 2, 256, 3 * H), F32),
            pltpu.VMEM((256, 256), BF16),
            pltpu.VMEM((256, 256), BF16),
            pltpu.VMEM((256, 256), BF16),
            pltpu.VMEM((TILE, H), F32),
            pltpu.VMEM((TILE, H), F32),
            pltpu.VMEM((TILE, 2 * H), BF16),
            pltpu.VMEM((TILE, 2 * H), BF16),
            pltpu.SMEM((48,), jnp.int32),
            pltpu.SMEM((48,), jnp.int32),
            pltpu.SemaphoreType.DMA((3,)),
        ],
        compiler_params=pltpu.CompilerParams(vmem_limit_bytes=LOCAL_VMEM),
        cost_estimate=pl.CostEstimate(
            flops=10_000_000_000, bytes_accessed=20_000_000, transcendentals=2_000_000
        ),
    )(bounds, *operands)


def place():
    return tuple(lax.axis_index(name) for name in ("gx", "gy", "gz"))


def sizes():
    return tuple(lax.axis_size(name) for name in ("gx", "gy", "gz"))


def across(side):
    dim, up = side // 2, side % 2
    here, count = place(), sizes()
    beyond = list(here)
    beyond[dim] = lax.rem(here[dim] + (1 if up else count[dim] - 1), count[dim])
    return tuple(beyond)


def face_copies(source, target, send_sems, recv_sems):
    copies = []
    for side, (first, rows) in enumerate(SPANS):
        opposite = SPANS[side ^ 1][0]
        copies.append(
            pltpu.make_async_remote_copy(
                src_ref=source.at[pl.ds(first, rows), :],
                dst_ref=target.at[pl.ds(opposite, rows), :],
                send_sem=send_sems.at[side],
                recv_sem=recv_sems.at[side],
                device_id=across(side),
                device_id_type=MESH,
            )
        )
    return copies


def halo_kernel(
    node_ref,
    send_ref,
    recv_ref,
    face_ref,
    bounds_ref,
    key_col,
    kind_col,
    cells,
    packed,
    send_sems,
    recv_sems,
):
    barrier = pltpu.get_barrier_semaphore()
    for side in range(6):
        pl.semaphore_signal(barrier, inc=1, device_id=across(side), device_id_type=MESH)
    cells[...] = node_ref[...].astype(F32)
    packed[X_LOW : X_LOW + ROWS, :] = node_ref[0:ROWS, :]
    packed[X_HIGH : X_HIGH + ROWS, :] = node_ref[CELLS - ROWS :, :]
    for first, at in ((Y_LOW, 0), (Y_HIGH, 124)):
        strips = [cells[ROWS * i + at : ROWS * i + at + 4, :] for i in range(PLANES)]
        packed[first : first + 64, :] = jnp.concatenate(strips, axis=0).astype(BF16)
    packed[Z_LOW : Z_LOW + 512, :] = cells[pl.ds(0, 512, stride=4), :].astype(BF16)
    packed[Z_HIGH : Z_HIGH + 512, :] = cells[pl.ds(3, 512, stride=4), :].astype(BF16)
    pl.semaphore_wait(barrier, 6)
    copies = face_copies(packed, face_ref, send_sems, recv_sems)
    for side in (5, 4, 1, 0, 3, 2):
        copies[side].start()
    recv = recv_ref[...]
    for i in range(PLANES + 1):
        below = jnp.where(recv < ROWS * i, 1.0, 0.0)
        bounds_ref[i] = jnp.sum(below).astype(jnp.int32)
    step, axis = steps_of(send_ref[...], recv)
    columns = (key_col, kind_col)
    zero = jnp.zeros((32, 128), F32)
    turned = jnp.concatenate(
        [
            jnp.concatenate([numbers.astype(F32), zero], axis=0).T
            for numbers in ((recv & 127) + jnp.where(step < 0, 128, 0), (recv >> 7) * 4 + axis)
        ],
        axis=0,
    ).astype(BF16)
    row = lax.broadcasted_iota(jnp.int32, (128, 256), 0)
    lane = lax.broadcasted_iota(jnp.int32, (128, 256), 1)
    for k in range(0, 96, 2):
        pick = jnp.where(row - (lane >> 7) == k, 1.0, 0.0).astype(BF16)
        both = dot(turned, pick).astype(BF16)
        for c, column in enumerate(columns):
            block = both[128 * c : 128 * c + 128]
            column[k * 128 : (k + 1) * 128, :] = block[:, :128]
            column[(k + 1) * 128 : (k + 2) * 128, :] = block[:, 128:]
    for column in columns:
        column[EDGES:, :] = jnp.full((TILE, 128), -4.0, BF16)
    for item in copies:
        item.wait()


def halo(node, send, recv):
    vmem = pl.BlockSpec(memory_space=pltpu.VMEM)
    return pl.pallas_call(
        halo_kernel,
        out_shape=(
            jax.ShapeDtypeStruct((FACES, H), BF16),
            jax.ShapeDtypeStruct((PLANES + 1,), jnp.int32),
        )
        + (pltpu.VMEM((PADDED, 128), BF16),) * 2,
        in_specs=[vmem] * 3,
        out_specs=(vmem, pl.BlockSpec(memory_space=pltpu.SMEM)) + (vmem,) * 2,
        scratch_shapes=[
            pltpu.VMEM((CELLS, H), F32),
            pltpu.VMEM((FACES, H), BF16),
            pltpu.SemaphoreType.DMA((6,)),
            pltpu.SemaphoreType.DMA((6,)),
        ],
        compiler_params=pltpu.CompilerParams(
            collective_id=0, has_side_effects=True, vmem_limit_bytes=12 * 1024 * 1024
        ),
    )(node, send, recv)


def finish_kernel(
    base_ref,
    out_ref,
    raw_ref,
    grad_ref,
    total_ref,
    faces,
    cells,
    partner_part,
    half,
    parts,
    mine,
    full,
    send_sems,
    recv_sems,
    pair_send,
    pair_recv,
    all_send,
    all_recv,
):
    (ga, gb, gc), (na, nb, nc) = place(), sizes()
    nz = nc // 2
    chips = na * nb * nz
    chip_z, core = lax.div(gc, 2), lax.rem(gc, 2)
    chip = (ga * nb + gb) * nz + chip_z
    partner = (ga, gb, 2 * chip_z + 1 - core)

    def peer(d):
        da, rest = lax.div(d, nb * nz), lax.rem(d, nb * nz)
        db, dz = lax.div(rest, nz), lax.rem(rest, nz)
        pa, pb = lax.rem(ga + da, na), lax.rem(gb + db, nb)
        pz = lax.rem(chip_z + dz, nz)
        return (pa, pb, 2 * pz + core), (pa * nb + pb) * nz + pz

    barrier = pltpu.get_barrier_semaphore()

    def greet(d, carry):
        pl.semaphore_signal(barrier, inc=1, device_id=peer(d)[0], device_id_type=MESH)
        return carry

    pl.semaphore_signal(barrier, inc=1, device_id=partner, device_id_type=MESH)
    lax.fori_loop(1, chips, greet, 0)
    for side in (4, 5):
        pl.semaphore_signal(barrier, inc=1, device_id=across(side), device_id_type=MESH)
    pl.semaphore_wait(barrier, chips + 2)

    def to_partner(source, target, k):
        return pltpu.make_async_remote_copy(
            src_ref=source,
            dst_ref=target,
            send_sem=pair_send.at[k],
            recv_sem=pair_recv.at[k],
            device_id=partner,
            device_id_type=MESH,
        )

    first = to_partner(raw_ref.at[pl.ds((1 - core) * chips, chips)], partner_part, 0)
    first.start()
    halos = face_copies(out_ref, faces, send_sems, recv_sems)
    for side in (0, 1, 2, 3):
        halos[side].start()
    first.wait()
    half[...] = raw_ref[pl.ds(core * chips, chips)] + partner_part[...]

    def scatter(d, carry):
        where, other = peer(d)
        pltpu.make_async_remote_copy(
            src_ref=half.at[other],
            dst_ref=parts.at[chip],
            send_sem=all_send.at[0],
            recv_sem=all_recv.at[0],
            device_id=where,
            device_id_type=MESH,
        ).start()
        return carry

    lax.fori_loop(1, chips, scatter, 0)
    for side in (4, 5):
        halos[side].start()
    parts[chip] = half[chip]

    def settle(buffer, sem):
        span = buffer.at[pl.ds(0, chips - 1)]
        pltpu.make_async_copy(span, span, sem).wait()

    settle(parts, all_recv.at[0])
    mine[...] = jnp.sum(parts[...], axis=0)

    def gather(d, carry):
        where, _ = peer(d)
        pltpu.make_async_remote_copy(
            src_ref=mine,
            dst_ref=full.at[core * chips + chip],
            send_sem=all_send.at[1],
            recv_sem=all_recv.at[1],
            device_id=where,
            device_id_type=MESH,
        ).start()
        return carry

    lax.fori_loop(1, chips, gather, 0)
    full[core * chips + chip] = mine[...]
    for item in halos:
        item.wait()
    cells[...] = base_ref[...]
    cells[0:ROWS, :] += faces[X_LOW : X_LOW + ROWS, :].astype(F32)
    cells[CELLS - ROWS :, :] += faces[X_HIGH : X_HIGH + ROWS, :].astype(F32)
    for start, at in ((Y_LOW, 0), (Y_HIGH, 124)):
        strip = faces[start : start + 64, :].astype(F32)
        for i in range(PLANES):
            cells[ROWS * i + at : ROWS * i + at + 4, :] += strip[4 * i : 4 * i + 4]
    cells[pl.ds(0, 512, stride=4), :] += faces[Z_LOW : Z_LOW + 512, :].astype(F32)
    cells[pl.ds(3, 512, stride=4), :] += faces[Z_HIGH : Z_HIGH + 512, :].astype(F32)
    grad_ref[...] = cells[...].astype(BF16)
    settle(full, all_recv.at[1])
    held = pl.ds(core * chips, chips)
    last = to_partner(full.at[held], full.at[held], 1)
    last.start()
    settle(half, all_send.at[0])
    settle(half, all_send.at[1])
    last.wait()
    total_ref[...] = full[...]


def write_kernel(grad_ref, total_ref, *refs):
    outs, scaled, sems = refs[:6], refs[6], refs[7]
    first = pltpu.make_async_copy(grad_ref, outs[0], sems.at[0])
    first.start()
    total = total_ref[...]
    squares = jnp.sum(total * total, axis=0, keepdims=True)
    squares = jnp.sum(squares, axis=1, keepdims=True)
    factor = 1.0 / jnp.maximum(1.0, jnp.sqrt(squares / (7 * H * H + 4 * H)))
    scaled[...] = total * factor
    copies = [first]
    at = 0
    for k, rows in enumerate((384, 128, 256, 128, 4)):
        copies.append(
            pltpu.make_async_copy(scaled.at[pl.ds(at, rows), :], outs[k + 1], sems.at[k + 1])
        )
        copies[-1].start()
        at += rows
    for item in copies:
        item.wait()


def write(grad, total):
    vmem = pl.BlockSpec(memory_space=pltpu.VMEM)
    return pl.pallas_call(
        write_kernel,
        out_shape=(jax.ShapeDtypeStruct((CELLS, H), BF16),)
        + tuple(jax.ShapeDtypeStruct((rows, H), F32) for rows in (384, 128, 256, 128, 4)),
        in_specs=[vmem] * 2,
        out_specs=(pl.BlockSpec(memory_space=pl.ANY),) * 6,
        scratch_shapes=[pltpu.VMEM((RAW_ROWS, H), F32), pltpu.SemaphoreType.DMA((6,))],
        compiler_params=pltpu.CompilerParams(vmem_limit_bytes=48 * 1024 * 1024),
    )(grad, total)


def finish(base, out, raw):
    chips = lax.axis_size("gx") * lax.axis_size("gy") * lax.axis_size("gz") // 2
    block = RAW_ROWS // (2 * chips)
    vmem = pl.BlockSpec(memory_space=pltpu.VMEM)
    grad, total = pl.pallas_call(
        finish_kernel,
        out_shape=(
            jax.ShapeDtypeStruct((CELLS, H), BF16),
            jax.ShapeDtypeStruct((2 * chips, block, H), F32),
        ),
        in_specs=[vmem] * 3,
        out_specs=(vmem,) * 2,
        scratch_shapes=[
            pltpu.VMEM((FACES, H), BF16),
            pltpu.VMEM((CELLS, H), F32),
            pltpu.VMEM((chips, block, H), F32),
            pltpu.VMEM((chips, block, H), F32),
            pltpu.VMEM((chips, block, H), F32),
            pltpu.VMEM((block, H), F32),
            pltpu.VMEM((2 * chips, block, H), F32),
            pltpu.SemaphoreType.DMA((6,)),
            pltpu.SemaphoreType.DMA((6,)),
            pltpu.SemaphoreType.DMA((2,)),
            pltpu.SemaphoreType.DMA((2,)),
            pltpu.SemaphoreType.DMA((2,)),
            pltpu.SemaphoreType.DMA((2,)),
        ],
        compiler_params=pltpu.CompilerParams(
            collective_id=1, has_side_effects=True, vmem_limit_bytes=24 * 1024 * 1024
        ),
    )(base, out, raw.reshape(2 * chips, block, H))
    return write(grad, total.reshape(RAW_ROWS, H))


def on_device(
    node_latent,
    edge_latent,
    senders,
    receivers,
    w1_edge,
    b1_edge,
    w2_edge,
    b2_edge,
    w1_node,
    b1_node,
    w2_node,
    cot_node,
    cot_edge,
):
    cells = node_latent.reshape(CELLS, H)
    receiver_ids = receivers.reshape(96, 128)
    sender_ids = senders.reshape(96, 128)
    faces, bounds, *columns = halo(cells, sender_ids, receiver_ids)
    grad_edge, base, out, raw = local_terms(
        bounds,
        sender_ids,
        receiver_ids,
        pltpu.with_memory_space_constraint(edge_latent.reshape(EDGES, H), pltpu.MemorySpace.HBM),
        pltpu.with_memory_space_constraint(cot_edge.reshape(EDGES, H), pltpu.MemorySpace.HBM),
        cells,
        cot_node.reshape(CELLS, H),
        faces,
        *columns,
        w1_edge,
        b1_edge.reshape(1, H),
        w2_edge,
        b2_edge.reshape(1, H),
        w1_node,
        b1_node.reshape(1, H),
        w2_node,
    )
    grad_node, *grads = finish(base, out, raw)
    return (grad_node.reshape(node_latent.shape), grad_edge.reshape(edge_latent.shape), *grads)


def solution(mesh):
    cell = P("gx", "gy", "gz", None)
    slots = P("gx", "gy", "gz", None, None)
    placed = (cell, slots, cell, cell, P(), P(), P(), P(), P(), P(), P(), cell, slots)
    return jax.shard_map(
        on_device,
        mesh=mesh,
        in_specs=placed,
        out_specs=(cell, slots, P(), P(), P(), P(), P()),
        check_vma=False,
    )
```

```python
import functools

import jax
import jax.numpy as jnp
from jax import lax
from jax.experimental import pallas as pl
from jax.experimental.pallas import tpu as pltpu
from jax.sharding import PartitionSpec as P

H = 128
PLANES = 16
ROWS = 128
CELLS = PLANES * ROWS
EDGES = 12288
TILE = 896
LOCAL_VMEM = 37 * 1024 * 1024
PADDED = EDGES + TILE
CHUNK = 512
RAW_ROWS = 1024
X_LOW, X_HIGH, Y_LOW, Y_HIGH, Z_LOW, Z_HIGH, FACES = 0, 128, 256, 320, 384, 896, 1408
SPANS = ((X_LOW, 128), (X_HIGH, 128), (Y_LOW, 64), (Y_HIGH, 64), (Z_LOW, 512), (Z_HIGH, 512))
MESH = pl.DeviceIdType.MESH

F32 = jnp.float32
BF16 = jnp.bfloat16


def dot(a, b):
    return jnp.dot(a, b, preferred_element_type=F32)


def dot_tn(a, b):
    return lax.dot_general(a, b, (((0,), (0,)), ((), ())), preferred_element_type=F32)


def pair_dot(rows, diagonal):
    half = rows.shape[0] // 2
    both = dot(jnp.concatenate([rows[:half], rows[half:]], axis=1), diagonal)
    return jnp.concatenate([both[:, :H], both[:, H:]], axis=0)


def block_diagonal(w):
    zero = jnp.zeros_like(w)
    return jnp.concatenate(
        [jnp.concatenate([w, zero], axis=1), jnp.concatenate([zero, w], axis=1)], axis=0
    )


def slope_and_value(z):
    sigma = 0.5 * jnp.tanh(0.5 * z) + 0.5
    value = z * sigma
    return value, sigma * (1.0 + (z - value))


def steps_of(send, recv):
    step = send - (((recv >> 7) + 1) * 204 + (((recv >> 2) & 31) + 1) * 6 + (recv & 3) + 1)
    size = jnp.abs(step)
    return step, jnp.where(size == 204, 0, jnp.where(size == 6, 1, 2))


def local_kernel(
    bounds,
    face_ref,
    key_col,
    kind_col,
    edge_hbm,
    cot_edge_hbm,
    *refs,
):
    small_hbm, refs = refs[:11], refs[11:]
    (
        grad_edge_hbm,
        base_ref,
        raw_ref,
        sums,
        edge,
        cot,
        value,
        slope,
        grad,
        code_row,
        proj,
        proj_own,
        proj_face,
        wide,
        gathered,
        degree,
        tables,
        diag_w1,
        diag_w2t,
        diag_w1t,
        z_a,
        z_b,
        d_a,
        d_b,
        starts,
        planes,
        sems,
        small_sems,
    ) = refs[:28]
    small = refs[28:]
    (
        recv_ref,
        send_ref,
        w1e_ref,
        b1e_ref,
        w2e_ref,
        node_ref,
        cot_node_ref,
        b2e_ref,
        w1n_ref,
        b1n_ref,
        w2n_ref,
    ) = small
    small_copies = [
        pltpu.make_async_copy(source, target, small_sems.at[k])
        for k, (source, target) in enumerate(zip(small_hbm, small))
    ]
    copies = [
        pltpu.make_async_copy(edge_hbm, edge.at[pl.ds(0, EDGES), :], sems.at[0]),
        pltpu.make_async_copy(cot_edge_hbm, cot.at[pl.ds(0, EDGES), :], sems.at[1]),
    ]
    for item in small_copies[:6] + copies[:1] + small_copies[6:] + copies[1:]:
        item.start()

    tail = jnp.zeros((TILE, H), BF16)
    for ref in (edge, cot, value, slope):
        ref[EDGES:, :] = tail

    def list_plane(i, n):
        lo, hi = bounds[i], bounds[i + 1]
        first = (lo >> 4) << 4
        count = jnp.where(hi > lo, (hi - first + (TILE - 1)) // TILE, 0)

        def put(t, n):
            starts[n] = first + t * TILE
            planes[n] = i
            return n + 1

        return lax.fori_loop(0, count, put, n)

    starts[0] = EDGES
    planes[0] = 0
    last = lax.fori_loop(0, PLANES, list_plane, 1)
    rounds = last // 2
    starts[last] = EDGES
    planes[last] = 0

    for item in small_copies[:6]:
        item.wait()
    recv, step, axis = recv_ref[...], *steps_of(send_ref[...], recv_ref[...])
    code = recv * 8 + jnp.where(step < 0, 4, 0) + axis
    code_row[0:96, :] = code
    code_row[96:, :] = jnp.full((code_row.shape[0] - 96, 128), -8, jnp.int32)
    w1a = w1e_ref[0:H, :]
    w1b = w1e_ref[H : 2 * H, :]
    w1c = w1e_ref[2 * H :, :]
    diag_w1[...] = block_diagonal(w1a)
    diag_w2t[...] = block_diagonal(w2e_ref[...].T)
    diag_w1t[...] = block_diagonal(w1a.T)
    b1e = b1e_ref[...]

    proj_face[...] = dot(face_ref[...], w1b)
    proj[0:ROWS, :] = proj_face[X_LOW : X_LOW + ROWS, :]
    proj[ROWS * (PLANES + 1) :, :] = proj_face[X_HIGH : X_HIGH + ROWS, :]
    wide[...] = jnp.zeros((2 * ROWS, H), F32)
    w1bc = jnp.concatenate([w1b, w1c], axis=1)

    def project(k, carry):
        rows = pl.ds(pl.multiple_of(k * CHUNK, CHUNK), CHUNK)
        both = dot(node_ref[rows, :], w1bc)
        proj[pl.ds(pl.multiple_of(k * CHUNK + ROWS, ROWS), CHUNK), :] = both[:, :H]
        proj_own[rows, :] = both[:, H:] + b1e
        gathered[rows, :] = jnp.zeros((CHUNK, 2 * H), F32)
        degree[rows, :] = jnp.zeros((CHUNK, H), F32)
        return carry

    lax.fori_loop(0, CELLS // CHUNK, project, 0)

    row_id = lax.broadcasted_iota(jnp.int32, (ROWS, H), 0)
    low_z = (row_id & 3) == 0
    high_z = (row_id & 3) == 3
    low_y = row_id < 4
    high_y = row_id >= 124

    def plane_rows(i):
        return pl.ds(pl.multiple_of(i * ROWS, ROWS), ROWS)

    def build_table(i, carry):
        own = proj_own[plane_rows(i), :]
        mine = proj[plane_rows(i + 1), :]
        above = proj[plane_rows(i + 2), :]
        below = proj[plane_rows(i), :]
        wide[0:4, :] = proj_face[pl.ds(Y_LOW + 4 * i, 4), :]
        wide[124:128, :] = proj_face[pl.ds(Y_HIGH + 4 * i, 4), :]
        wide[pl.ds(ROWS, 32, stride=4), :] = proj_face[pl.ds(Z_LOW + 32 * i, 32), :]
        wide[pl.ds(ROWS + 3, 32, stride=4), :] = proj_face[pl.ds(Z_HIGH + 32 * i, 32), :]
        side_y = wide[:ROWS, :]
        side_z = wide[ROWS:, :]
        up_y = jnp.where(high_y, side_y, pltpu.roll(mine, 124, 0))
        down_y = jnp.where(low_y, side_y, pltpu.roll(mine, 4, 0))
        up_z = jnp.where(high_z, side_z, pltpu.roll(mine, 127, 0))
        down_z = jnp.where(low_z, side_z, pltpu.roll(mine, 1, 0))
        tables[i, 0:ROWS, :] = jnp.concatenate(
            [above + own, up_y + own, up_z + own], axis=1
        ).astype(BF16)
        tables[i, ROWS : 2 * ROWS, :] = jnp.concatenate(
            [below + own, down_y + own, down_z + own], axis=1
        ).astype(BF16)
        return carry

    lax.fori_loop(0, PLANES, build_table, 0)

    def tile_at(j):
        start = pl.multiple_of(starts[j], 16)
        return start, pl.ds(start, TILE), planes[j]

    lane = lax.broadcasted_iota(jnp.int32, (1, 128), 1).astype(F32)
    lane_low, lane_high = lane.astype(BF16), (lane + 128.0).astype(BF16)

    one, zero = jnp.ones((TILE, 128), BF16), jnp.zeros((TILE, 128), BF16)

    def kinds(i, count):
        first = jnp.full((1, 128), 4 * i, jnp.int32).astype(F32)
        return [first + float(k) for k in range(count)]

    def head_inside(start, i):
        kind = kind_col[pl.ds(start, 16), :].astype(F32)
        low, _, high = kinds(i, 3)
        return (kind >= low) & (kind <= high)

    def row_codes(start):
        q = start >> 7
        off = start & 127
        turn = (128 - off) & 127
        here = pltpu.roll(code_row[pl.ds(q, 8), :], turn, 1)
        there = pltpu.roll(code_row[pl.ds(q + 1, 8), :], turn, 1)
        spot = lax.broadcasted_iota(jnp.int32, (8, 128), 1)
        return jnp.where(spot < 128 - off, here, there)

    def one_hot_turned(keys, slots):
        slot = lax.broadcasted_iota(jnp.int32, (slots, 128), 0)
        return [
            jnp.where(jnp.broadcast_to(keys[k : k + 1, :], (slots, 128)) == slot, 1.0, 0.0)
            for k in range(TILE // 128)
        ]

    def keep_head(ref, start, new, inside):
        old = ref[pl.ds(start, 16), :].astype(F32)
        return jnp.concatenate([jnp.where(inside, new[:16], old), new[16:]], axis=0)

    copies[0].wait()

    def forward_sums(j, z_buffer):
        start, span, i = tile_at(j)
        u, sp = slope_and_value(z_buffer[...])
        inside = head_inside(start, i)
        u = keep_head(value, start, u, inside).astype(BF16)
        value[span, :] = u
        slope[span, :] = keep_head(slope, start, sp, inside).astype(BF16)
        pieces = one_hot_turned((row_codes(start) >> 3) - 128 * i, ROWS)
        count = pieces[0]
        for piece in pieces[1:]:
            count = count + piece
        degree[plane_rows(i), :] += count
        spread = jnp.concatenate(pieces, axis=1).astype(BF16)
        gathered[plane_rows(i), :] += dot(spread, jnp.concatenate([edge[span, :], u], axis=1))

    def forward_values(j, z_buffer):
        start, span, i = tile_at(j)
        keys = key_col[span, :]
        hot = jnp.concatenate(
            [jnp.where(keys == lane_low, one, zero), jnp.where(keys == lane_high, one, zero)],
            axis=1,
        )
        picked = dot(hot, tables[i])
        kind = kind_col[span, :].astype(F32)
        first, second = kinds(i, 2)
        z_buffer[...] = pair_dot(edge[span, :], diag_w1[...]) + jnp.where(
            kind == first,
            picked[:, :H],
            jnp.where(kind == second, picked[:, H : 2 * H], picked[:, 2 * H :]),
        )

    def forward(m, carry):
        forward_values(2 * m + 1, z_a)
        forward_sums(2 * m, z_b)
        forward_values(2 * m + 2, z_b)
        forward_sums(2 * m + 1, z_a)
        return carry

    z_b[...] = jnp.zeros((TILE, H), F32)
    lax.fori_loop(0, rounds, forward, 0)
    forward_sums(2 * rounds, z_b)

    for item in small_copies[6:]:
        item.wait()
    raw_ref[...] = jnp.zeros((RAW_ROWS, H), F32)
    w2nt = w2n_ref[...].T
    w1nt = w1n_ref[...].T

    def nodes(k, carry):
        rows = pl.ds(pl.multiple_of(k * CHUNK, CHUNK), CHUNK)
        packed = gathered[rows, :]
        count = jnp.sum(degree[rows, :], axis=1, keepdims=True)
        aggregate = (
            packed[:, :H]
            + dot(packed[:, H:].astype(BF16), w2e_ref[...])
            + count * b2e_ref[...]
        ).astype(BF16)
        x_node = jnp.concatenate([node_ref[rows, :], aggregate], axis=1)
        z_node = dot(x_node, w1n_ref[...]) + b1n_ref[...]
        u_node, sp_node = slope_and_value(z_node)
        cot_cells = cot_node_ref[rows, :]
        dz_node = (dot(cot_cells, w2nt) * sp_node).astype(BF16)
        dx_node = dot(dz_node, w1nt)
        base_ref[rows, :] = cot_cells.astype(F32) + dx_node[:, :H]
        gathered[rows, 0:H] = dx_node[:, H:]
        raw_ref[512:768, :] += dot_tn(x_node, dz_node)
        raw_ref[768:896, :] += dot_tn(u_node.astype(BF16), cot_cells)
        raw_ref[898:899, :] += jnp.sum(dz_node.astype(F32), axis=0, keepdims=True)
        raw_ref[899:900, :] += jnp.sum(cot_cells.astype(F32), axis=0, keepdims=True)
        return carry

    lax.fori_loop(0, CELLS // CHUNK, nodes, 0)
    copies[1].wait()

    def clear(i, carry):
        sums[i] = jnp.zeros((256, 3 * H), F32)
        return carry

    lax.fori_loop(0, PLANES + 2, clear, 0)
    ones = jnp.ones((16, TILE), BF16)

    def backward_sums(j, d_buffer):
        start, span, i = tile_at(j)
        dz_edge = d_buffer[:, :H]
        both = dot(
            jnp.concatenate([edge[span, :].T, value[span, :].T, ones], axis=0), d_buffer[...]
        )
        raw_ref[0:H, :] += both[:H, :H]
        raw_ref[384:512, :] += both[H : 2 * H, H:]
        raw_ref[897:898, :] += both[2 * H : 2 * H + 1, H:]
        codes = row_codes(start)
        keys = (codes >> 3) - 128 * i + ((codes >> 2) & 1) * 128
        keys = jnp.where((codes >> 10) == i, keys, -1)
        spread = jnp.concatenate(one_hot_turned(keys, 2 * ROWS), axis=1).astype(BF16)
        kind = kind_col[span, :]
        first, second = (number.astype(BF16) for number in kinds(i, 2))
        parted = jnp.concatenate(
            [
                jnp.where(kind == first, dz_edge, zero),
                jnp.where(kind == second, dz_edge, zero),
                dz_edge,
            ],
            axis=1,
        )
        sums[i + 1] += dot(spread, parted)

    def backward_values(j, d_buffer):
        start, span, i = tile_at(j)
        keys, kind = key_col[span, :], kind_col[span, :]
        hot = jnp.where((keys == lane_low) | (keys == lane_high), one, zero)
        added = pair_dot(hot, block_diagonal(gathered[plane_rows(i), 0:H].astype(BF16)))
        d_wide = cot[span, :].astype(F32) + added
        low, _, high = (number.astype(BF16) for number in kinds(i, 3))
        d_edge = jnp.where((kind >= low) & (kind <= high), d_wide.astype(BF16), zero)
        dz_edge = (pair_dot(d_edge, diag_w2t[...]) * slope[span, :].astype(F32)).astype(BF16)
        d_buffer[...] = jnp.concatenate([dz_edge, d_edge], axis=1)
        new = d_wide + pair_dot(dz_edge, diag_w1t[...])
        grad[span, :] = keep_head(grad, start, new, head_inside(start, i)).astype(BF16)

    def backward(m, carry):
        backward_values(2 * m + 1, d_a)
        backward_sums(2 * m, d_b)
        backward_values(2 * m + 2, d_b)
        backward_sums(2 * m + 1, d_a)
        return carry

    d_b[...] = jnp.zeros((TILE, 2 * H), BF16)
    lax.fori_loop(0, rounds, backward, 0)
    backward_sums(2 * rounds, d_b)
    grad_copy = pltpu.make_async_copy(grad.at[pl.ds(0, EDGES), :], grad_edge_hbm, sems.at[2])
    grad_copy.start()

    grad_copy.wait()


def local_terms(bounds, faces, columns, edge_rows, cot_rows, small):
    vmem = pl.BlockSpec(memory_space=pltpu.VMEM)
    hbm = pl.BlockSpec(memory_space=pltpu.MemorySpace.HBM)
    return pl.pallas_call(
        local_kernel,
        out_shape=(
            jax.ShapeDtypeStruct((EDGES, H), BF16),
            pltpu.VMEM((CELLS, H), F32),
            pltpu.VMEM((RAW_ROWS, H), F32),
            pltpu.VMEM((PLANES + 2, 256, 3 * H), F32),
        ),
        in_specs=[pl.BlockSpec(memory_space=pltpu.SMEM)] + [vmem] * 3 + [hbm] * 13,
        out_specs=(hbm, vmem, vmem, vmem),
        scratch_shapes=[pltpu.VMEM((PADDED, H), BF16)] * 5
        + [
            pltpu.VMEM((112, 128), jnp.int32),
            pltpu.VMEM((CELLS + 2 * ROWS, H), F32),
            pltpu.VMEM((CELLS, H), F32),
            pltpu.VMEM((FACES, H), F32),
            pltpu.VMEM((2 * ROWS, H), F32),
            pltpu.VMEM((CELLS, 2 * H), F32),
            pltpu.VMEM((CELLS, H), F32),
            pltpu.VMEM((PLANES, 256, 3 * H), BF16),
            pltpu.VMEM((256, 256), BF16),
            pltpu.VMEM((256, 256), BF16),
            pltpu.VMEM((256, 256), BF16),
            pltpu.VMEM((TILE, H), F32),
            pltpu.VMEM((TILE, H), F32),
            pltpu.VMEM((TILE, 2 * H), BF16),
            pltpu.VMEM((TILE, 2 * H), BF16),
            pltpu.SMEM((48,), jnp.int32),
            pltpu.SMEM((48,), jnp.int32),
            pltpu.SemaphoreType.DMA((3,)),
            pltpu.SemaphoreType.DMA((11,)),
        ]
        + [pltpu.VMEM(item.shape, item.dtype) for item in small],
        compiler_params=pltpu.CompilerParams(vmem_limit_bytes=LOCAL_VMEM),
        cost_estimate=pl.CostEstimate(
            flops=10_000_000_000, bytes_accessed=20_000_000, transcendentals=2_000_000
        ),
    )(bounds, faces, *columns, edge_rows, cot_rows, *small)


def place():
    return tuple(lax.axis_index(name) for name in ("gx", "gy", "gz"))


def sizes():
    return tuple(lax.axis_size(name) for name in ("gx", "gy", "gz"))


def across(side):
    dim, up = side // 2, side % 2
    here, count = place(), sizes()
    beyond = list(here)
    beyond[dim] = lax.rem(here[dim] + (1 if up else count[dim] - 1), count[dim])
    return tuple(beyond)


def face_copies(source, target, send_sems, recv_sems):
    copies = []
    for side, (first, rows) in enumerate(SPANS):
        opposite = SPANS[side ^ 1][0]
        copies.append(
            pltpu.make_async_remote_copy(
                src_ref=source.at[pl.ds(first, rows), :],
                dst_ref=target.at[pl.ds(opposite, rows), :],
                send_sem=send_sems.at[side],
                recv_sem=recv_sems.at[side],
                device_id=across(side),
                device_id_type=MESH,
            )
        )
    return copies


def halo_kernel(
    node_hbm,
    send_hbm,
    recv_hbm,
    face_ref,
    bounds_ref,
    key_col,
    kind_col,
    node_ref,
    send_ref,
    recv_ref,
    cells,
    packed,
    load_sems,
    send_sems,
    recv_sems,
):
    loads = [
        pltpu.make_async_copy(source, target, load_sems.at[k])
        for k, (source, target) in enumerate(
            ((node_hbm, node_ref), (send_hbm, send_ref), (recv_hbm, recv_ref))
        )
    ]
    for item in loads:
        item.start()
    barrier = pltpu.get_barrier_semaphore()
    for side in range(6):
        pl.semaphore_signal(barrier, inc=1, device_id=across(side), device_id_type=MESH)
    for item in loads:
        item.wait()
    cells[...] = node_ref[...].astype(F32)
    packed[X_LOW : X_LOW + ROWS, :] = node_ref[0:ROWS, :]
    packed[X_HIGH : X_HIGH + ROWS, :] = node_ref[CELLS - ROWS :, :]
    for first, at in ((Y_LOW, 0), (Y_HIGH, 124)):
        strips = [cells[ROWS * i + at : ROWS * i + at + 4, :] for i in range(PLANES)]
        packed[first : first + 64, :] = jnp.concatenate(strips, axis=0).astype(BF16)
    packed[Z_LOW : Z_LOW + 512, :] = cells[pl.ds(0, 512, stride=4), :].astype(BF16)
    packed[Z_HIGH : Z_HIGH + 512, :] = cells[pl.ds(3, 512, stride=4), :].astype(BF16)
    pl.semaphore_wait(barrier, 6)
    copies = face_copies(packed, face_ref, send_sems, recv_sems)
    for side in (5, 4, 1, 0, 3, 2):
        copies[side].start()
    recv = recv_ref[...]
    for i in range(PLANES + 1):
        below = jnp.where(recv < ROWS * i, 1.0, 0.0)
        bounds_ref[i] = jnp.sum(below).astype(jnp.int32)
    step, axis = steps_of(send_ref[...], recv)
    columns = (key_col, kind_col)
    zero = jnp.zeros((32, 128), F32)
    turned = jnp.concatenate(
        [
            jnp.concatenate([numbers.astype(F32), zero], axis=0).T
            for numbers in ((recv & 127) + jnp.where(step < 0, 128, 0), (recv >> 7) * 4 + axis)
        ],
        axis=0,
    ).astype(BF16)
    row = lax.broadcasted_iota(jnp.int32, (128, 256), 0)
    lane = lax.broadcasted_iota(jnp.int32, (128, 256), 1)
    for k in range(0, 96, 2):
        pick = jnp.where(row - (lane >> 7) == k, 1.0, 0.0).astype(BF16)
        both = dot(turned, pick).astype(BF16)
        for c, column in enumerate(columns):
            block = both[128 * c : 128 * c + 128]
            column[k * 128 : (k + 1) * 128, :] = block[:, :128]
            column[(k + 1) * 128 : (k + 2) * 128, :] = block[:, 128:]
    for column in columns:
        column[EDGES:, :] = jnp.full((TILE, 128), -4.0, BF16)
    for item in copies:
        item.wait()


def halo(node, send, recv):
    vmem = pl.BlockSpec(memory_space=pltpu.VMEM)
    return pl.pallas_call(
        halo_kernel,
        out_shape=(
            pltpu.VMEM((FACES, H), BF16),
            jax.ShapeDtypeStruct((PLANES + 1,), jnp.int32),
        )
        + (pltpu.VMEM((PADDED, 128), BF16),) * 2,
        in_specs=[pl.BlockSpec(memory_space=pltpu.MemorySpace.HBM)] * 3,
        out_specs=(vmem, pl.BlockSpec(memory_space=pltpu.SMEM)) + (vmem,) * 2,
        scratch_shapes=[
            pltpu.VMEM((CELLS, H), BF16),
            pltpu.VMEM((96, 128), jnp.int32),
            pltpu.VMEM((96, 128), jnp.int32),
            pltpu.VMEM((CELLS, H), F32),
            pltpu.VMEM((FACES, H), BF16),
            pltpu.SemaphoreType.DMA((3,)),
            pltpu.SemaphoreType.DMA((6,)),
            pltpu.SemaphoreType.DMA((6,)),
        ],
        compiler_params=pltpu.CompilerParams(
            collective_id=0, has_side_effects=True, vmem_limit_bytes=12 * 1024 * 1024
        ),
    )(node, send, recv)


def finish_kernel(
    base_ref,
    raw_in,
    sums,
    face_ref,
    node_hbm,
    w1e_hbm,
    grad_ref,
    total_ref,
    node_ref,
    w1e_ref,
    raw_ref,
    edge_raw,
    leaving,
    wide,
    out_ref,
    faces,
    cells,
    partner_part,
    half,
    parts,
    mine,
    full,
    send_sems,
    recv_sems,
    pair_send,
    pair_recv,
    all_send,
    all_recv,
    load_sems,
):
    (ga, gb, gc), (na, nb, nc) = place(), sizes()
    nz = nc // 2
    chips = na * nb * nz
    chip_z, core = lax.div(gc, 2), lax.rem(gc, 2)
    chip = (ga * nb + gb) * nz + chip_z
    partner = (ga, gb, 2 * chip_z + 1 - core)

    def peer(d):
        da, rest = lax.div(d, nb * nz), lax.rem(d, nb * nz)
        db, dz = lax.div(rest, nz), lax.rem(rest, nz)
        pa, pb = lax.rem(ga + da, na), lax.rem(gb + db, nb)
        pz = lax.rem(chip_z + dz, nz)
        return (pa, pb, 2 * pz + core), (pa * nb + pb) * nz + pz

    barrier = pltpu.get_barrier_semaphore()

    def greet(d, carry):
        pl.semaphore_signal(barrier, inc=1, device_id=peer(d)[0], device_id_type=MESH)
        return carry

    pl.semaphore_signal(barrier, inc=1, device_id=partner, device_id_type=MESH)
    lax.fori_loop(1, chips, greet, 0)
    for side in (4, 5):
        pl.semaphore_signal(barrier, inc=1, device_id=across(side), device_id_type=MESH)

    loads = [
        pltpu.make_async_copy(node_hbm, node_ref, load_sems.at[0]),
        pltpu.make_async_copy(w1e_hbm, w1e_ref, load_sems.at[1]),
    ]
    for item in loads:
        item.start()
    raw_ref[...] = raw_in[...]
    edge_raw[...] = jnp.zeros_like(edge_raw)
    for item in loads:
        item.wait()

    w1bt = w1e_ref[H : 2 * H, :].T
    w1bct = jnp.concatenate([w1bt, w1e_ref[2 * H :, :].T], axis=0)
    row_id = lax.broadcasted_iota(jnp.int32, (ROWS, H), 0)
    low_z = lax.rem(row_id, 4) == 0
    high_z = lax.rem(row_id, 4) == 3
    low_y = row_id < 4
    high_y = row_id >= 124

    def collect(i, carry):
        rows = pl.ds(pl.multiple_of(i * ROWS, ROWS), ROWS)
        here = sums[i + 1]
        third = here[:, 2 * H :] - here[:, :H] - here[:, H : 2 * H]
        arrived = here[:ROWS, 2 * H :] + here[ROWS:, 2 * H :]
        yp, ym = here[:ROWS, H : 2 * H], here[ROWS:, H : 2 * H]
        zp, zm = third[:ROWS], third[ROWS:]
        left = (
            sums[i, 0:ROWS, 0:H]
            + sums[i + 2, ROWS : 2 * ROWS, 0:H]
            + jnp.where(low_y, 0.0, pltpu.roll(yp, 4, 0))
            + jnp.where(high_y, 0.0, pltpu.roll(ym, 124, 0))
            + jnp.where(low_z, 0.0, pltpu.roll(zp, 1, 0))
            + jnp.where(high_z, 0.0, pltpu.roll(zm, 127, 0))
        )
        moved = jnp.concatenate([left, arrived], axis=1).astype(BF16)
        leaving[pl.ds(Y_LOW + 4 * i, 4), :] = ym[:4]
        leaving[pl.ds(Y_HIGH + 4 * i, 4), :] = yp[124:]
        wide[0:ROWS, :] = zm
        wide[ROWS:, :] = zp
        leaving[pl.ds(Z_LOW + 32 * i, 32), :] = wide[pl.ds(0, 32, stride=4), :]
        leaving[pl.ds(Z_HIGH + 32 * i, 32), :] = wide[pl.ds(ROWS + 3, 32, stride=4), :]
        cells[rows, :] = base_ref[rows, :] + dot(moved, w1bct)
        both = dot_tn(node_ref[rows, :], moved)
        edge_raw[0:H, :] += both[:, :H]
        edge_raw[H : 2 * H, :] += both[:, H:]
        edge_raw[2 * H : 2 * H + 1, :] += jnp.sum(arrived, axis=0, keepdims=True)
        return carry

    lax.fori_loop(0, PLANES, collect, 0)
    leaving[X_LOW : X_LOW + ROWS, :] = sums[1, ROWS : 2 * ROWS, 0:H]
    leaving[X_HIGH : X_HIGH + ROWS, :] = sums[PLANES, 0:ROWS, 0:H]
    gone = leaving[...].astype(BF16)
    out_ref[...] = dot(gone, w1bt).astype(BF16)
    edge_raw[0:H, :] += dot_tn(face_ref[...], gone)
    block = raw_ref.shape[1]
    raw_ref[H // block : 3 * H // block] = edge_raw[0 : 2 * H, :].reshape(2 * H // block, block, H)
    raw_ref[896 // block, 896 % block : 896 % block + 1, :] = edge_raw[2 * H : 2 * H + 1, :]
    pl.semaphore_wait(barrier, chips + 2)

    def to_partner(source, target, k):
        return pltpu.make_async_remote_copy(
            src_ref=source,
            dst_ref=target,
            send_sem=pair_send.at[k],
            recv_sem=pair_recv.at[k],
            device_id=partner,
            device_id_type=MESH,
        )

    first = to_partner(raw_ref.at[pl.ds((1 - core) * chips, chips)], partner_part, 0)
    first.start()
    halos = face_copies(out_ref, faces, send_sems, recv_sems)
    for side in (0, 1, 2, 3):
        halos[side].start()
    first.wait()
    half[...] = raw_ref[pl.ds(core * chips, chips)] + partner_part[...]

    def scatter(d, carry):
        where, other = peer(d)
        pltpu.make_async_remote_copy(
            src_ref=half.at[other],
            dst_ref=parts.at[chip],
            send_sem=all_send.at[0],
            recv_sem=all_recv.at[0],
            device_id=where,
            device_id_type=MESH,
        ).start()
        return carry

    lax.fori_loop(1, chips, scatter, 0)
    for side in (4, 5):
        halos[side].start()
    parts[chip] = half[chip]

    def settle(buffer, sem):
        span = buffer.at[pl.ds(0, chips - 1)]
        pltpu.make_async_copy(span, span, sem).wait()

    settle(parts, all_recv.at[0])
    mine[...] = jnp.sum(parts[...], axis=0)

    def gather(d, carry):
        where, _ = peer(d)
        pltpu.make_async_remote_copy(
            src_ref=mine,
            dst_ref=full.at[core * chips + chip],
            send_sem=all_send.at[1],
            recv_sem=all_recv.at[1],
            device_id=where,
            device_id_type=MESH,
        ).start()
        return carry

    lax.fori_loop(1, chips, gather, 0)
    full[core * chips + chip] = mine[...]
    for item in halos:
        item.wait()
    cells[0:ROWS, :] += faces[X_LOW : X_LOW + ROWS, :].astype(F32)
    cells[CELLS - ROWS :, :] += faces[X_HIGH : X_HIGH + ROWS, :].astype(F32)
    for start, at in ((Y_LOW, 0), (Y_HIGH, 124)):
        strip = faces[start : start + 64, :].astype(F32)
        for i in range(PLANES):
            cells[ROWS * i + at : ROWS * i + at + 4, :] += strip[4 * i : 4 * i + 4]
    cells[pl.ds(0, 512, stride=4), :] += faces[Z_LOW : Z_LOW + 512, :].astype(F32)
    cells[pl.ds(3, 512, stride=4), :] += faces[Z_HIGH : Z_HIGH + 512, :].astype(F32)
    grad_ref[...] = cells[...].astype(BF16)
    settle(full, all_recv.at[1])
    held = pl.ds(core * chips, chips)
    last = to_partner(full.at[held], full.at[held], 1)
    last.start()
    settle(half, all_send.at[0])
    settle(half, all_send.at[1])
    last.wait()
    total_ref[...] = full[...]


def write_kernel(grad_ref, total_ref, *refs):
    outs, scaled, sems = refs[:6], refs[6], refs[7]
    first = pltpu.make_async_copy(grad_ref, outs[0], sems.at[0])
    first.start()
    total = total_ref[...]
    squares = jnp.sum(total * total, axis=0, keepdims=True)
    squares = jnp.sum(squares, axis=1, keepdims=True)
    factor = 1.0 / jnp.maximum(1.0, jnp.sqrt(squares / (7 * H * H + 4 * H)))
    scaled[...] = total * factor
    copies = [first]
    at = 0
    for k, rows in enumerate((384, 128, 256, 128, 4)):
        copies.append(
            pltpu.make_async_copy(scaled.at[pl.ds(at, rows), :], outs[k + 1], sems.at[k + 1])
        )
        copies[-1].start()
        at += rows
    for item in copies:
        item.wait()


def write(grad, total):
    vmem = pl.BlockSpec(memory_space=pltpu.VMEM)
    return pl.pallas_call(
        write_kernel,
        out_shape=(jax.ShapeDtypeStruct((CELLS, H), BF16),)
        + tuple(jax.ShapeDtypeStruct((rows, H), F32) for rows in (384, 128, 256, 128, 4)),
        in_specs=[vmem] * 2,
        out_specs=(pl.BlockSpec(memory_space=pl.ANY),) * 6,
        scratch_shapes=[pltpu.VMEM((RAW_ROWS, H), F32), pltpu.SemaphoreType.DMA((6,))],
        compiler_params=pltpu.CompilerParams(vmem_limit_bytes=48 * 1024 * 1024),
    )(grad, total)


def finish(base, raw, sums, faces, node, w1_edge):
    chips = lax.axis_size("gx") * lax.axis_size("gy") * lax.axis_size("gz") // 2
    block = RAW_ROWS // (2 * chips)
    vmem = pl.BlockSpec(memory_space=pltpu.VMEM)
    grad, total = pl.pallas_call(
        finish_kernel,
        out_shape=(
            jax.ShapeDtypeStruct((CELLS, H), BF16),
            jax.ShapeDtypeStruct((2 * chips, block, H), F32),
        ),
        in_specs=[vmem] * 4 + [pl.BlockSpec(memory_space=pltpu.MemorySpace.HBM)] * 2,
        out_specs=(vmem,) * 2,
        scratch_shapes=[
            pltpu.VMEM((CELLS, H), BF16),
            pltpu.VMEM((3 * H, H), BF16),
            pltpu.VMEM((2 * chips, block, H), F32),
            pltpu.VMEM((2 * H + 8, H), F32),
            pltpu.VMEM((FACES, H), F32),
            pltpu.VMEM((2 * ROWS, H), F32),
            pltpu.VMEM((FACES, H), BF16),
            pltpu.VMEM((FACES, H), BF16),
            pltpu.VMEM((CELLS, H), F32),
            pltpu.VMEM((chips, block, H), F32),
            pltpu.VMEM((chips, block, H), F32),
            pltpu.VMEM((chips, block, H), F32),
            pltpu.VMEM((block, H), F32),
            pltpu.VMEM((2 * chips, block, H), F32),
            pltpu.SemaphoreType.DMA((6,)),
            pltpu.SemaphoreType.DMA((6,)),
            pltpu.SemaphoreType.DMA((2,)),
            pltpu.SemaphoreType.DMA((2,)),
            pltpu.SemaphoreType.DMA((2,)),
            pltpu.SemaphoreType.DMA((2,)),
            pltpu.SemaphoreType.DMA((2,)),
        ],
        compiler_params=pltpu.CompilerParams(
            collective_id=1, has_side_effects=True, vmem_limit_bytes=24 * 1024 * 1024
        ),
    )(base, raw.reshape(2 * chips, block, H), sums, faces, node, w1_edge)
    return write(grad, total.reshape(RAW_ROWS, H))


def on_device(
    node_latent,
    edge_latent,
    senders,
    receivers,
    w1_edge,
    b1_edge,
    w2_edge,
    b2_edge,
    w1_node,
    b1_node,
    w2_node,
    cot_node,
    cot_edge,
):
    keep = functools.partial(
        pltpu.with_memory_space_constraint, memory_space=pltpu.MemorySpace.HBM
    )
    cells = keep(node_latent.reshape(CELLS, H))
    sender_ids = keep(senders.reshape(96, 128))
    receiver_ids = keep(receivers.reshape(96, 128))
    w1_edge = keep(w1_edge)
    faces, bounds, *columns = halo(cells, sender_ids, receiver_ids)
    grad_edge, base, raw, sums = local_terms(
        bounds,
        faces,
        columns,
        keep(edge_latent.reshape(EDGES, H)),
        keep(cot_edge.reshape(EDGES, H)),
        (
            receiver_ids,
            sender_ids,
            w1_edge,
            keep(b1_edge.reshape(1, H)),
            keep(w2_edge),
            cells,
            keep(cot_node.reshape(CELLS, H)),
            keep(b2_edge.reshape(1, H)),
            keep(w1_node),
            keep(b1_node.reshape(1, H)),
            keep(w2_node),
        ),
    )
    grad_node, *grads = finish(base, raw, sums, faces, cells, w1_edge)
    return (grad_node.reshape(node_latent.shape), grad_edge.reshape(edge_latent.shape), *grads)


def solution(mesh):
    cell = P("gx", "gy", "gz", None)
    slots = P("gx", "gy", "gz", None, None)
    placed = (cell, slots, cell, cell, P(), P(), P(), P(), P(), P(), P(), cell, slots)
    return jax.shard_map(
        on_device,
        mesh=mesh,
        in_specs=placed,
        out_specs=(cell, slots, P(), P(), P(), P(), P()),
        check_vma=False,
    )
```

```python
import functools

import jax
import jax.numpy as jnp
from jax import lax
from jax.experimental import pallas as pl
from jax.experimental.pallas import tpu as pltpu
from jax.sharding import PartitionSpec as P

H = 128
PLANES = 16
ROWS = 128
CELLS = PLANES * ROWS
EDGES = 12288
TILE = 896
LOCAL_VMEM = 37 * 1024 * 1024
PADDED = EDGES + TILE
CHUNK = 512
NODE_CHUNK = 1024
PIECE = 1024
RAW_ROWS = 1024
X_LOW, X_HIGH, Y_LOW, Y_HIGH, Z_LOW, Z_HIGH, FACES = 0, 128, 256, 320, 384, 896, 1408
SPANS = ((X_LOW, 128), (X_HIGH, 128), (Y_LOW, 64), (Y_HIGH, 64), (Z_LOW, 512), (Z_HIGH, 512))
MESH = pl.DeviceIdType.MESH

F32 = jnp.float32
BF16 = jnp.bfloat16


def dot(a, b):
    return jnp.dot(a, b, preferred_element_type=F32)


def dot_tn(a, b):
    return lax.dot_general(a, b, (((0,), (0,)), ((), ())), preferred_element_type=F32)


def pair_dot(rows, diagonal):
    half = rows.shape[0] // 2
    both = dot(jnp.concatenate([rows[:half], rows[half:]], axis=1), diagonal)
    return jnp.concatenate([both[:, :H], both[:, H:]], axis=0)


def block_diagonal(w):
    zero = jnp.zeros_like(w)
    return jnp.concatenate(
        [jnp.concatenate([w, zero], axis=1), jnp.concatenate([zero, w], axis=1)], axis=0
    )


def slope_and_value(z):
    sigma = 0.5 * jnp.tanh(0.5 * z) + 0.5
    value = z * sigma
    return value, sigma * (1.0 + (z - value))


def steps_of(send, recv):
    step = send - (((recv >> 7) + 1) * 204 + (((recv >> 2) & 31) + 1) * 6 + (recv & 3) + 1)
    size = jnp.abs(step)
    return step, jnp.where(size == 204, 0, jnp.where(size == 6, 1, 2))


def local_kernel(
    bounds,
    face_ref,
    key_col,
    kind_col,
    edge_hbm,
    cot_edge_hbm,
    *refs,
):
    small_hbm, refs = refs[:11], refs[11:]
    (
        grad_edge_hbm,
        base_ref,
        raw_ref,
        sums,
        edge,
        cot,
        value,
        slope,
        grad,
        code_row,
        proj,
        proj_own,
        proj_face,
        wide,
        gathered,
        degree,
        tables,
        diag_w1,
        diag_w2t,
        diag_w1t,
        z_a,
        z_b,
        d_a,
        d_b,
        starts,
        planes,
        sems,
        small_sems,
    ) = refs[:28]
    small = refs[28:]
    (
        recv_ref,
        send_ref,
        w1e_ref,
        b1e_ref,
        w2e_ref,
        node_ref,
        cot_node_ref,
        b2e_ref,
        w1n_ref,
        b1n_ref,
        w2n_ref,
    ) = small
    small_copies = [
        pltpu.make_async_copy(source, target, small_sems.at[k])
        for k, (source, target) in enumerate(zip(small_hbm, small))
    ]
    copies = [
        pltpu.make_async_copy(edge_hbm, edge.at[pl.ds(0, EDGES), :], sems.at[0]),
        pltpu.make_async_copy(cot_edge_hbm, cot.at[pl.ds(0, EDGES), :], sems.at[1]),
    ]
    for item in small_copies[:6] + copies[:1] + small_copies[6:] + copies[1:]:
        item.start()

    tail = jnp.zeros((TILE, H), BF16)
    for ref in (edge, cot, value, slope):
        ref[EDGES:, :] = tail

    def list_plane(i, n):
        lo, hi = bounds[i], bounds[i + 1]
        first = (lo >> 4) << 4
        count = jnp.where(hi > lo, (hi - first + (TILE - 1)) // TILE, 0)

        def put(t, n):
            starts[n] = first + t * TILE
            planes[n] = i
            return n + 1

        return lax.fori_loop(0, count, put, n)

    starts[0] = EDGES
    planes[0] = 0
    last = lax.fori_loop(0, PLANES, list_plane, 1)
    rounds = last // 2
    for k in range(3):
        starts[last + k] = EDGES
        planes[last + k] = 0

    def clear(i, carry):
        sums[i] = jnp.zeros((256, 3 * H), F32)
        return carry

    lax.fori_loop(0, PLANES + 2, clear, 0)
    gathered[...] = jnp.zeros((CELLS, 2 * H), F32)
    degree[...] = jnp.zeros((CELLS, H), F32)
    wide[...] = jnp.zeros((2 * ROWS, H), F32)
    raw_ref[...] = jnp.zeros((RAW_ROWS, H), F32)

    for item in small_copies[:6]:
        item.wait()
    recv, step, axis = recv_ref[...], *steps_of(send_ref[...], recv_ref[...])
    code = recv * 8 + jnp.where(step < 0, 4, 0) + axis
    code_row[0:96, :] = code
    code_row[96:, :] = jnp.full((code_row.shape[0] - 96, 128), -8, jnp.int32)
    w1a = w1e_ref[0:H, :]
    w1b = w1e_ref[H : 2 * H, :]
    w1c = w1e_ref[2 * H :, :]
    diag_w1[...] = block_diagonal(w1a)
    diag_w2t[...] = block_diagonal(w2e_ref[...].T)
    diag_w1t[...] = block_diagonal(w1a.T)
    b1e = b1e_ref[...]

    proj_face[...] = dot(face_ref[...], w1b)
    proj[0:ROWS, :] = proj_face[X_LOW : X_LOW + ROWS, :]
    proj[ROWS * (PLANES + 1) :, :] = proj_face[X_HIGH : X_HIGH + ROWS, :]
    w1bc = jnp.concatenate([w1b, w1c], axis=1)

    def project(k, carry):
        rows = pl.ds(pl.multiple_of(k * CHUNK, CHUNK), CHUNK)
        both = dot(node_ref[rows, :], w1bc)
        proj[pl.ds(pl.multiple_of(k * CHUNK + ROWS, ROWS), CHUNK), :] = both[:, :H]
        proj_own[rows, :] = both[:, H:] + b1e
        return carry

    lax.fori_loop(0, CELLS // CHUNK, project, 0)

    row_id = lax.broadcasted_iota(jnp.int32, (ROWS, H), 0)
    low_z = (row_id & 3) == 0
    high_z = (row_id & 3) == 3
    low_y = row_id < 4
    high_y = row_id >= 124

    def plane_rows(i):
        return pl.ds(pl.multiple_of(i * ROWS, ROWS), ROWS)

    def build_table(i, carry):
        own = proj_own[plane_rows(i), :]
        mine = proj[plane_rows(i + 1), :]
        above = proj[plane_rows(i + 2), :]
        below = proj[plane_rows(i), :]
        wide[0:4, :] = proj_face[pl.ds(Y_LOW + 4 * i, 4), :]
        wide[124:128, :] = proj_face[pl.ds(Y_HIGH + 4 * i, 4), :]
        wide[pl.ds(ROWS, 32, stride=4), :] = proj_face[pl.ds(Z_LOW + 32 * i, 32), :]
        wide[pl.ds(ROWS + 3, 32, stride=4), :] = proj_face[pl.ds(Z_HIGH + 32 * i, 32), :]
        side_y = wide[:ROWS, :]
        side_z = wide[ROWS:, :]
        up_y = jnp.where(high_y, side_y, pltpu.roll(mine, 124, 0))
        down_y = jnp.where(low_y, side_y, pltpu.roll(mine, 4, 0))
        up_z = jnp.where(high_z, side_z, pltpu.roll(mine, 127, 0))
        down_z = jnp.where(low_z, side_z, pltpu.roll(mine, 1, 0))
        tables[i, 0:ROWS, :] = jnp.concatenate(
            [above + own, up_y + own, up_z + own], axis=1
        ).astype(BF16)
        tables[i, ROWS : 2 * ROWS, :] = jnp.concatenate(
            [below + own, down_y + own, down_z + own], axis=1
        ).astype(BF16)
        return carry

    lax.fori_loop(0, PLANES, build_table, 0)

    def tile_at(j):
        start = pl.multiple_of(starts[j], 16)
        return start, pl.ds(start, TILE), planes[j]

    lane = lax.broadcasted_iota(jnp.int32, (1, 128), 1).astype(F32)
    lane_low, lane_high = lane.astype(BF16), (lane + 128.0).astype(BF16)

    one, zero = jnp.ones((TILE, 128), BF16), jnp.zeros((TILE, 128), BF16)

    def kinds(i, count):
        first = jnp.full((1, 128), 4 * i, jnp.int32).astype(F32)
        return [first + float(k) for k in range(count)]

    def head_inside(start, i):
        kind = kind_col[pl.ds(start, 16), :].astype(F32)
        low, _, high = kinds(i, 3)
        return (kind >= low) & (kind <= high)

    def row_codes(start):
        q = start >> 7
        off = start & 127
        turn = (128 - off) & 127
        here = pltpu.roll(code_row[pl.ds(q, 8), :], turn, 1)
        there = pltpu.roll(code_row[pl.ds(q + 1, 8), :], turn, 1)
        spot = lax.broadcasted_iota(jnp.int32, (8, 128), 1)
        return jnp.where(spot < 128 - off, here, there)

    def one_hot_turned(keys, slots):
        slot = lax.broadcasted_iota(jnp.int32, (slots, 128), 0)
        return [
            jnp.where(jnp.broadcast_to(keys[k : k + 1, :], (slots, 128)) == slot, 1.0, 0.0)
            for k in range(TILE // 128)
        ]

    def keep_head(ref, start, new, inside):
        old = ref[pl.ds(start, 16), :].astype(F32)
        return jnp.concatenate([jnp.where(inside, new[:16], old), new[16:]], axis=0)

    copies[0].wait()

    def forward_sums(j, z_buffer):
        start, span, i = tile_at(j)
        u, sp = slope_and_value(z_buffer[...])
        inside = head_inside(start, i)
        u = keep_head(value, start, u, inside).astype(BF16)
        value[span, :] = u
        slope[span, :] = keep_head(slope, start, sp, inside).astype(BF16)
        pieces = one_hot_turned((row_codes(start) >> 3) - 128 * i, ROWS)
        count = pieces[0]
        for piece in pieces[1:]:
            count = count + piece
        degree[plane_rows(i), :] += count
        spread = jnp.concatenate(pieces, axis=1).astype(BF16)
        gathered[plane_rows(i), :] += dot(spread, jnp.concatenate([edge[span, :], u], axis=1))

    def forward_values(j, z_buffer):
        start, span, i = tile_at(j)
        keys = key_col[span, :]
        hot = jnp.concatenate(
            [jnp.where(keys == lane_low, one, zero), jnp.where(keys == lane_high, one, zero)],
            axis=1,
        )
        picked = dot(hot, tables[i])
        kind = kind_col[span, :].astype(F32)
        first, second = kinds(i, 2)
        z_buffer[...] = pair_dot(edge[span, :], diag_w1[...]) + jnp.where(
            kind == first,
            picked[:, :H],
            jnp.where(kind == second, picked[:, H : 2 * H], picked[:, 2 * H :]),
        )

    def forward(m, carry):
        forward_values(2 * m + 1, z_a)
        forward_sums(2 * m, z_b)
        forward_values(2 * m + 2, z_b)
        forward_sums(2 * m + 1, z_a)
        return carry

    z_b[...] = jnp.zeros((TILE, H), F32)
    lax.fori_loop(0, rounds, forward, 0)
    forward_sums(2 * rounds, z_b)

    for item in small_copies[6:]:
        item.wait()
    w2nt = w2n_ref[...].T
    w1nt = w1n_ref[...].T

    def nodes(k, carry):
        rows = pl.ds(pl.multiple_of(k * NODE_CHUNK, NODE_CHUNK), NODE_CHUNK)
        packed = gathered[rows, :]
        count = jnp.sum(degree[rows, :], axis=1, keepdims=True)
        aggregate = (
            packed[:, :H]
            + dot(packed[:, H:].astype(BF16), w2e_ref[...])
            + count * b2e_ref[...]
        ).astype(BF16)
        x_node = jnp.concatenate([node_ref[rows, :], aggregate], axis=1)
        z_node = dot(x_node, w1n_ref[...]) + b1n_ref[...]
        u_node, sp_node = slope_and_value(z_node)
        cot_cells = cot_node_ref[rows, :]
        dz_node = (dot(cot_cells, w2nt) * sp_node).astype(BF16)
        dx_node = dot(dz_node, w1nt)
        base_ref[rows, :] = cot_cells.astype(F32) + dx_node[:, :H]
        gathered[rows, 0:H] = dx_node[:, H:]
        raw_ref[512:768, :] += dot_tn(x_node, dz_node)
        raw_ref[768:896, :] += dot_tn(u_node.astype(BF16), cot_cells)
        raw_ref[898:899, :] += jnp.sum(dz_node.astype(F32), axis=0, keepdims=True)
        raw_ref[899:900, :] += jnp.sum(cot_cells.astype(F32), axis=0, keepdims=True)
        return carry

    lax.fori_loop(0, CELLS // NODE_CHUNK, nodes, 0)
    copies[1].wait()

    ones = jnp.ones((16, TILE), BF16)

    def backward_sums(j, d_buffer):
        start, span, i = tile_at(j)
        dz_edge = d_buffer[:, :H]
        both = dot(
            jnp.concatenate([edge[span, :].T, value[span, :].T, ones], axis=0), d_buffer[...]
        )
        raw_ref[0:H, :] += both[:H, :H]
        raw_ref[384:512, :] += both[H : 2 * H, H:]
        raw_ref[897:898, :] += both[2 * H : 2 * H + 1, H:]
        codes = row_codes(start)
        keys = (codes >> 3) - 128 * i + ((codes >> 2) & 1) * 128
        keys = jnp.where((codes >> 10) == i, keys, -1)
        spread = jnp.concatenate(one_hot_turned(keys, 2 * ROWS), axis=1).astype(BF16)
        kind = kind_col[span, :]
        first, second = (number.astype(BF16) for number in kinds(i, 2))
        parted = jnp.concatenate(
            [
                jnp.where(kind == first, dz_edge, zero),
                jnp.where(kind == second, dz_edge, zero),
                dz_edge,
            ],
            axis=1,
        )
        sums[i + 1] += dot(spread, parted)

    def backward_values(j, d_buffer):
        start, span, i = tile_at(j)
        keys, kind = key_col[span, :], kind_col[span, :]
        hot = jnp.where((keys == lane_low) | (keys == lane_high), one, zero)
        added = pair_dot(hot, block_diagonal(gathered[plane_rows(i), 0:H].astype(BF16)))
        d_wide = cot[span, :].astype(F32) + added
        low, _, high = (number.astype(BF16) for number in kinds(i, 3))
        d_edge = jnp.where((kind >= low) & (kind <= high), d_wide.astype(BF16), zero)
        dz_edge = (pair_dot(d_edge, diag_w2t[...]) * slope[span, :].astype(F32)).astype(BF16)
        d_buffer[...] = jnp.concatenate([dz_edge, d_edge], axis=1)
        new = d_wide + pair_dot(dz_edge, diag_w1t[...])
        grad[span, :] = keep_head(grad, start, new, head_inside(start, i)).astype(BF16)

    def piece(c):
        rows = pl.ds(pl.multiple_of(c * PIECE, PIECE), PIECE)
        return pltpu.make_async_copy(grad.at[rows, :], grad_edge_hbm.at[rows, :], sems.at[2])

    def send_pieces(done, final):
        upto = final // PIECE

        def send(c, carry):
            piece(c).start()
            return carry

        lax.fori_loop(done, upto, send, 0)
        return jnp.maximum(done, upto)

    def backward(m, carry):
        backward_values(2 * m + 1, d_a)
        backward_sums(2 * m, d_b)
        backward_values(2 * m + 2, d_b)
        backward_sums(2 * m + 1, d_a)
        return send_pieces(carry, starts[2 * m + 3])

    d_b[...] = jnp.zeros((TILE, 2 * H), BF16)
    sent = lax.fori_loop(0, rounds, backward, 0)
    send_pieces(sent, EDGES)
    backward_sums(2 * rounds, d_b)
    whole = pltpu.make_async_copy(grad.at[pl.ds(0, EDGES), :], grad_edge_hbm, sems.at[2])
    whole.wait()


def local_terms(bounds, faces, columns, edge_rows, cot_rows, small):
    vmem = pl.BlockSpec(memory_space=pltpu.VMEM)
    hbm = pl.BlockSpec(memory_space=pltpu.MemorySpace.HBM)
    return pl.pallas_call(
        local_kernel,
        out_shape=(
            jax.ShapeDtypeStruct((EDGES, H), BF16),
            pltpu.VMEM((CELLS, H), F32),
            pltpu.VMEM((RAW_ROWS, H), F32),
            pltpu.VMEM((PLANES + 2, 256, 3 * H), F32),
        ),
        in_specs=[pl.BlockSpec(memory_space=pltpu.SMEM)] + [vmem] * 3 + [hbm] * 13,
        out_specs=(hbm, vmem, vmem, vmem),
        scratch_shapes=[pltpu.VMEM((PADDED, H), BF16)] * 5
        + [
            pltpu.VMEM((112, 128), jnp.int32),
            pltpu.VMEM((CELLS + 2 * ROWS, H), F32),
            pltpu.VMEM((CELLS, H), F32),
            pltpu.VMEM((FACES, H), F32),
            pltpu.VMEM((2 * ROWS, H), F32),
            pltpu.VMEM((CELLS, 2 * H), F32),
            pltpu.VMEM((CELLS, H), F32),
            pltpu.VMEM((PLANES, 256, 3 * H), BF16),
            pltpu.VMEM((256, 256), BF16),
            pltpu.VMEM((256, 256), BF16),
            pltpu.VMEM((256, 256), BF16),
            pltpu.VMEM((TILE, H), F32),
            pltpu.VMEM((TILE, H), F32),
            pltpu.VMEM((TILE, 2 * H), BF16),
            pltpu.VMEM((TILE, 2 * H), BF16),
            pltpu.SMEM((48,), jnp.int32),
            pltpu.SMEM((48,), jnp.int32),
            pltpu.SemaphoreType.DMA((3,)),
            pltpu.SemaphoreType.DMA((11,)),
        ]
        + [pltpu.VMEM(item.shape, item.dtype) for item in small],
        compiler_params=pltpu.CompilerParams(vmem_limit_bytes=LOCAL_VMEM),
        cost_estimate=pl.CostEstimate(
            flops=10_000_000_000, bytes_accessed=20_000_000, transcendentals=2_000_000
        ),
    )(bounds, faces, *columns, edge_rows, cot_rows, *small)


def place():
    return tuple(lax.axis_index(name) for name in ("gx", "gy", "gz"))


def sizes():
    return tuple(lax.axis_size(name) for name in ("gx", "gy", "gz"))


def across(side):
    dim, up = side // 2, side % 2
    here, count = place(), sizes()
    beyond = list(here)
    beyond[dim] = lax.rem(here[dim] + (1 if up else count[dim] - 1), count[dim])
    return tuple(beyond)


def face_copies(source, target, send_sems, recv_sems):
    copies = []
    for side, (first, rows) in enumerate(SPANS):
        opposite = SPANS[side ^ 1][0]
        copies.append(
            pltpu.make_async_remote_copy(
                src_ref=source.at[pl.ds(first, rows), :],
                dst_ref=target.at[pl.ds(opposite, rows), :],
                send_sem=send_sems.at[side],
                recv_sem=recv_sems.at[side],
                device_id=across(side),
                device_id_type=MESH,
            )
        )
    return copies


def halo_kernel(
    node_hbm,
    send_hbm,
    recv_hbm,
    face_ref,
    bounds_ref,
    key_col,
    kind_col,
    node_ref,
    send_ref,
    recv_ref,
    cells,
    packed,
    load_sems,
    send_sems,
    recv_sems,
):
    loads = [
        pltpu.make_async_copy(source, target, load_sems.at[k])
        for k, (source, target) in enumerate(
            ((node_hbm, node_ref), (send_hbm, send_ref), (recv_hbm, recv_ref))
        )
    ]
    for item in loads:
        item.start()
    barrier = pltpu.get_barrier_semaphore()
    for side in range(6):
        pl.semaphore_signal(barrier, inc=1, device_id=across(side), device_id_type=MESH)
    for item in loads:
        item.wait()
    cells[...] = node_ref[...].astype(F32)
    packed[X_LOW : X_LOW + ROWS, :] = node_ref[0:ROWS, :]
    packed[X_HIGH : X_HIGH + ROWS, :] = node_ref[CELLS - ROWS :, :]
    for first, at in ((Y_LOW, 0), (Y_HIGH, 124)):
        strips = [cells[ROWS * i + at : ROWS * i + at + 4, :] for i in range(PLANES)]
        packed[first : first + 64, :] = jnp.concatenate(strips, axis=0).astype(BF16)
    packed[Z_LOW : Z_LOW + 512, :] = cells[pl.ds(0, 512, stride=4), :].astype(BF16)
    packed[Z_HIGH : Z_HIGH + 512, :] = cells[pl.ds(3, 512, stride=4), :].astype(BF16)
    pl.semaphore_wait(barrier, 6)
    copies = face_copies(packed, face_ref, send_sems, recv_sems)
    for side in (5, 4, 1, 0, 3, 2):
        copies[side].start()
    recv = recv_ref[...]
    for i in range(PLANES + 1):
        below = jnp.where(recv < ROWS * i, 1.0, 0.0)
        bounds_ref[i] = jnp.sum(below).astype(jnp.int32)
    step, axis = steps_of(send_ref[...], recv)
    columns = (key_col, kind_col)
    zero = jnp.zeros((32, 128), F32)
    turned = jnp.concatenate(
        [
            jnp.concatenate([numbers.astype(F32), zero], axis=0).T
            for numbers in ((recv & 127) + jnp.where(step < 0, 128, 0), (recv >> 7) * 4 + axis)
        ],
        axis=0,
    ).astype(BF16)
    row = lax.broadcasted_iota(jnp.int32, (128, 256), 0)
    lane = lax.broadcasted_iota(jnp.int32, (128, 256), 1)
    for k in range(0, 96, 2):
        pick = jnp.where(row - (lane >> 7) == k, 1.0, 0.0).astype(BF16)
        both = dot(turned, pick).astype(BF16)
        for c, column in enumerate(columns):
            block = both[128 * c : 128 * c + 128]
            column[k * 128 : (k + 1) * 128, :] = block[:, :128]
            column[(k + 1) * 128 : (k + 2) * 128, :] = block[:, 128:]
    for column in columns:
        column[EDGES:, :] = jnp.full((TILE, 128), -4.0, BF16)
    for item in copies:
        item.wait()


def halo(node, send, recv):
    vmem = pl.BlockSpec(memory_space=pltpu.VMEM)
    return pl.pallas_call(
        halo_kernel,
        out_shape=(
            pltpu.VMEM((FACES, H), BF16),
            jax.ShapeDtypeStruct((PLANES + 1,), jnp.int32),
        )
        + (pltpu.VMEM((PADDED, 128), BF16),) * 2,
        in_specs=[pl.BlockSpec(memory_space=pltpu.MemorySpace.HBM)] * 3,
        out_specs=(vmem, pl.BlockSpec(memory_space=pltpu.SMEM)) + (vmem,) * 2,
        scratch_shapes=[
            pltpu.VMEM((CELLS, H), BF16),
            pltpu.VMEM((96, 128), jnp.int32),
            pltpu.VMEM((96, 128), jnp.int32),
            pltpu.VMEM((CELLS, H), F32),
            pltpu.VMEM((FACES, H), BF16),
            pltpu.SemaphoreType.DMA((3,)),
            pltpu.SemaphoreType.DMA((6,)),
            pltpu.SemaphoreType.DMA((6,)),
        ],
        compiler_params=pltpu.CompilerParams(
            collective_id=0, has_side_effects=True, vmem_limit_bytes=12 * 1024 * 1024
        ),
    )(node, send, recv)


def finish_kernel(
    base_ref,
    raw_in,
    sums,
    face_ref,
    node_hbm,
    w1e_hbm,
    grad_ref,
    total_ref,
    node_ref,
    w1e_ref,
    raw_ref,
    edge_raw,
    leaving,
    wide,
    out_ref,
    faces,
    cells,
    partner_part,
    half,
    parts,
    mine,
    full,
    send_sems,
    recv_sems,
    pair_send,
    pair_recv,
    all_send,
    all_recv,
    load_sems,
):
    (ga, gb, gc), (na, nb, nc) = place(), sizes()
    nz = nc // 2
    chips = na * nb * nz
    chip_z, core = lax.div(gc, 2), lax.rem(gc, 2)
    chip = (ga * nb + gb) * nz + chip_z
    partner = (ga, gb, 2 * chip_z + 1 - core)

    spots = (
        [lax.rem(ga + d, na) for d in range(na)],
        [lax.rem(gb + d, nb) for d in range(nb)],
        [lax.rem(chip_z + d, nz) for d in range(nz)],
    )
    rows_a = [spot * (nb * nz) for spot in spots[0]]
    rows_b = [spot * nz for spot in spots[1]]
    cores = [2 * spot + core for spot in spots[2]]

    def hops(d):
        da, db, dz = d
        return min(da, na - da) + min(db, nb - db) // 2 + db % 2 + 2 * dz

    offsets = sorted(
        ((da, db, dz) for da in range(na) for db in range(nb) for dz in range(nz)),
        key=lambda d: (-hops(d), d),
    )[:-1]

    def peer(d):
        da, db, dz = d
        where = (spots[0][da], spots[1][db], cores[dz])
        return where, rows_a[da] + rows_b[db] + spots[2][dz]

    barrier = pltpu.get_barrier_semaphore()
    for d in offsets:
        pl.semaphore_signal(barrier, inc=1, device_id=peer(d)[0], device_id_type=MESH)
    pl.semaphore_signal(barrier, inc=1, device_id=partner, device_id_type=MESH)
    for side in (4, 5):
        pl.semaphore_signal(barrier, inc=1, device_id=across(side), device_id_type=MESH)

    loads = [
        pltpu.make_async_copy(node_hbm, node_ref, load_sems.at[0]),
        pltpu.make_async_copy(w1e_hbm, w1e_ref, load_sems.at[1]),
    ]
    for item in loads:
        item.start()
    raw_ref[...] = raw_in[...]
    edge_raw[...] = jnp.zeros_like(edge_raw)
    for item in loads:
        item.wait()

    w1bt = w1e_ref[H : 2 * H, :].T
    w1bct = jnp.concatenate([w1bt, w1e_ref[2 * H :, :].T], axis=0)
    row_id = lax.broadcasted_iota(jnp.int32, (ROWS, H), 0)
    low_z = lax.rem(row_id, 4) == 0
    high_z = lax.rem(row_id, 4) == 3
    low_y = row_id < 4
    high_y = row_id >= 124

    def collect(i, carry):
        rows = pl.ds(pl.multiple_of(i * ROWS, ROWS), ROWS)
        here = sums[i + 1]
        third = here[:, 2 * H :] - here[:, :H] - here[:, H : 2 * H]
        arrived = here[:ROWS, 2 * H :] + here[ROWS:, 2 * H :]
        yp, ym = here[:ROWS, H : 2 * H], here[ROWS:, H : 2 * H]
        zp, zm = third[:ROWS], third[ROWS:]
        left = (
            sums[i, 0:ROWS, 0:H]
            + sums[i + 2, ROWS : 2 * ROWS, 0:H]
            + jnp.where(low_y, 0.0, pltpu.roll(yp, 4, 0))
            + jnp.where(high_y, 0.0, pltpu.roll(ym, 124, 0))
            + jnp.where(low_z, 0.0, pltpu.roll(zp, 1, 0))
            + jnp.where(high_z, 0.0, pltpu.roll(zm, 127, 0))
        )
        moved = jnp.concatenate([left, arrived], axis=1).astype(BF16)
        leaving[pl.ds(Y_LOW + 4 * i, 4), :] = ym[:4]
        leaving[pl.ds(Y_HIGH + 4 * i, 4), :] = yp[124:]
        wide[0:ROWS, :] = zm
        wide[ROWS:, :] = zp
        leaving[pl.ds(Z_LOW + 32 * i, 32), :] = wide[pl.ds(0, 32, stride=4), :]
        leaving[pl.ds(Z_HIGH + 32 * i, 32), :] = wide[pl.ds(ROWS + 3, 32, stride=4), :]
        cells[rows, :] = base_ref[rows, :] + dot(moved, w1bct)
        both = dot_tn(node_ref[rows, :], moved)
        edge_raw[0:H, :] += both[:, :H]
        edge_raw[H : 2 * H, :] += both[:, H:]
        edge_raw[2 * H : 2 * H + 1, :] += jnp.sum(arrived, axis=0, keepdims=True)
        return carry

    lax.fori_loop(0, PLANES, collect, 0)
    leaving[X_LOW : X_LOW + ROWS, :] = sums[1, ROWS : 2 * ROWS, 0:H]
    leaving[X_HIGH : X_HIGH + ROWS, :] = sums[PLANES, 0:ROWS, 0:H]
    gone = leaving[...].astype(BF16)
    out_ref[...] = dot(gone, w1bt).astype(BF16)
    edge_raw[0:H, :] += dot_tn(face_ref[...], gone)
    block = raw_ref.shape[1]
    raw_ref[H // block : 3 * H // block] = edge_raw[0 : 2 * H, :].reshape(2 * H // block, block, H)
    raw_ref[896 // block, 896 % block : 896 % block + 1, :] = edge_raw[2 * H : 2 * H + 1, :]
    pl.semaphore_wait(barrier, chips + 2)

    def to_partner(source, target, k):
        return pltpu.make_async_remote_copy(
            src_ref=source,
            dst_ref=target,
            send_sem=pair_send.at[k],
            recv_sem=pair_recv.at[k],
            device_id=partner,
            device_id_type=MESH,
        )

    first = to_partner(raw_ref.at[pl.ds((1 - core) * chips, chips)], partner_part, 0)
    first.start()
    halos = face_copies(out_ref, faces, send_sems, recv_sems)
    for side in (0, 1, 2, 3):
        halos[side].start()
    first.wait()
    half[...] = raw_ref[pl.ds(core * chips, chips)] + partner_part[...]

    for d in offsets:
        where, other = peer(d)
        pltpu.make_async_remote_copy(
            src_ref=half.at[other],
            dst_ref=parts.at[chip],
            send_sem=all_send.at[0],
            recv_sem=all_recv.at[0],
            device_id=where,
            device_id_type=MESH,
        ).start()
    parts[chip] = half[chip]

    def settle(buffer, sem):
        span = buffer.at[pl.ds(0, chips - 1)]
        pltpu.make_async_copy(span, span, sem).wait()

    settle(parts, all_recv.at[0])
    mine[...] = jnp.sum(parts[...], axis=0)

    slot = core * chips + chip
    for d in offsets:
        pltpu.make_async_remote_copy(
            src_ref=mine,
            dst_ref=full.at[slot],
            send_sem=all_send.at[1],
            recv_sem=all_recv.at[1],
            device_id=peer(d)[0],
            device_id_type=MESH,
        ).start()
    for side in (4, 5):
        halos[side].start()
    full[slot] = mine[...]
    settle(full, all_recv.at[1])
    held = pl.ds(core * chips, chips)
    last = to_partner(full.at[held], full.at[held], 1)
    last.start()
    for item in halos:
        item.wait()
    cells[0:ROWS, :] += faces[X_LOW : X_LOW + ROWS, :].astype(F32)
    cells[CELLS - ROWS :, :] += faces[X_HIGH : X_HIGH + ROWS, :].astype(F32)
    for start, at in ((Y_LOW, 0), (Y_HIGH, 124)):
        strip = faces[start : start + 64, :].astype(F32)
        for i in range(PLANES):
            cells[ROWS * i + at : ROWS * i + at + 4, :] += strip[4 * i : 4 * i + 4]
    cells[pl.ds(0, 512, stride=4), :] += faces[Z_LOW : Z_LOW + 512, :].astype(F32)
    cells[pl.ds(3, 512, stride=4), :] += faces[Z_HIGH : Z_HIGH + 512, :].astype(F32)
    grad_ref[...] = cells[...].astype(BF16)
    settle(half, all_send.at[0])
    settle(half, all_send.at[1])
    last.wait()
    total_ref[...] = full[...]


def write_kernel(grad_ref, total_ref, *refs):
    outs, scaled, sems = refs[:6], refs[6], refs[7]
    first = pltpu.make_async_copy(grad_ref, outs[0], sems.at[0])
    first.start()
    total = total_ref[...]
    squares = jnp.sum(total * total, axis=0, keepdims=True)
    squares = jnp.sum(squares, axis=1, keepdims=True)
    factor = 1.0 / jnp.maximum(1.0, jnp.sqrt(squares / (7 * H * H + 4 * H)))
    scaled[...] = total * factor
    copies = [first]
    at = 0
    for k, rows in enumerate((384, 128, 256, 128, 4)):
        copies.append(
            pltpu.make_async_copy(scaled.at[pl.ds(at, rows), :], outs[k + 1], sems.at[k + 1])
        )
        copies[-1].start()
        at += rows
    for item in copies:
        item.wait()


def write(grad, total):
    vmem = pl.BlockSpec(memory_space=pltpu.VMEM)
    return pl.pallas_call(
        write_kernel,
        out_shape=(jax.ShapeDtypeStruct((CELLS, H), BF16),)
        + tuple(jax.ShapeDtypeStruct((rows, H), F32) for rows in (384, 128, 256, 128, 4)),
        in_specs=[vmem] * 2,
        out_specs=(pl.BlockSpec(memory_space=pl.ANY),) * 6,
        scratch_shapes=[pltpu.VMEM((RAW_ROWS, H), F32), pltpu.SemaphoreType.DMA((6,))],
        compiler_params=pltpu.CompilerParams(vmem_limit_bytes=48 * 1024 * 1024),
    )(grad, total)


def finish(base, raw, sums, faces, node, w1_edge):
    chips = lax.axis_size("gx") * lax.axis_size("gy") * lax.axis_size("gz") // 2
    block = RAW_ROWS // (2 * chips)
    vmem = pl.BlockSpec(memory_space=pltpu.VMEM)
    grad, total = pl.pallas_call(
        finish_kernel,
        out_shape=(
            jax.ShapeDtypeStruct((CELLS, H), BF16),
            jax.ShapeDtypeStruct((2 * chips, block, H), F32),
        ),
        in_specs=[vmem] * 4 + [pl.BlockSpec(memory_space=pltpu.MemorySpace.HBM)] * 2,
        out_specs=(vmem,) * 2,
        scratch_shapes=[
            pltpu.VMEM((CELLS, H), BF16),
            pltpu.VMEM((3 * H, H), BF16),
            pltpu.VMEM((2 * chips, block, H), F32),
            pltpu.VMEM((2 * H + 8, H), F32),
            pltpu.VMEM((FACES, H), F32),
            pltpu.VMEM((2 * ROWS, H), F32),
            pltpu.VMEM((FACES, H), BF16),
            pltpu.VMEM((FACES, H), BF16),
            pltpu.VMEM((CELLS, H), F32),
            pltpu.VMEM((chips, block, H), F32),
            pltpu.VMEM((chips, block, H), F32),
            pltpu.VMEM((chips, block, H), F32),
            pltpu.VMEM((block, H), F32),
            pltpu.VMEM((2 * chips, block, H), F32),
            pltpu.SemaphoreType.DMA((6,)),
            pltpu.SemaphoreType.DMA((6,)),
            pltpu.SemaphoreType.DMA((2,)),
            pltpu.SemaphoreType.DMA((2,)),
            pltpu.SemaphoreType.DMA((2,)),
            pltpu.SemaphoreType.DMA((2,)),
            pltpu.SemaphoreType.DMA((2,)),
        ],
        compiler_params=pltpu.CompilerParams(
            collective_id=1, has_side_effects=True, vmem_limit_bytes=24 * 1024 * 1024
        ),
    )(base, raw.reshape(2 * chips, block, H), sums, faces, node, w1_edge)
    return write(grad, total.reshape(RAW_ROWS, H))


def on_device(
    node_latent,
    edge_latent,
    senders,
    receivers,
    w1_edge,
    b1_edge,
    w2_edge,
    b2_edge,
    w1_node,
    b1_node,
    w2_node,
    cot_node,
    cot_edge,
):
    keep = functools.partial(
        pltpu.with_memory_space_constraint, memory_space=pltpu.MemorySpace.HBM
    )
    cells = keep(node_latent.reshape(CELLS, H))
    sender_ids = keep(senders.reshape(96, 128))
    receiver_ids = keep(receivers.reshape(96, 128))
    w1_edge = keep(w1_edge)
    faces, bounds, *columns = halo(cells, sender_ids, receiver_ids)
    grad_edge, base, raw, sums = local_terms(
        bounds,
        faces,
        columns,
        keep(edge_latent.reshape(EDGES, H)),
        keep(cot_edge.reshape(EDGES, H)),
        (
            receiver_ids,
            sender_ids,
            w1_edge,
            keep(b1_edge.reshape(1, H)),
            keep(w2_edge),
            cells,
            keep(cot_node.reshape(CELLS, H)),
            keep(b2_edge.reshape(1, H)),
            keep(w1_node),
            keep(b1_node.reshape(1, H)),
            keep(w2_node),
        ),
    )
    grad_node, *grads = finish(base, raw, sums, faces, cells, w1_edge)
    return (grad_node.reshape(node_latent.shape), grad_edge.reshape(edge_latent.shape), *grads)


def solution(mesh):
    cell = P("gx", "gy", "gz", None)
    slots = P("gx", "gy", "gz", None, None)
    placed = (cell, slots, cell, cell, P(), P(), P(), P(), P(), P(), P(), cell, slots)
    return jax.shard_map(
        on_device,
        mesh=mesh,
        in_specs=placed,
        out_specs=(cell, slots, P(), P(), P(), P(), P()),
        check_vma=False,
    )
```

```python
import functools

import jax
import jax.numpy as jnp
from jax import lax
from jax.experimental import pallas as pl
from jax.experimental.pallas import tpu as pltpu
from jax.sharding import PartitionSpec as P

H = 128
PLANES = 16
ROWS = 128
CELLS = PLANES * ROWS
EDGES = 12288
TILE = 896
LOCAL_VMEM = 26 * 1024 * 1024
PADDED = EDGES + TILE
CHUNK = 512
NODE_CHUNK = 1024
PIECE = 1024
DENSE = 2048
RAW_ROWS = 1024
X_LOW, X_HIGH, Y_LOW, Y_HIGH, Z_LOW, Z_HIGH, FACES = 0, 128, 256, 320, 384, 896, 1408
SPANS = ((X_LOW, 128), (X_HIGH, 128), (Y_LOW, 64), (Y_HIGH, 64), (Z_LOW, 512), (Z_HIGH, 512))
MESH = pl.DeviceIdType.MESH

F32 = jnp.float32
BF16 = jnp.bfloat16


def dot(a, b):
    return jnp.dot(a, b, preferred_element_type=F32)


def dot_tn(a, b):
    return lax.dot_general(a, b, (((0,), (0,)), ((), ())), preferred_element_type=F32)


def pair_dot(rows, diagonal):
    half = rows.shape[0] // 2
    both = dot(jnp.concatenate([rows[:half], rows[half:]], axis=1), diagonal)
    return jnp.concatenate([both[:, :H], both[:, H:]], axis=0)


def block_diagonal(w):
    zero = jnp.zeros_like(w)
    return jnp.concatenate(
        [jnp.concatenate([w, zero], axis=1), jnp.concatenate([zero, w], axis=1)], axis=0
    )


def slope_and_value(z):
    sigma = 0.5 * jnp.tanh(0.5 * z) + 0.5
    value = z * sigma
    return value, sigma * (1.0 + (z - value))


def steps_of(send, recv):
    step = send - (((recv >> 7) + 1) * 204 + (((recv >> 2) & 31) + 1) * 6 + (recv & 3) + 1)
    size = jnp.abs(step)
    return step, jnp.where(size == 204, 0, jnp.where(size == 6, 1, 2))


def local_kernel(
    bounds,
    face_ref,
    key_col,
    kind_col,
    edge_hbm,
    cot_edge_hbm,
    *refs,
):
    small_hbm, refs = refs[:11], refs[11:]
    (
        grad_edge_hbm,
        base_ref,
        raw_ref,
        sums,
        edge,
        value,
        dz_all,
        cot,
        slope,
        grad,
        code_row,
        proj,
        proj_own,
        proj_face,
        wide,
        gathered,
        degree,
        tables,
        diag_w1,
        diag_w2t,
        diag_w1t,
        z_a,
        z_b,
        d_a,
        d_b,
        starts,
        planes,
        sems,
        small_sems,
    ) = refs[:29]
    small = refs[29:]
    (
        recv_ref,
        send_ref,
        w1e_ref,
        b1e_ref,
        w2e_ref,
        node_ref,
        cot_node_ref,
        b2e_ref,
        w1n_ref,
        b1n_ref,
        w2n_ref,
    ) = small
    small_copies = [
        pltpu.make_async_copy(source, target, small_sems.at[k])
        for k, (source, target) in enumerate(zip(small_hbm, small))
    ]
    copies = [
        pltpu.make_async_copy(edge_hbm, edge.at[pl.ds(0, EDGES), :], sems.at[0]),
        pltpu.make_async_copy(cot_edge_hbm, cot.at[pl.ds(0, EDGES), :], sems.at[1]),
    ]
    for item in small_copies[:6] + copies[:1] + small_copies[6:] + copies[1:]:
        item.start()

    tail = jnp.zeros((TILE, H), BF16)
    for ref in (edge, cot, value, slope):
        ref[EDGES:, :] = tail

    def list_plane(i, n):
        lo, hi = bounds[i], bounds[i + 1]
        first = (lo >> 4) << 4
        count = jnp.where(hi > lo, (hi - first + (TILE - 1)) // TILE, 0)

        def put(t, n):
            starts[n] = first + t * TILE
            planes[n] = i
            return n + 1

        return lax.fori_loop(0, count, put, n)

    starts[0] = EDGES
    planes[0] = 0
    last = lax.fori_loop(0, PLANES, list_plane, 1)
    rounds = last // 2
    for k in range(3):
        starts[last + k] = EDGES
        planes[last + k] = 0

    def clear(i, carry):
        sums[i] = jnp.zeros((256, 3 * H), F32)
        return carry

    lax.fori_loop(0, PLANES + 2, clear, 0)
    gathered[...] = jnp.zeros((CELLS, 2 * H), F32)
    degree[...] = jnp.zeros((CELLS, H), F32)
    wide[...] = jnp.zeros((2 * ROWS, H), F32)
    raw_ref[...] = jnp.zeros((RAW_ROWS, H), F32)

    for item in small_copies[:6]:
        item.wait()
    recv, step, axis = recv_ref[...], *steps_of(send_ref[...], recv_ref[...])
    code = recv * 8 + jnp.where(step < 0, 4, 0) + axis
    code_row[0:96, :] = code
    code_row[96:, :] = jnp.full((code_row.shape[0] - 96, 128), -8, jnp.int32)
    w1a = w1e_ref[0:H, :]
    w1b = w1e_ref[H : 2 * H, :]
    w1c = w1e_ref[2 * H :, :]
    diag_w1[...] = block_diagonal(w1a)
    diag_w2t[...] = block_diagonal(w2e_ref[...].T)
    diag_w1t[...] = block_diagonal(w1a.T)
    b1e = b1e_ref[...]

    proj_face[...] = dot(face_ref[...], w1b)
    proj[0:ROWS, :] = proj_face[X_LOW : X_LOW + ROWS, :]
    proj[ROWS * (PLANES + 1) :, :] = proj_face[X_HIGH : X_HIGH + ROWS, :]
    w1bc = jnp.concatenate([w1b, w1c], axis=1)

    def project(k, carry):
        rows = pl.ds(pl.multiple_of(k * CHUNK, CHUNK), CHUNK)
        both = dot(node_ref[rows, :], w1bc)
        proj[pl.ds(pl.multiple_of(k * CHUNK + ROWS, ROWS), CHUNK), :] = both[:, :H]
        proj_own[rows, :] = both[:, H:] + b1e
        return carry

    lax.fori_loop(0, CELLS // CHUNK, project, 0)

    row_id = lax.broadcasted_iota(jnp.int32, (ROWS, H), 0)
    low_z = (row_id & 3) == 0
    high_z = (row_id & 3) == 3
    low_y = row_id < 4
    high_y = row_id >= 124

    def plane_rows(i):
        return pl.ds(pl.multiple_of(i * ROWS, ROWS), ROWS)

    def build_table(i, carry):
        own = proj_own[plane_rows(i), :]
        mine = proj[plane_rows(i + 1), :]
        above = proj[plane_rows(i + 2), :]
        below = proj[plane_rows(i), :]
        wide[0:4, :] = proj_face[pl.ds(Y_LOW + 4 * i, 4), :]
        wide[124:128, :] = proj_face[pl.ds(Y_HIGH + 4 * i, 4), :]
        wide[pl.ds(ROWS, 32, stride=4), :] = proj_face[pl.ds(Z_LOW + 32 * i, 32), :]
        wide[pl.ds(ROWS + 3, 32, stride=4), :] = proj_face[pl.ds(Z_HIGH + 32 * i, 32), :]
        side_y = wide[:ROWS, :]
        side_z = wide[ROWS:, :]
        up_y = jnp.where(high_y, side_y, pltpu.roll(mine, 124, 0))
        down_y = jnp.where(low_y, side_y, pltpu.roll(mine, 4, 0))
        up_z = jnp.where(high_z, side_z, pltpu.roll(mine, 127, 0))
        down_z = jnp.where(low_z, side_z, pltpu.roll(mine, 1, 0))
        tables[i, 0:ROWS, :] = jnp.concatenate(
            [above + own, up_y + own, up_z + own], axis=1
        ).astype(BF16)
        tables[i, ROWS : 2 * ROWS, :] = jnp.concatenate(
            [below + own, down_y + own, down_z + own], axis=1
        ).astype(BF16)
        return carry

    lax.fori_loop(0, PLANES, build_table, 0)

    def tile_at(j):
        start = pl.multiple_of(starts[j], 16)
        return start, pl.ds(start, TILE), planes[j]

    lane = lax.broadcasted_iota(jnp.int32, (1, 128), 1).astype(F32)
    lane_low, lane_high = lane.astype(BF16), (lane + 128.0).astype(BF16)

    one, zero = jnp.ones((TILE, 128), BF16), jnp.zeros((TILE, 128), BF16)

    def kinds(i, count):
        first = jnp.full((1, 128), 4 * i, jnp.int32).astype(F32)
        return [first + float(k) for k in range(count)]

    def head_inside(start, i):
        kind = kind_col[pl.ds(start, 16), :].astype(F32)
        low, _, high = kinds(i, 3)
        return (kind >= low) & (kind <= high)

    def row_codes(start):
        q = start >> 7
        off = start & 127
        turn = (128 - off) & 127
        here = pltpu.roll(code_row[pl.ds(q, 8), :], turn, 1)
        there = pltpu.roll(code_row[pl.ds(q + 1, 8), :], turn, 1)
        spot = lax.broadcasted_iota(jnp.int32, (8, 128), 1)
        return jnp.where(spot < 128 - off, here, there)

    def one_hot_turned(keys, slots):
        slot = lax.broadcasted_iota(jnp.int32, (slots, 128), 0)
        return [
            jnp.where(jnp.broadcast_to(keys[k : k + 1, :], (slots, 128)) == slot, 1.0, 0.0)
            for k in range(TILE // 128)
        ]

    def keep_head(ref, start, new, inside):
        old = ref[pl.ds(start, 16), :].astype(F32)
        return jnp.concatenate([jnp.where(inside, new[:16], old), new[16:]], axis=0)

    def keep_rows(ref, start, new, inside):
        head = pl.ds(start, 16)
        old = ref[head, :].astype(F32)
        ref[head, :] = jnp.where(inside, new[:16].astype(F32), old).astype(BF16)
        ref[pl.ds(pl.multiple_of(start + 16, 16), TILE - 16), :] = new[16:]

    copies[0].wait()

    def forward_sums(j, z_buffer):
        start, span, i = tile_at(j)
        u, sp = slope_and_value(z_buffer[...])
        inside = head_inside(start, i)
        u = keep_head(value, start, u, inside).astype(BF16)
        value[span, :] = u
        slope[span, :] = keep_head(slope, start, sp, inside).astype(BF16)
        pieces = one_hot_turned((row_codes(start) >> 3) - 128 * i, ROWS)
        count = pieces[0]
        for piece in pieces[1:]:
            count = count + piece
        degree[plane_rows(i), :] += count
        spread = jnp.concatenate(pieces, axis=1).astype(BF16)
        gathered[plane_rows(i), :] += dot(spread, jnp.concatenate([edge[span, :], u], axis=1))

    def forward_values(j, z_buffer):
        start, span, i = tile_at(j)
        keys = key_col[span, :]
        hot = jnp.concatenate(
            [jnp.where(keys == lane_low, one, zero), jnp.where(keys == lane_high, one, zero)],
            axis=1,
        )
        picked = dot(hot, tables[i])
        kind = kind_col[span, :].astype(F32)
        first, second = kinds(i, 2)
        z_buffer[...] = pair_dot(edge[span, :], diag_w1[...]) + jnp.where(
            kind == first,
            picked[:, :H],
            jnp.where(kind == second, picked[:, H : 2 * H], picked[:, 2 * H :]),
        )

    def forward(m, carry):
        forward_values(2 * m + 1, z_a)
        forward_sums(2 * m, z_b)
        forward_values(2 * m + 2, z_b)
        forward_sums(2 * m + 1, z_a)
        return carry

    z_b[...] = jnp.zeros((TILE, H), F32)
    lax.fori_loop(0, rounds, forward, 0)
    forward_sums(2 * rounds, z_b)

    for item in small_copies[6:]:
        item.wait()
    w2nt = w2n_ref[...].T
    w1nt = w1n_ref[...].T

    def nodes(k, carry):
        rows = pl.ds(pl.multiple_of(k * NODE_CHUNK, NODE_CHUNK), NODE_CHUNK)
        packed = gathered[rows, :]
        count = jnp.sum(degree[rows, :], axis=1, keepdims=True)
        aggregate = (
            packed[:, :H]
            + dot(packed[:, H:].astype(BF16), w2e_ref[...])
            + count * b2e_ref[...]
        ).astype(BF16)
        x_node = jnp.concatenate([node_ref[rows, :], aggregate], axis=1)
        z_node = dot(x_node, w1n_ref[...]) + b1n_ref[...]
        u_node, sp_node = slope_and_value(z_node)
        cot_cells = cot_node_ref[rows, :]
        dz_node = (dot(cot_cells, w2nt) * sp_node).astype(BF16)
        dx_node = dot(dz_node, w1nt)
        base_ref[rows, :] = cot_cells.astype(F32) + dx_node[:, :H]
        gathered[rows, 0:H] = dx_node[:, H:]
        raw_ref[384:512, :] += dot_tn(packed[:, H:].astype(BF16), dx_node[:, H:].astype(BF16))
        raw_ref[897:898, :] += jnp.sum(count * dx_node[:, H:], axis=0, keepdims=True)
        raw_ref[512:768, :] += dot_tn(x_node, dz_node)
        raw_ref[768:896, :] += dot_tn(u_node.astype(BF16), cot_cells)
        raw_ref[898:899, :] += jnp.sum(dz_node.astype(F32), axis=0, keepdims=True)
        raw_ref[899:900, :] += jnp.sum(cot_cells.astype(F32), axis=0, keepdims=True)
        return carry

    lax.fori_loop(0, CELLS // NODE_CHUNK, nodes, 0)
    copies[1].wait()

    def backward_sums(j, d_buffer):
        start, span, i = tile_at(j)
        dz_edge = d_buffer[...]
        codes = row_codes(start)
        keys = (codes >> 3) - 128 * i + ((codes >> 2) & 1) * 128
        keys = jnp.where((codes >> 10) == i, keys, -1)
        spread = jnp.concatenate(one_hot_turned(keys, 2 * ROWS), axis=1).astype(BF16)
        kind = kind_col[span, :]
        first, second = (number.astype(BF16) for number in kinds(i, 2))
        parted = jnp.concatenate(
            [
                jnp.where(kind == first, dz_edge, zero),
                jnp.where(kind == second, dz_edge, zero),
                dz_edge,
            ],
            axis=1,
        )
        sums[i + 1] += dot(spread, parted)

    def backward_values(j, d_buffer):
        start, span, i = tile_at(j)
        keys = key_col[span, :]
        hot = jnp.where((keys == lane_low) | (keys == lane_high), one, zero)
        added = pair_dot(hot, block_diagonal(gathered[plane_rows(i), 0:H].astype(BF16)))
        d_wide = cot[span, :].astype(F32) + added
        d_edge = d_wide.astype(BF16)
        inside = head_inside(start, i)
        dz_edge = (pair_dot(d_edge, diag_w2t[...]) * slope[span, :].astype(F32)).astype(BF16)
        d_buffer[...] = dz_edge
        keep_rows(dz_all, start, dz_edge, inside)
        new = d_wide + pair_dot(dz_edge, diag_w1t[...])
        grad[span, :] = keep_head(grad, start, new, inside).astype(BF16)

    def piece(c):
        rows = pl.ds(pl.multiple_of(c * PIECE, PIECE), PIECE)
        return pltpu.make_async_copy(grad.at[rows, :], grad_edge_hbm.at[rows, :], sems.at[2])

    def send_pieces(done, final):
        upto = final // PIECE

        def send(c, carry):
            piece(c).start()
            return carry

        lax.fori_loop(done, upto, send, 0)
        return jnp.maximum(done, upto)

    def backward(m, carry):
        backward_values(2 * m + 1, d_a)
        backward_sums(2 * m, d_b)
        backward_values(2 * m + 2, d_b)
        backward_sums(2 * m + 1, d_a)
        return send_pieces(carry, starts[2 * m + 3])

    d_b[...] = jnp.zeros((TILE, H), BF16)
    sent = lax.fori_loop(0, rounds, backward, 0)
    send_pieces(sent, EDGES)
    backward_sums(2 * rounds, d_b)
    whole = pltpu.make_async_copy(grad.at[pl.ds(0, EDGES), :], grad_edge_hbm, sems.at[2])
    whole.wait()


def local_terms(bounds, faces, columns, edge_rows, cot_rows, small):
    vmem = pl.BlockSpec(memory_space=pltpu.VMEM)
    hbm = pl.BlockSpec(memory_space=pltpu.MemorySpace.HBM)
    return pl.pallas_call(
        local_kernel,
        out_shape=(
            jax.ShapeDtypeStruct((EDGES, H), BF16),
            pltpu.VMEM((CELLS, H), F32),
            pltpu.VMEM((RAW_ROWS, H), F32),
            pltpu.VMEM((PLANES + 2, 256, 3 * H), F32),
        )
        + (pltpu.VMEM((PADDED, H), BF16),) * 4,
        in_specs=[pl.BlockSpec(memory_space=pltpu.SMEM)] + [vmem] * 3 + [hbm] * 13,
        out_specs=(hbm,) + (vmem,) * 7,
        scratch_shapes=[pltpu.VMEM((PADDED, H), BF16)] * 2
        + [
            pltpu.VMEM((112, 128), jnp.int32),
            pltpu.VMEM((CELLS + 2 * ROWS, H), F32),
            pltpu.VMEM((CELLS, H), F32),
            pltpu.VMEM((FACES, H), F32),
            pltpu.VMEM((2 * ROWS, H), F32),
            pltpu.VMEM((CELLS, 2 * H), F32),
            pltpu.VMEM((CELLS, H), F32),
            pltpu.VMEM((PLANES, 256, 3 * H), BF16),
            pltpu.VMEM((256, 256), BF16),
            pltpu.VMEM((256, 256), BF16),
            pltpu.VMEM((256, 256), BF16),
            pltpu.VMEM((TILE, H), F32),
            pltpu.VMEM((TILE, H), F32),
            pltpu.VMEM((TILE, H), BF16),
            pltpu.VMEM((TILE, H), BF16),
            pltpu.SMEM((48,), jnp.int32),
            pltpu.SMEM((48,), jnp.int32),
            pltpu.SemaphoreType.DMA((3,)),
            pltpu.SemaphoreType.DMA((11,)),
        ]
        + [pltpu.VMEM(item.shape, item.dtype) for item in small],
        compiler_params=pltpu.CompilerParams(vmem_limit_bytes=LOCAL_VMEM),
        cost_estimate=pl.CostEstimate(
            flops=10_000_000_000, bytes_accessed=20_000_000, transcendentals=2_000_000
        ),
    )(bounds, faces, *columns, edge_rows, cot_rows, *small)


def place():
    return tuple(lax.axis_index(name) for name in ("gx", "gy", "gz"))


def sizes():
    return tuple(lax.axis_size(name) for name in ("gx", "gy", "gz"))


def across(side):
    dim, up = side // 2, side % 2
    here, count = place(), sizes()
    beyond = list(here)
    beyond[dim] = lax.rem(here[dim] + (1 if up else count[dim] - 1), count[dim])
    return tuple(beyond)


def face_copies(source, target, send_sems, recv_sems):
    copies = []
    for side, (first, rows) in enumerate(SPANS):
        opposite = SPANS[side ^ 1][0]
        copies.append(
            pltpu.make_async_remote_copy(
                src_ref=source.at[pl.ds(first, rows), :],
                dst_ref=target.at[pl.ds(opposite, rows), :],
                send_sem=send_sems.at[side],
                recv_sem=recv_sems.at[side],
                device_id=across(side),
                device_id_type=MESH,
            )
        )
    return copies


def halo_kernel(
    node_hbm,
    send_hbm,
    recv_hbm,
    face_ref,
    bounds_ref,
    key_col,
    kind_col,
    node_ref,
    send_ref,
    recv_ref,
    cells,
    packed,
    load_sems,
    send_sems,
    recv_sems,
):
    loads = [
        pltpu.make_async_copy(source, target, load_sems.at[k])
        for k, (source, target) in enumerate(
            ((node_hbm, node_ref), (send_hbm, send_ref), (recv_hbm, recv_ref))
        )
    ]
    for item in loads:
        item.start()
    barrier = pltpu.get_barrier_semaphore()
    for side in range(6):
        pl.semaphore_signal(barrier, inc=1, device_id=across(side), device_id_type=MESH)
    for item in loads:
        item.wait()
    cells[...] = node_ref[...].astype(F32)
    packed[X_LOW : X_LOW + ROWS, :] = node_ref[0:ROWS, :]
    packed[X_HIGH : X_HIGH + ROWS, :] = node_ref[CELLS - ROWS :, :]
    for first, at in ((Y_LOW, 0), (Y_HIGH, 124)):
        strips = [cells[ROWS * i + at : ROWS * i + at + 4, :] for i in range(PLANES)]
        packed[first : first + 64, :] = jnp.concatenate(strips, axis=0).astype(BF16)
    packed[Z_LOW : Z_LOW + 512, :] = cells[pl.ds(0, 512, stride=4), :].astype(BF16)
    packed[Z_HIGH : Z_HIGH + 512, :] = cells[pl.ds(3, 512, stride=4), :].astype(BF16)
    pl.semaphore_wait(barrier, 6)
    copies = face_copies(packed, face_ref, send_sems, recv_sems)
    for side in (5, 4, 1, 0, 3, 2):
        copies[side].start()
    recv = recv_ref[...]
    for i in range(PLANES + 1):
        below = jnp.where(recv < ROWS * i, 1.0, 0.0)
        bounds_ref[i] = jnp.sum(below).astype(jnp.int32)
    step, axis = steps_of(send_ref[...], recv)
    columns = (key_col, kind_col)
    zero = jnp.zeros((32, 128), F32)
    turned = jnp.concatenate(
        [
            jnp.concatenate([numbers.astype(F32), zero], axis=0).T
            for numbers in ((recv & 127) + jnp.where(step < 0, 128, 0), (recv >> 7) * 4 + axis)
        ],
        axis=0,
    ).astype(BF16)
    row = lax.broadcasted_iota(jnp.int32, (128, 256), 0)
    lane = lax.broadcasted_iota(jnp.int32, (128, 256), 1)
    for k in range(0, 96, 2):
        pick = jnp.where(row - (lane >> 7) == k, 1.0, 0.0).astype(BF16)
        both = dot(turned, pick).astype(BF16)
        for c, column in enumerate(columns):
            block = both[128 * c : 128 * c + 128]
            column[k * 128 : (k + 1) * 128, :] = block[:, :128]
            column[(k + 1) * 128 : (k + 2) * 128, :] = block[:, 128:]
    for column in columns:
        column[EDGES:, :] = jnp.full((TILE, 128), -4.0, BF16)
    for item in copies:
        item.wait()


def halo(node, send, recv):
    vmem = pl.BlockSpec(memory_space=pltpu.VMEM)
    return pl.pallas_call(
        halo_kernel,
        out_shape=(
            pltpu.VMEM((FACES, H), BF16),
            jax.ShapeDtypeStruct((PLANES + 1,), jnp.int32),
        )
        + (pltpu.VMEM((PADDED, 128), BF16),) * 2,
        in_specs=[pl.BlockSpec(memory_space=pltpu.MemorySpace.HBM)] * 3,
        out_specs=(vmem, pl.BlockSpec(memory_space=pltpu.SMEM)) + (vmem,) * 2,
        scratch_shapes=[
            pltpu.VMEM((CELLS, H), BF16),
            pltpu.VMEM((96, 128), jnp.int32),
            pltpu.VMEM((96, 128), jnp.int32),
            pltpu.VMEM((CELLS, H), F32),
            pltpu.VMEM((FACES, H), BF16),
            pltpu.SemaphoreType.DMA((3,)),
            pltpu.SemaphoreType.DMA((6,)),
            pltpu.SemaphoreType.DMA((6,)),
        ],
        compiler_params=pltpu.CompilerParams(
            collective_id=0, has_side_effects=True, vmem_limit_bytes=12 * 1024 * 1024
        ),
    )(node, send, recv)


def finish_kernel(
    base_ref,
    raw_in,
    sums,
    face_ref,
    edge,
    value,
    dz_all,
    cot,
    node_hbm,
    w1e_hbm,
    grad_ref,
    total_ref,
    node_ref,
    w1e_ref,
    raw_ref,
    edge_raw,
    dense_raw,
    leaving,
    wide,
    out_ref,
    faces,
    cells,
    partner_part,
    half,
    parts,
    mine,
    full,
    send_sems,
    recv_sems,
    pair_send,
    pair_recv,
    all_send,
    all_recv,
    load_sems,
):
    (ga, gb, gc), (na, nb, nc) = place(), sizes()
    nz = nc // 2
    chips = na * nb * nz
    chip_z, core = lax.div(gc, 2), lax.rem(gc, 2)
    chip = (ga * nb + gb) * nz + chip_z
    partner = (ga, gb, 2 * chip_z + 1 - core)

    spots = (
        [lax.rem(ga + d, na) for d in range(na)],
        [lax.rem(gb + d, nb) for d in range(nb)],
        [lax.rem(chip_z + d, nz) for d in range(nz)],
    )
    rows_a = [spot * (nb * nz) for spot in spots[0]]
    rows_b = [spot * nz for spot in spots[1]]
    cores = [2 * spot + core for spot in spots[2]]

    def hops(d):
        da, db, dz = d
        return min(da, na - da) + min(db, nb - db) // 2 + db % 2 + 2 * dz

    offsets = sorted(
        ((da, db, dz) for da in range(na) for db in range(nb) for dz in range(nz)),
        key=lambda d: (-hops(d), d),
    )[:-1]

    def peer(d):
        da, db, dz = d
        where = (spots[0][da], spots[1][db], cores[dz])
        return where, rows_a[da] + rows_b[db] + spots[2][dz]

    barrier = pltpu.get_barrier_semaphore()
    for d in offsets:
        pl.semaphore_signal(barrier, inc=1, device_id=peer(d)[0], device_id_type=MESH)
    pl.semaphore_signal(barrier, inc=1, device_id=partner, device_id_type=MESH)
    for side in (4, 5):
        pl.semaphore_signal(barrier, inc=1, device_id=across(side), device_id_type=MESH)

    loads = [
        pltpu.make_async_copy(node_hbm, node_ref, load_sems.at[0]),
        pltpu.make_async_copy(w1e_hbm, w1e_ref, load_sems.at[1]),
    ]
    for item in loads:
        item.start()
    raw_ref[...] = raw_in[...]
    edge_raw[...] = jnp.zeros_like(edge_raw)
    for item in loads:
        item.wait()

    w1bt = w1e_ref[H : 2 * H, :].T
    w1bct = jnp.concatenate([w1bt, w1e_ref[2 * H :, :].T], axis=0)
    row_id = lax.broadcasted_iota(jnp.int32, (ROWS, H), 0)
    low_z = lax.rem(row_id, 4) == 0
    high_z = lax.rem(row_id, 4) == 3
    low_y = row_id < 4
    high_y = row_id >= 124

    def collect(i, carry):
        rows = pl.ds(pl.multiple_of(i * ROWS, ROWS), ROWS)
        here = sums[i + 1]
        third = here[:, 2 * H :] - here[:, :H] - here[:, H : 2 * H]
        arrived = here[:ROWS, 2 * H :] + here[ROWS:, 2 * H :]
        yp, ym = here[:ROWS, H : 2 * H], here[ROWS:, H : 2 * H]
        zp, zm = third[:ROWS], third[ROWS:]
        left = (
            sums[i, 0:ROWS, 0:H]
            + sums[i + 2, ROWS : 2 * ROWS, 0:H]
            + jnp.where(low_y, 0.0, pltpu.roll(yp, 4, 0))
            + jnp.where(high_y, 0.0, pltpu.roll(ym, 124, 0))
            + jnp.where(low_z, 0.0, pltpu.roll(zp, 1, 0))
            + jnp.where(high_z, 0.0, pltpu.roll(zm, 127, 0))
        )
        moved = jnp.concatenate([left, arrived], axis=1).astype(BF16)
        leaving[pl.ds(Y_LOW + 4 * i, 4), :] = ym[:4]
        leaving[pl.ds(Y_HIGH + 4 * i, 4), :] = yp[124:]
        wide[0:ROWS, :] = zm
        wide[ROWS:, :] = zp
        leaving[pl.ds(Z_LOW + 32 * i, 32), :] = wide[pl.ds(0, 32, stride=4), :]
        leaving[pl.ds(Z_HIGH + 32 * i, 32), :] = wide[pl.ds(ROWS + 3, 32, stride=4), :]
        cells[rows, :] = base_ref[rows, :] + dot(moved, w1bct)
        both = dot_tn(node_ref[rows, :], moved)
        edge_raw[0:H, :] += both[:, :H]
        edge_raw[H : 2 * H, :] += both[:, H:]
        edge_raw[2 * H : 2 * H + 1, :] += jnp.sum(arrived, axis=0, keepdims=True)
        return carry

    lax.fori_loop(0, PLANES, collect, 0)
    leaving[X_LOW : X_LOW + ROWS, :] = sums[1, ROWS : 2 * ROWS, 0:H]
    leaving[X_HIGH : X_HIGH + ROWS, :] = sums[PLANES, 0:ROWS, 0:H]
    gone = leaving[...].astype(BF16)
    out_ref[...] = dot(gone, w1bt).astype(BF16)
    edge_raw[0:H, :] += dot_tn(face_ref[...], gone)
    block = raw_ref.shape[1]
    raw_ref[H // block : 3 * H // block] = edge_raw[0 : 2 * H, :].reshape(2 * H // block, block, H)
    raw_ref[896 // block, 896 % block : 896 % block + 1, :] = edge_raw[2 * H : 2 * H + 1, :]

    dense_raw[...] = jnp.zeros_like(dense_raw)
    ones = jnp.ones((16, DENSE), BF16)

    def dense(k, carry):
        rows = pl.ds(pl.multiple_of(k * DENSE, DENSE), DENSE)
        dense_raw[...] += dot(
            jnp.concatenate([edge[rows, :].T, value[rows, :].T, ones], axis=0),
            jnp.concatenate([dz_all[rows, :], cot[rows, :]], axis=1),
        )
        return carry

    lax.fori_loop(0, EDGES // DENSE, dense, 0)
    per = H // block
    raw_ref[0:per] = dense_raw[0:H, :H].reshape(per, block, H)
    raw_ref[3 * per : 4 * per] += dense_raw[H : 2 * H, H:].reshape(per, block, H)
    raw_ref[897 // block, 897 % block : 897 % block + 1, :] += dense_raw[2 * H : 2 * H + 1, H:]
    pl.semaphore_wait(barrier, chips + 2)

    def to_partner(source, target, k):
        return pltpu.make_async_remote_copy(
            src_ref=source,
            dst_ref=target,
            send_sem=pair_send.at[k],
            recv_sem=pair_recv.at[k],
            device_id=partner,
            device_id_type=MESH,
        )

    first = to_partner(raw_ref.at[pl.ds((1 - core) * chips, chips)], partner_part, 0)
    first.start()
    halos = face_copies(out_ref, faces, send_sems, recv_sems)
    for side in (0, 1, 2, 3):
        halos[side].start()
    first.wait()
    half[...] = raw_ref[pl.ds(core * chips, chips)] + partner_part[...]

    for d in offsets:
        where, other = peer(d)
        pltpu.make_async_remote_copy(
            src_ref=half.at[other],
            dst_ref=parts.at[chip],
            send_sem=all_send.at[0],
            recv_sem=all_recv.at[0],
            device_id=where,
            device_id_type=MESH,
        ).start()
    parts[chip] = half[chip]

    def settle(buffer, sem):
        span = buffer.at[pl.ds(0, chips - 1)]
        pltpu.make_async_copy(span, span, sem).wait()

    settle(parts, all_recv.at[0])
    mine[...] = jnp.sum(parts[...], axis=0)

    slot = core * chips + chip
    for d in offsets:
        pltpu.make_async_remote_copy(
            src_ref=mine,
            dst_ref=full.at[slot],
            send_sem=all_send.at[1],
            recv_sem=all_recv.at[1],
            device_id=peer(d)[0],
            device_id_type=MESH,
        ).start()
    for side in (4, 5):
        halos[side].start()
    full[slot] = mine[...]
    settle(full, all_recv.at[1])
    held = pl.ds(core * chips, chips)
    last = to_partner(full.at[held], full.at[held], 1)
    last.start()
    for item in halos:
        item.wait()
    cells[0:ROWS, :] += faces[X_LOW : X_LOW + ROWS, :].astype(F32)
    cells[CELLS - ROWS :, :] += faces[X_HIGH : X_HIGH + ROWS, :].astype(F32)
    for start, at in ((Y_LOW, 0), (Y_HIGH, 124)):
        strip = faces[start : start + 64, :].astype(F32)
        for i in range(PLANES):
            cells[ROWS * i + at : ROWS * i + at + 4, :] += strip[4 * i : 4 * i + 4]
    cells[pl.ds(0, 512, stride=4), :] += faces[Z_LOW : Z_LOW + 512, :].astype(F32)
    cells[pl.ds(3, 512, stride=4), :] += faces[Z_HIGH : Z_HIGH + 512, :].astype(F32)
    grad_ref[...] = cells[...].astype(BF16)
    settle(half, all_send.at[0])
    settle(half, all_send.at[1])
    last.wait()
    total_ref[...] = full[...]


def write_kernel(grad_ref, total_ref, *refs):
    outs, scaled, sems = refs[:6], refs[6], refs[7]
    first = pltpu.make_async_copy(grad_ref, outs[0], sems.at[0])
    first.start()
    total = total_ref[...]
    squares = jnp.sum(total * total, axis=0, keepdims=True)
    squares = jnp.sum(squares, axis=1, keepdims=True)
    factor = 1.0 / jnp.maximum(1.0, jnp.sqrt(squares / (7 * H * H + 4 * H)))
    scaled[...] = total * factor
    copies = [first]
    at = 0
    for k, rows in enumerate((384, 128, 256, 128, 4)):
        copies.append(
            pltpu.make_async_copy(scaled.at[pl.ds(at, rows), :], outs[k + 1], sems.at[k + 1])
        )
        copies[-1].start()
        at += rows
    for item in copies:
        item.wait()


def write(grad, total):
    vmem = pl.BlockSpec(memory_space=pltpu.VMEM)
    return pl.pallas_call(
        write_kernel,
        out_shape=(jax.ShapeDtypeStruct((CELLS, H), BF16),)
        + tuple(jax.ShapeDtypeStruct((rows, H), F32) for rows in (384, 128, 256, 128, 4)),
        in_specs=[vmem] * 2,
        out_specs=(pl.BlockSpec(memory_space=pl.ANY),) * 6,
        scratch_shapes=[pltpu.VMEM((RAW_ROWS, H), F32), pltpu.SemaphoreType.DMA((6,))],
        compiler_params=pltpu.CompilerParams(vmem_limit_bytes=48 * 1024 * 1024),
    )(grad, total)


def finish(base, raw, sums, faces, slots, node, w1_edge):
    chips = lax.axis_size("gx") * lax.axis_size("gy") * lax.axis_size("gz") // 2
    block = RAW_ROWS // (2 * chips)
    vmem = pl.BlockSpec(memory_space=pltpu.VMEM)
    grad, total = pl.pallas_call(
        finish_kernel,
        out_shape=(
            jax.ShapeDtypeStruct((CELLS, H), BF16),
            jax.ShapeDtypeStruct((2 * chips, block, H), F32),
        ),
        in_specs=[vmem] * 8 + [pl.BlockSpec(memory_space=pltpu.MemorySpace.HBM)] * 2,
        out_specs=(vmem,) * 2,
        scratch_shapes=[
            pltpu.VMEM((CELLS, H), BF16),
            pltpu.VMEM((3 * H, H), BF16),
            pltpu.VMEM((2 * chips, block, H), F32),
            pltpu.VMEM((2 * H + 8, H), F32),
            pltpu.VMEM((2 * H + 16, 2 * H), F32),
            pltpu.VMEM((FACES, H), F32),
            pltpu.VMEM((2 * ROWS, H), F32),
            pltpu.VMEM((FACES, H), BF16),
            pltpu.VMEM((FACES, H), BF16),
            pltpu.VMEM((CELLS, H), F32),
            pltpu.VMEM((chips, block, H), F32),
            pltpu.VMEM((chips, block, H), F32),
            pltpu.VMEM((chips, block, H), F32),
            pltpu.VMEM((block, H), F32),
            pltpu.VMEM((2 * chips, block, H), F32),
            pltpu.SemaphoreType.DMA((6,)),
            pltpu.SemaphoreType.DMA((6,)),
            pltpu.SemaphoreType.DMA((2,)),
            pltpu.SemaphoreType.DMA((2,)),
            pltpu.SemaphoreType.DMA((2,)),
            pltpu.SemaphoreType.DMA((2,)),
            pltpu.SemaphoreType.DMA((2,)),
        ],
        compiler_params=pltpu.CompilerParams(
            collective_id=1, has_side_effects=True, vmem_limit_bytes=24 * 1024 * 1024
        ),
    )(base, raw.reshape(2 * chips, block, H), sums, faces, *slots, node, w1_edge)
    return write(grad, total.reshape(RAW_ROWS, H))


def on_device(
    node_latent,
    edge_latent,
    senders,
    receivers,
    w1_edge,
    b1_edge,
    w2_edge,
    b2_edge,
    w1_node,
    b1_node,
    w2_node,
    cot_node,
    cot_edge,
):
    keep = functools.partial(
        pltpu.with_memory_space_constraint, memory_space=pltpu.MemorySpace.HBM
    )
    cells = keep(node_latent.reshape(CELLS, H))
    sender_ids = keep(senders.reshape(96, 128))
    receiver_ids = keep(receivers.reshape(96, 128))
    w1_edge = keep(w1_edge)
    faces, bounds, *columns = halo(cells, sender_ids, receiver_ids)
    grad_edge, base, raw, sums, *slots = local_terms(
        bounds,
        faces,
        columns,
        keep(edge_latent.reshape(EDGES, H)),
        keep(cot_edge.reshape(EDGES, H)),
        (
            receiver_ids,
            sender_ids,
            w1_edge,
            keep(b1_edge.reshape(1, H)),
            keep(w2_edge),
            cells,
            keep(cot_node.reshape(CELLS, H)),
            keep(b2_edge.reshape(1, H)),
            keep(w1_node),
            keep(b1_node.reshape(1, H)),
            keep(w2_node),
        ),
    )
    grad_node, *grads = finish(base, raw, sums, faces, slots, cells, w1_edge)
    return (grad_node.reshape(node_latent.shape), grad_edge.reshape(edge_latent.shape), *grads)


def solution(mesh):
    cell = P("gx", "gy", "gz", None)
    slots = P("gx", "gy", "gz", None, None)
    placed = (cell, slots, cell, cell, P(), P(), P(), P(), P(), P(), P(), cell, slots)
    return jax.shard_map(
        on_device,
        mesh=mesh,
        in_specs=placed,
        out_specs=(cell, slots, P(), P(), P(), P(), P()),
        check_vma=False,
    )
```

```python
import functools

import jax
import jax.numpy as jnp
from jax import lax
from jax.experimental import pallas as pl
from jax.experimental.pallas import tpu as pltpu
from jax.sharding import PartitionSpec as P

H = 128
PLANES = 16
ROWS = 128
CELLS = PLANES * ROWS
EDGES = 12288
TILE = 896
LOCAL_VMEM = 26 * 1024 * 1024
PADDED = EDGES + TILE
CHUNK = 512
NODE_CHUNK = 2048
PIECE = 1024
PROJECT = 2048
DENSE = 4096
RAW_ROWS = 1024
X_LOW, X_HIGH, Y_LOW, Y_HIGH, Z_LOW, Z_HIGH, FACES = 0, 128, 256, 320, 384, 896, 1408
SPANS = ((X_LOW, 128), (X_HIGH, 128), (Y_LOW, 64), (Y_HIGH, 64), (Z_LOW, 512), (Z_HIGH, 512))
MESH = pl.DeviceIdType.MESH

F32 = jnp.float32
BF16 = jnp.bfloat16


def dot(a, b):
    return jnp.dot(a, b, preferred_element_type=F32)


def dot_tn(a, b):
    return lax.dot_general(a, b, (((0,), (0,)), ((), ())), preferred_element_type=F32)


def pair_dot(rows, diagonal):
    half = rows.shape[0] // 2
    both = dot(jnp.concatenate([rows[:half], rows[half:]], axis=1), diagonal)
    return jnp.concatenate([both[:, :H], both[:, H:]], axis=0)


def block_diagonal(w):
    zero = jnp.zeros_like(w)
    return jnp.concatenate(
        [jnp.concatenate([w, zero], axis=1), jnp.concatenate([zero, w], axis=1)], axis=0
    )


def slope_and_value(z):
    sigma = 0.5 * jnp.tanh(0.5 * z) + 0.5
    value = z * sigma
    return value, sigma * (1.0 + (z - value))


def steps_of(send, recv):
    step = send - (((recv >> 7) + 1) * 204 + (((recv >> 2) & 31) + 1) * 6 + (recv & 3) + 1)
    size = jnp.abs(step)
    return step, jnp.where(size == 204, 0, jnp.where(size == 6, 1, 2))


def local_kernel(
    bounds,
    face_ref,
    key_col,
    kind_col,
    edge_hbm,
    cot_edge_hbm,
    *refs,
):
    small_hbm, refs = refs[:11], refs[11:]
    (
        grad_edge_hbm,
        base_ref,
        raw_ref,
        sums,
        edge,
        value,
        dz_all,
        cot,
        slope,
        grad,
        code_row,
        proj,
        proj_own,
        proj_face,
        wide,
        gathered,
        degree,
        tables,
        diag_w1,
        diag_w2t,
        diag_w1t,
        z_a,
        z_b,
        d_a,
        d_b,
        starts,
        planes,
        sems,
        small_sems,
    ) = refs[:29]
    small = refs[29:]
    (
        recv_ref,
        send_ref,
        w1e_ref,
        b1e_ref,
        w2e_ref,
        node_ref,
        cot_node_ref,
        b2e_ref,
        w1n_ref,
        b1n_ref,
        w2n_ref,
    ) = small
    small_copies = [
        pltpu.make_async_copy(source, target, small_sems.at[k])
        for k, (source, target) in enumerate(zip(small_hbm, small))
    ]
    copies = [
        pltpu.make_async_copy(edge_hbm, edge.at[pl.ds(0, EDGES), :], sems.at[0]),
        pltpu.make_async_copy(cot_edge_hbm, cot.at[pl.ds(0, EDGES), :], sems.at[1]),
    ]
    for item in small_copies[:6] + copies[:1] + small_copies[6:] + copies[1:]:
        item.start()

    tail = jnp.zeros((TILE, H), BF16)
    for ref in (edge, cot, value, slope):
        ref[EDGES:, :] = tail

    def list_plane(i, n):
        lo, hi = bounds[i], bounds[i + 1]
        first = (lo >> 4) << 4
        count = jnp.where(hi > lo, (hi - first + (TILE - 1)) // TILE, 0)

        def put(t, n):
            starts[n] = first + t * TILE
            planes[n] = i
            return n + 1

        return lax.fori_loop(0, count, put, n)

    starts[0] = EDGES
    planes[0] = 0
    last = lax.fori_loop(0, PLANES, list_plane, 1)
    rounds = last // 2
    for k in range(3):
        starts[last + k] = EDGES
        planes[last + k] = 0

    def clear(i, carry):
        sums[i] = jnp.zeros((256, 3 * H), F32)
        return carry

    lax.fori_loop(0, PLANES + 2, clear, 0)
    gathered[...] = jnp.zeros((CELLS, 2 * H), F32)
    degree[...] = jnp.zeros((CELLS, H), F32)
    wide[...] = jnp.zeros((2 * ROWS, H), F32)
    raw_ref[...] = jnp.zeros((RAW_ROWS, H), F32)

    for item in small_copies[:6]:
        item.wait()
    recv, step, axis = recv_ref[...], *steps_of(send_ref[...], recv_ref[...])
    code = recv * 8 + jnp.where(step < 0, 4, 0) + axis
    code_row[0:96, :] = code
    code_row[96:, :] = jnp.full((code_row.shape[0] - 96, 128), -8, jnp.int32)
    w1a = w1e_ref[0:H, :]
    w1b = w1e_ref[H : 2 * H, :]
    w1c = w1e_ref[2 * H :, :]
    diag_w1[...] = block_diagonal(w1a)
    diag_w2t[...] = block_diagonal(w2e_ref[...].T)
    diag_w1t[...] = block_diagonal(w1a.T)
    b1e = b1e_ref[...]

    proj_face[...] = dot(face_ref[...], w1b)
    proj[0:ROWS, :] = proj_face[X_LOW : X_LOW + ROWS, :]
    proj[ROWS * (PLANES + 1) :, :] = proj_face[X_HIGH : X_HIGH + ROWS, :]
    w1bc = jnp.concatenate([w1b, w1c], axis=1)

    def project(k, carry):
        rows = pl.ds(pl.multiple_of(k * PROJECT, PROJECT), PROJECT)
        both = dot(node_ref[rows, :], w1bc)
        proj[pl.ds(pl.multiple_of(k * PROJECT + ROWS, ROWS), PROJECT), :] = both[:, :H]
        proj_own[rows, :] = both[:, H:] + b1e
        return carry

    lax.fori_loop(0, CELLS // PROJECT, project, 0)

    row_id = lax.broadcasted_iota(jnp.int32, (ROWS, H), 0)
    low_z = (row_id & 3) == 0
    high_z = (row_id & 3) == 3
    low_y = row_id < 4
    high_y = row_id >= 124

    def plane_rows(i):
        return pl.ds(pl.multiple_of(i * ROWS, ROWS), ROWS)

    def build_table(i, carry):
        own = proj_own[plane_rows(i), :]
        mine = proj[plane_rows(i + 1), :]
        above = proj[plane_rows(i + 2), :]
        below = proj[plane_rows(i), :]
        wide[0:4, :] = proj_face[pl.ds(Y_LOW + 4 * i, 4), :]
        wide[124:128, :] = proj_face[pl.ds(Y_HIGH + 4 * i, 4), :]
        wide[pl.ds(ROWS, 32, stride=4), :] = proj_face[pl.ds(Z_LOW + 32 * i, 32), :]
        wide[pl.ds(ROWS + 3, 32, stride=4), :] = proj_face[pl.ds(Z_HIGH + 32 * i, 32), :]
        side_y = wide[:ROWS, :]
        side_z = wide[ROWS:, :]
        up_y = jnp.where(high_y, side_y, pltpu.roll(mine, 124, 0))
        down_y = jnp.where(low_y, side_y, pltpu.roll(mine, 4, 0))
        up_z = jnp.where(high_z, side_z, pltpu.roll(mine, 127, 0))
        down_z = jnp.where(low_z, side_z, pltpu.roll(mine, 1, 0))
        tables[i, 0:ROWS, :] = jnp.concatenate(
            [above + own, up_y + own, up_z + own], axis=1
        ).astype(BF16)
        tables[i, ROWS : 2 * ROWS, :] = jnp.concatenate(
            [below + own, down_y + own, down_z + own], axis=1
        ).astype(BF16)
        return carry

    lax.fori_loop(0, PLANES, build_table, 0)

    def tile_at(j):
        start = pl.multiple_of(starts[j], 16)
        return start, pl.ds(start, TILE), planes[j]

    lane = lax.broadcasted_iota(jnp.int32, (1, 128), 1).astype(F32)
    lane_low, lane_high = lane.astype(BF16), (lane + 128.0).astype(BF16)

    one, zero = jnp.ones((TILE, 128), BF16), jnp.zeros((TILE, 128), BF16)

    def kinds(i, count):
        first = jnp.full((1, 128), 4 * i, jnp.int32).astype(F32)
        return [first + float(k) for k in range(count)]

    def head_inside(start, i):
        kind = kind_col[pl.ds(start, 16), :].astype(F32)
        low, _, high = kinds(i, 3)
        return (kind >= low) & (kind <= high)

    def row_codes(start):
        q = start >> 7
        off = start & 127
        turn = (128 - off) & 127
        here = pltpu.roll(code_row[pl.ds(q, 8), :], turn, 1)
        there = pltpu.roll(code_row[pl.ds(q + 1, 8), :], turn, 1)
        spot = lax.broadcasted_iota(jnp.int32, (8, 128), 1)
        return jnp.where(spot < 128 - off, here, there)

    def one_hot_turned(keys, slots):
        slot = lax.broadcasted_iota(jnp.int32, (slots, 128), 0)
        return [
            jnp.where(jnp.broadcast_to(keys[k : k + 1, :], (slots, 128)) == slot, 1.0, 0.0)
            for k in range(TILE // 128)
        ]

    def keep_head(ref, start, new, inside):
        old = ref[pl.ds(start, 16), :].astype(F32)
        return jnp.concatenate([jnp.where(inside, new[:16], old), new[16:]], axis=0)

    def keep_rows(ref, start, new, inside):
        head = pl.ds(start, 16)
        old = ref[head, :].astype(F32)
        ref[head, :] = jnp.where(inside, new[:16].astype(F32), old).astype(BF16)
        ref[pl.ds(pl.multiple_of(start + 16, 16), TILE - 16), :] = new[16:]

    copies[0].wait()

    def forward_sums(j, z_buffer):
        start, span, i = tile_at(j)
        u, sp = slope_and_value(z_buffer[...])
        inside = head_inside(start, i)
        u = keep_head(value, start, u, inside).astype(BF16)
        value[span, :] = u
        slope[span, :] = keep_head(slope, start, sp, inside).astype(BF16)
        pieces = one_hot_turned((row_codes(start) >> 3) - 128 * i, ROWS)
        count = pieces[0]
        for piece in pieces[1:]:
            count = count + piece
        degree[plane_rows(i), :] += count
        spread = jnp.concatenate(pieces, axis=1).astype(BF16)
        gathered[plane_rows(i), :] += dot(spread, jnp.concatenate([edge[span, :], u], axis=1))

    def forward_values(j, z_buffer):
        start, span, i = tile_at(j)
        keys = key_col[span, :]
        hot = jnp.concatenate(
            [jnp.where(keys == lane_low, one, zero), jnp.where(keys == lane_high, one, zero)],
            axis=1,
        )
        picked = dot(hot, tables[i])
        kind = kind_col[span, :].astype(F32)
        first, second = kinds(i, 2)
        z_buffer[...] = pair_dot(edge[span, :], diag_w1[...]) + jnp.where(
            kind == first,
            picked[:, :H],
            jnp.where(kind == second, picked[:, H : 2 * H], picked[:, 2 * H :]),
        )

    def forward(m, carry):
        forward_values(2 * m + 1, z_a)
        forward_sums(2 * m, z_b)
        forward_values(2 * m + 2, z_b)
        forward_sums(2 * m + 1, z_a)
        return carry

    z_b[...] = jnp.zeros((TILE, H), F32)
    lax.fori_loop(0, rounds, forward, 0)
    forward_sums(2 * rounds, z_b)

    for item in small_copies[6:]:
        item.wait()
    w2nt = w2n_ref[...].T
    w1nt = w1n_ref[...].T

    def nodes(k, carry):
        rows = pl.ds(pl.multiple_of(k * NODE_CHUNK, NODE_CHUNK), NODE_CHUNK)
        packed = gathered[rows, :]
        count = jnp.sum(degree[rows, :], axis=1, keepdims=True)
        aggregate = (
            packed[:, :H]
            + dot(packed[:, H:].astype(BF16), w2e_ref[...])
            + count * b2e_ref[...]
        ).astype(BF16)
        x_node = jnp.concatenate([node_ref[rows, :], aggregate], axis=1)
        z_node = dot(x_node, w1n_ref[...]) + b1n_ref[...]
        u_node, sp_node = slope_and_value(z_node)
        cot_cells = cot_node_ref[rows, :]
        dz_node = (dot(cot_cells, w2nt) * sp_node).astype(BF16)
        dx_node = dot(dz_node, w1nt)
        base_ref[rows, :] = cot_cells.astype(F32) + dx_node[:, :H]
        gathered[rows, 0:H] = dx_node[:, H:]
        raw_ref[384:512, :] += dot_tn(packed[:, H:].astype(BF16), dx_node[:, H:].astype(BF16))
        raw_ref[897:898, :] += jnp.sum(count * dx_node[:, H:], axis=0, keepdims=True)
        raw_ref[512:768, :] += dot_tn(x_node, dz_node)
        raw_ref[768:896, :] += dot_tn(u_node.astype(BF16), cot_cells)
        raw_ref[898:899, :] += jnp.sum(dz_node.astype(F32), axis=0, keepdims=True)
        raw_ref[899:900, :] += jnp.sum(cot_cells.astype(F32), axis=0, keepdims=True)
        return carry

    lax.fori_loop(0, CELLS // NODE_CHUNK, nodes, 0)
    copies[1].wait()

    def backward_sums(j, d_buffer):
        start, span, i = tile_at(j)
        dz_edge = d_buffer[...]
        codes = row_codes(start)
        keys = (codes >> 3) - 128 * i + ((codes >> 2) & 1) * 128
        keys = jnp.where((codes >> 10) == i, keys, -1)
        spread = jnp.concatenate(one_hot_turned(keys, 2 * ROWS), axis=1).astype(BF16)
        kind = kind_col[span, :]
        first, second = (number.astype(BF16) for number in kinds(i, 2))
        parted = jnp.concatenate(
            [
                jnp.where(kind == first, dz_edge, zero),
                jnp.where(kind == second, dz_edge, zero),
                dz_edge,
            ],
            axis=1,
        )
        sums[i + 1] += dot(spread, parted)

    def backward_values(j, d_buffer):
        start, span, i = tile_at(j)
        keys = key_col[span, :]
        hot = jnp.where((keys == lane_low) | (keys == lane_high), one, zero)
        added = pair_dot(hot, block_diagonal(gathered[plane_rows(i), 0:H].astype(BF16)))
        d_wide = cot[span, :].astype(F32) + added
        d_edge = d_wide.astype(BF16)
        inside = head_inside(start, i)
        dz_edge = (pair_dot(d_edge, diag_w2t[...]) * slope[span, :].astype(F32)).astype(BF16)
        d_buffer[...] = dz_edge
        keep_rows(dz_all, start, dz_edge, inside)
        new = d_wide + pair_dot(dz_edge, diag_w1t[...])
        grad[span, :] = keep_head(grad, start, new, inside).astype(BF16)

    def piece(c):
        rows = pl.ds(pl.multiple_of(c * PIECE, PIECE), PIECE)
        return pltpu.make_async_copy(grad.at[rows, :], grad_edge_hbm.at[rows, :], sems.at[2])

    def send_pieces(done, final):
        upto = final // PIECE

        def send(c, carry):
            piece(c).start()
            return carry

        lax.fori_loop(done, upto, send, 0)
        return jnp.maximum(done, upto)

    def backward(m, carry):
        backward_values(2 * m + 1, d_a)
        backward_sums(2 * m, d_b)
        backward_values(2 * m + 2, d_b)
        backward_sums(2 * m + 1, d_a)
        return send_pieces(carry, starts[2 * m + 3])

    d_b[...] = jnp.zeros((TILE, H), BF16)
    sent = lax.fori_loop(0, rounds, backward, 0)
    send_pieces(sent, EDGES)
    backward_sums(2 * rounds, d_b)
    whole = pltpu.make_async_copy(grad.at[pl.ds(0, EDGES), :], grad_edge_hbm, sems.at[2])
    whole.wait()


def local_terms(bounds, faces, columns, edge_rows, cot_rows, small):
    vmem = pl.BlockSpec(memory_space=pltpu.VMEM)
    hbm = pl.BlockSpec(memory_space=pltpu.MemorySpace.HBM)
    return pl.pallas_call(
        local_kernel,
        out_shape=(
            jax.ShapeDtypeStruct((EDGES, H), BF16),
            pltpu.VMEM((CELLS, H), F32),
            pltpu.VMEM((RAW_ROWS, H), F32),
            pltpu.VMEM((PLANES + 2, 256, 3 * H), F32),
        )
        + (pltpu.VMEM((PADDED, H), BF16),) * 4,
        in_specs=[pl.BlockSpec(memory_space=pltpu.SMEM)] + [vmem] * 3 + [hbm] * 13,
        out_specs=(hbm,) + (vmem,) * 7,
        scratch_shapes=[pltpu.VMEM((PADDED, H), BF16)] * 2
        + [
            pltpu.VMEM((112, 128), jnp.int32),
            pltpu.VMEM((CELLS + 2 * ROWS, H), F32),
            pltpu.VMEM((CELLS, H), F32),
            pltpu.VMEM((FACES, H), F32),
            pltpu.VMEM((2 * ROWS, H), F32),
            pltpu.VMEM((CELLS, 2 * H), F32),
            pltpu.VMEM((CELLS, H), F32),
            pltpu.VMEM((PLANES, 256, 3 * H), BF16),
            pltpu.VMEM((256, 256), BF16),
            pltpu.VMEM((256, 256), BF16),
            pltpu.VMEM((256, 256), BF16),
            pltpu.VMEM((TILE, H), F32),
            pltpu.VMEM((TILE, H), F32),
            pltpu.VMEM((TILE, H), BF16),
            pltpu.VMEM((TILE, H), BF16),
            pltpu.SMEM((48,), jnp.int32),
            pltpu.SMEM((48,), jnp.int32),
            pltpu.SemaphoreType.DMA((3,)),
            pltpu.SemaphoreType.DMA((11,)),
        ]
        + [pltpu.VMEM(item.shape, item.dtype) for item in small],
        compiler_params=pltpu.CompilerParams(vmem_limit_bytes=LOCAL_VMEM),
        cost_estimate=pl.CostEstimate(
            flops=10_000_000_000, bytes_accessed=20_000_000, transcendentals=2_000_000
        ),
    )(bounds, faces, *columns, edge_rows, cot_rows, *small)


def place():
    return tuple(lax.axis_index(name) for name in ("gx", "gy", "gz"))


def sizes():
    return tuple(lax.axis_size(name) for name in ("gx", "gy", "gz"))


def across(side):
    dim, up = side // 2, side % 2
    here, count = place(), sizes()
    beyond = list(here)
    beyond[dim] = lax.rem(here[dim] + (1 if up else count[dim] - 1), count[dim])
    return tuple(beyond)


def face_copies(source, target, send_sems, recv_sems):
    copies = []
    for side, (first, rows) in enumerate(SPANS):
        opposite = SPANS[side ^ 1][0]
        copies.append(
            pltpu.make_async_remote_copy(
                src_ref=source.at[pl.ds(first, rows), :],
                dst_ref=target.at[pl.ds(opposite, rows), :],
                send_sem=send_sems.at[side],
                recv_sem=recv_sems.at[side],
                device_id=across(side),
                device_id_type=MESH,
            )
        )
    return copies


def halo_kernel(
    node_hbm,
    send_hbm,
    recv_hbm,
    face_ref,
    bounds_ref,
    key_col,
    kind_col,
    node_ref,
    send_ref,
    recv_ref,
    cells,
    packed,
    load_sems,
    send_sems,
    recv_sems,
):
    loads = [
        pltpu.make_async_copy(source, target, load_sems.at[k])
        for k, (source, target) in enumerate(
            ((node_hbm, node_ref), (send_hbm, send_ref), (recv_hbm, recv_ref))
        )
    ]
    for item in loads:
        item.start()
    barrier = pltpu.get_barrier_semaphore()
    for side in range(6):
        pl.semaphore_signal(barrier, inc=1, device_id=across(side), device_id_type=MESH)
    for item in loads:
        item.wait()
    cells[...] = node_ref[...].astype(F32)
    packed[X_LOW : X_LOW + ROWS, :] = node_ref[0:ROWS, :]
    packed[X_HIGH : X_HIGH + ROWS, :] = node_ref[CELLS - ROWS :, :]
    for first, at in ((Y_LOW, 0), (Y_HIGH, 124)):
        strips = [cells[ROWS * i + at : ROWS * i + at + 4, :] for i in range(PLANES)]
        packed[first : first + 64, :] = jnp.concatenate(strips, axis=0).astype(BF16)
    packed[Z_LOW : Z_LOW + 512, :] = cells[pl.ds(0, 512, stride=4), :].astype(BF16)
    packed[Z_HIGH : Z_HIGH + 512, :] = cells[pl.ds(3, 512, stride=4), :].astype(BF16)
    pl.semaphore_wait(barrier, 6)
    copies = face_copies(packed, face_ref, send_sems, recv_sems)
    for side in (5, 4, 1, 0, 3, 2):
        copies[side].start()
    recv = recv_ref[...]
    for i in range(PLANES + 1):
        below = jnp.where(recv < ROWS * i, 1.0, 0.0)
        bounds_ref[i] = jnp.sum(below).astype(jnp.int32)
    step, axis = steps_of(send_ref[...], recv)
    columns = (key_col, kind_col)
    zero = jnp.zeros((32, 128), F32)
    turned = jnp.concatenate(
        [
            jnp.concatenate([numbers.astype(F32), zero], axis=0).T
            for numbers in ((recv & 127) + jnp.where(step < 0, 128, 0), (recv >> 7) * 4 + axis)
        ],
        axis=0,
    ).astype(BF16)
    row = lax.broadcasted_iota(jnp.int32, (128, 256), 0)
    lane = lax.broadcasted_iota(jnp.int32, (128, 256), 1)
    for k in range(0, 96, 2):
        pick = jnp.where(row - (lane >> 7) == k, 1.0, 0.0).astype(BF16)
        both = dot(turned, pick).astype(BF16)
        for c, column in enumerate(columns):
            block = both[128 * c : 128 * c + 128]
            column[k * 128 : (k + 1) * 128, :] = block[:, :128]
            column[(k + 1) * 128 : (k + 2) * 128, :] = block[:, 128:]
    for column in columns:
        column[EDGES:, :] = jnp.full((TILE, 128), -4.0, BF16)
    for item in copies:
        item.wait()


def halo(node, send, recv):
    vmem = pl.BlockSpec(memory_space=pltpu.VMEM)
    return pl.pallas_call(
        halo_kernel,
        out_shape=(
            pltpu.VMEM((FACES, H), BF16),
            jax.ShapeDtypeStruct((PLANES + 1,), jnp.int32),
        )
        + (pltpu.VMEM((PADDED, 128), BF16),) * 2,
        in_specs=[pl.BlockSpec(memory_space=pltpu.MemorySpace.HBM)] * 3,
        out_specs=(vmem, pl.BlockSpec(memory_space=pltpu.SMEM)) + (vmem,) * 2,
        scratch_shapes=[
            pltpu.VMEM((CELLS, H), BF16),
            pltpu.VMEM((96, 128), jnp.int32),
            pltpu.VMEM((96, 128), jnp.int32),
            pltpu.VMEM((CELLS, H), F32),
            pltpu.VMEM((FACES, H), BF16),
            pltpu.SemaphoreType.DMA((3,)),
            pltpu.SemaphoreType.DMA((6,)),
            pltpu.SemaphoreType.DMA((6,)),
        ],
        compiler_params=pltpu.CompilerParams(
            collective_id=0, has_side_effects=True, vmem_limit_bytes=12 * 1024 * 1024
        ),
    )(node, send, recv)


def finish_kernel(
    base_ref,
    raw_in,
    sums,
    face_ref,
    edge,
    value,
    dz_all,
    cot,
    node_hbm,
    w1e_hbm,
    grad_ref,
    total_ref,
    node_ref,
    w1e_ref,
    raw_ref,
    edge_raw,
    dense_raw,
    leaving,
    moved,
    wide,
    out_ref,
    faces,
    cells,
    partner_part,
    half,
    parts,
    mine,
    full,
    send_sems,
    recv_sems,
    pair_send,
    pair_recv,
    all_send,
    all_recv,
    load_sems,
):
    (ga, gb, gc), (na, nb, nc) = place(), sizes()
    nz = nc // 2
    chips = na * nb * nz
    chip_z, core = lax.div(gc, 2), lax.rem(gc, 2)
    chip = (ga * nb + gb) * nz + chip_z
    partner = (ga, gb, 2 * chip_z + 1 - core)

    spots = (
        [lax.rem(ga + d, na) for d in range(na)],
        [lax.rem(gb + d, nb) for d in range(nb)],
        [lax.rem(chip_z + d, nz) for d in range(nz)],
    )
    rows_a = [spot * (nb * nz) for spot in spots[0]]
    rows_b = [spot * nz for spot in spots[1]]
    cores = [2 * spot + core for spot in spots[2]]

    def hops(d):
        da, db, dz = d
        return min(da, na - da) + min(db, nb - db) // 2 + db % 2 + 2 * dz

    offsets = sorted(
        ((da, db, dz) for da in range(na) for db in range(nb) for dz in range(nz)),
        key=lambda d: (-hops(d), d),
    )[:-1]

    def peer(d):
        da, db, dz = d
        where = (spots[0][da], spots[1][db], cores[dz])
        return where, rows_a[da] + rows_b[db] + spots[2][dz]

    barrier = pltpu.get_barrier_semaphore()
    for d in offsets:
        pl.semaphore_signal(barrier, inc=1, device_id=peer(d)[0], device_id_type=MESH)
    pl.semaphore_signal(barrier, inc=1, device_id=partner, device_id_type=MESH)
    for side in (4, 5):
        pl.semaphore_signal(barrier, inc=1, device_id=across(side), device_id_type=MESH)

    loads = [
        pltpu.make_async_copy(node_hbm, node_ref, load_sems.at[0]),
        pltpu.make_async_copy(w1e_hbm, w1e_ref, load_sems.at[1]),
    ]
    for item in loads:
        item.start()
    raw_ref[...] = raw_in[...]
    edge_raw[...] = jnp.zeros_like(edge_raw)
    for item in loads:
        item.wait()

    w1bt = w1e_ref[H : 2 * H, :].T
    w1bct = jnp.concatenate([w1bt, w1e_ref[2 * H :, :].T], axis=0)
    row_id = lax.broadcasted_iota(jnp.int32, (ROWS, H), 0)
    low_z = lax.rem(row_id, 4) == 0
    high_z = lax.rem(row_id, 4) == 3
    low_y = row_id < 4
    high_y = row_id >= 124

    def collect(i, carry):
        rows = pl.ds(pl.multiple_of(i * ROWS, ROWS), ROWS)
        here = sums[i + 1]
        third = here[:, 2 * H :] - here[:, :H] - here[:, H : 2 * H]
        arrived = here[:ROWS, 2 * H :] + here[ROWS:, 2 * H :]
        yp, ym = here[:ROWS, H : 2 * H], here[ROWS:, H : 2 * H]
        zp, zm = third[:ROWS], third[ROWS:]
        left = (
            sums[i, 0:ROWS, 0:H]
            + sums[i + 2, ROWS : 2 * ROWS, 0:H]
            + jnp.where(low_y, 0.0, pltpu.roll(yp, 4, 0))
            + jnp.where(high_y, 0.0, pltpu.roll(ym, 124, 0))
            + jnp.where(low_z, 0.0, pltpu.roll(zp, 1, 0))
            + jnp.where(high_z, 0.0, pltpu.roll(zm, 127, 0))
        )
        both_ways = jnp.concatenate([left, arrived], axis=1).astype(BF16)
        moved[rows, :] = both_ways
        leaving[pl.ds(Y_LOW + 4 * i, 4), :] = ym[:4]
        leaving[pl.ds(Y_HIGH + 4 * i, 4), :] = yp[124:]
        wide[0:ROWS, :] = zm
        wide[ROWS:, :] = zp
        leaving[pl.ds(Z_LOW + 32 * i, 32), :] = wide[pl.ds(0, 32, stride=4), :]
        leaving[pl.ds(Z_HIGH + 32 * i, 32), :] = wide[pl.ds(ROWS + 3, 32, stride=4), :]
        both = dot_tn(node_ref[rows, :], both_ways)
        edge_raw[0:H, :] += both[:, :H]
        edge_raw[H : 2 * H, :] += both[:, H:]
        edge_raw[2 * H : 2 * H + 1, :] += jnp.sum(arrived, axis=0, keepdims=True)
        return carry

    lax.fori_loop(0, PLANES, collect, 0)
    leaving[X_LOW : X_LOW + ROWS, :] = sums[1, ROWS : 2 * ROWS, 0:H]
    leaving[X_HIGH : X_HIGH + ROWS, :] = sums[PLANES, 0:ROWS, 0:H]
    edge_raw[0:H, :] += dot_tn(face_ref[...], leaving[...].astype(BF16))
    block = raw_ref.shape[1]
    raw_ref[H // block : 3 * H // block] = edge_raw[0 : 2 * H, :].reshape(2 * H // block, block, H)
    raw_ref[896 // block, 896 % block : 896 % block + 1, :] = edge_raw[2 * H : 2 * H + 1, :]

    dense_raw[...] = jnp.zeros_like(dense_raw)
    ones = jnp.ones((16, DENSE), BF16)

    def dense(k, carry):
        rows = pl.ds(pl.multiple_of(k * DENSE, DENSE), DENSE)
        dense_raw[...] += dot(
            jnp.concatenate([edge[rows, :].T, value[rows, :].T, ones], axis=0),
            jnp.concatenate([dz_all[rows, :], cot[rows, :]], axis=1),
        )
        return carry

    lax.fori_loop(0, EDGES // DENSE, dense, 0)
    per = H // block
    raw_ref[0:per] = dense_raw[0:H, :H].reshape(per, block, H)
    raw_ref[3 * per : 4 * per] += dense_raw[H : 2 * H, H:].reshape(per, block, H)
    raw_ref[897 // block, 897 % block : 897 % block + 1, :] += dense_raw[2 * H : 2 * H + 1, H:]
    pl.semaphore_wait(barrier, chips + 2)

    def to_partner(source, target, k):
        return pltpu.make_async_remote_copy(
            src_ref=source,
            dst_ref=target,
            send_sem=pair_send.at[k],
            recv_sem=pair_recv.at[k],
            device_id=partner,
            device_id_type=MESH,
        )

    first = to_partner(raw_ref.at[pl.ds((1 - core) * chips, chips)], partner_part, 0)
    first.start()
    first.wait()
    half[...] = raw_ref[pl.ds(core * chips, chips)] + partner_part[...]

    for d in offsets:
        where, other = peer(d)
        pltpu.make_async_remote_copy(
            src_ref=half.at[other],
            dst_ref=parts.at[chip],
            send_sem=all_send.at[0],
            recv_sem=all_recv.at[0],
            device_id=where,
            device_id_type=MESH,
        ).start()
    parts[chip] = half[chip]

    out_ref[...] = dot(leaving[...].astype(BF16), w1bt).astype(BF16)
    halos = face_copies(out_ref, faces, send_sems, recv_sems)
    for side in (0, 1, 2, 3):
        halos[side].start()

    def combine(k, carry):
        rows = pl.ds(pl.multiple_of(k * CHUNK, CHUNK), CHUNK)
        cells[rows, :] = base_ref[rows, :] + dot(moved[rows, :], w1bct)
        return carry

    lax.fori_loop(0, CELLS // CHUNK, combine, 0)

    def settle(buffer, sem):
        span = buffer.at[pl.ds(0, chips - 1)]
        pltpu.make_async_copy(span, span, sem).wait()

    settle(parts, all_recv.at[0])
    mine[...] = jnp.sum(parts[...], axis=0)

    slot = core * chips + chip
    for d in offsets:
        pltpu.make_async_remote_copy(
            src_ref=mine,
            dst_ref=full.at[slot],
            send_sem=all_send.at[1],
            recv_sem=all_recv.at[1],
            device_id=peer(d)[0],
            device_id_type=MESH,
        ).start()
    for side in (4, 5):
        halos[side].start()
    full[slot] = mine[...]
    settle(full, all_recv.at[1])
    held = pl.ds(core * chips, chips)
    last = to_partner(full.at[held], full.at[held], 1)
    last.start()
    for item in halos:
        item.wait()
    cells[0:ROWS, :] += faces[X_LOW : X_LOW + ROWS, :].astype(F32)
    cells[CELLS - ROWS :, :] += faces[X_HIGH : X_HIGH + ROWS, :].astype(F32)
    for start, at in ((Y_LOW, 0), (Y_HIGH, 124)):
        strip = faces[start : start + 64, :].astype(F32)
        for i in range(PLANES):
            cells[ROWS * i + at : ROWS * i + at + 4, :] += strip[4 * i : 4 * i + 4]
    cells[pl.ds(0, 512, stride=4), :] += faces[Z_LOW : Z_LOW + 512, :].astype(F32)
    cells[pl.ds(3, 512, stride=4), :] += faces[Z_HIGH : Z_HIGH + 512, :].astype(F32)
    grad_ref[...] = cells[...].astype(BF16)
    settle(half, all_send.at[0])
    settle(half, all_send.at[1])
    last.wait()
    total_ref[...] = full[...]


def write_kernel(grad_ref, total_ref, *refs):
    outs, scaled, sems = refs[:6], refs[6], refs[7]
    first = pltpu.make_async_copy(grad_ref, outs[0], sems.at[0])
    first.start()
    total = total_ref[...]
    squares = jnp.sum(total * total, axis=0, keepdims=True)
    squares = jnp.sum(squares, axis=1, keepdims=True)
    factor = 1.0 / jnp.maximum(1.0, jnp.sqrt(squares / (7 * H * H + 4 * H)))
    scaled[...] = total * factor
    copies = [first]
    at = 0
    for k, rows in enumerate((384, 128, 256, 128, 4)):
        copies.append(
            pltpu.make_async_copy(scaled.at[pl.ds(at, rows), :], outs[k + 1], sems.at[k + 1])
        )
        copies[-1].start()
        at += rows
    for item in copies:
        item.wait()


def write(grad, total):
    vmem = pl.BlockSpec(memory_space=pltpu.VMEM)
    return pl.pallas_call(
        write_kernel,
        out_shape=(jax.ShapeDtypeStruct((CELLS, H), BF16),)
        + tuple(jax.ShapeDtypeStruct((rows, H), F32) for rows in (384, 128, 256, 128, 4)),
        in_specs=[vmem] * 2,
        out_specs=(pl.BlockSpec(memory_space=pl.ANY),) * 6,
        scratch_shapes=[pltpu.VMEM((RAW_ROWS, H), F32), pltpu.SemaphoreType.DMA((6,))],
        compiler_params=pltpu.CompilerParams(vmem_limit_bytes=48 * 1024 * 1024),
    )(grad, total)


def finish(base, raw, sums, faces, slots, node, w1_edge):
    chips = lax.axis_size("gx") * lax.axis_size("gy") * lax.axis_size("gz") // 2
    block = RAW_ROWS // (2 * chips)
    vmem = pl.BlockSpec(memory_space=pltpu.VMEM)
    grad, total = pl.pallas_call(
        finish_kernel,
        out_shape=(
            jax.ShapeDtypeStruct((CELLS, H), BF16),
            jax.ShapeDtypeStruct((2 * chips, block, H), F32),
        ),
        in_specs=[vmem] * 8 + [pl.BlockSpec(memory_space=pltpu.MemorySpace.HBM)] * 2,
        out_specs=(vmem,) * 2,
        scratch_shapes=[
            pltpu.VMEM((CELLS, H), BF16),
            pltpu.VMEM((3 * H, H), BF16),
            pltpu.VMEM((2 * chips, block, H), F32),
            pltpu.VMEM((2 * H + 8, H), F32),
            pltpu.VMEM((2 * H + 16, 2 * H), F32),
            pltpu.VMEM((FACES, H), F32),
            pltpu.VMEM((CELLS, 2 * H), BF16),
            pltpu.VMEM((2 * ROWS, H), F32),
            pltpu.VMEM((FACES, H), BF16),
            pltpu.VMEM((FACES, H), BF16),
            pltpu.VMEM((CELLS, H), F32),
            pltpu.VMEM((chips, block, H), F32),
            pltpu.VMEM((chips, block, H), F32),
            pltpu.VMEM((chips, block, H), F32),
            pltpu.VMEM((block, H), F32),
            pltpu.VMEM((2 * chips, block, H), F32),
            pltpu.SemaphoreType.DMA((6,)),
            pltpu.SemaphoreType.DMA((6,)),
            pltpu.SemaphoreType.DMA((2,)),
            pltpu.SemaphoreType.DMA((2,)),
            pltpu.SemaphoreType.DMA((2,)),
            pltpu.SemaphoreType.DMA((2,)),
            pltpu.SemaphoreType.DMA((2,)),
        ],
        compiler_params=pltpu.CompilerParams(
            collective_id=1, has_side_effects=True, vmem_limit_bytes=24 * 1024 * 1024
        ),
    )(base, raw.reshape(2 * chips, block, H), sums, faces, *slots, node, w1_edge)
    return write(grad, total.reshape(RAW_ROWS, H))


def on_device(
    node_latent,
    edge_latent,
    senders,
    receivers,
    w1_edge,
    b1_edge,
    w2_edge,
    b2_edge,
    w1_node,
    b1_node,
    w2_node,
    cot_node,
    cot_edge,
):
    keep = functools.partial(
        pltpu.with_memory_space_constraint, memory_space=pltpu.MemorySpace.HBM
    )
    cells = keep(node_latent.reshape(CELLS, H))
    sender_ids = keep(senders.reshape(96, 128))
    receiver_ids = keep(receivers.reshape(96, 128))
    w1_edge = keep(w1_edge)
    faces, bounds, *columns = halo(cells, sender_ids, receiver_ids)
    grad_edge, base, raw, sums, *slots = local_terms(
        bounds,
        faces,
        columns,
        keep(edge_latent.reshape(EDGES, H)),
        keep(cot_edge.reshape(EDGES, H)),
        (
            receiver_ids,
            sender_ids,
            w1_edge,
            keep(b1_edge.reshape(1, H)),
            keep(w2_edge),
            cells,
            keep(cot_node.reshape(CELLS, H)),
            keep(b2_edge.reshape(1, H)),
            keep(w1_node),
            keep(b1_node.reshape(1, H)),
            keep(w2_node),
        ),
    )
    grad_node, *grads = finish(base, raw, sums, faces, slots, cells, w1_edge)
    return (grad_node.reshape(node_latent.shape), grad_edge.reshape(edge_latent.shape), *grads)


def solution(mesh):
    cell = P("gx", "gy", "gz", None)
    slots = P("gx", "gy", "gz", None, None)
    placed = (cell, slots, cell, cell, P(), P(), P(), P(), P(), P(), P(), cell, slots)
    return jax.shard_map(
        on_device,
        mesh=mesh,
        in_specs=placed,
        out_specs=(cell, slots, P(), P(), P(), P(), P()),
        check_vma=False,
    )
```

```python
import functools

import jax
import jax.numpy as jnp
from jax import lax
from jax.experimental import pallas as pl
from jax.experimental.pallas import tpu as pltpu
from jax.sharding import PartitionSpec as P

H = 128
PLANES = 16
ROWS = 128
CELLS = PLANES * ROWS
EDGES = 12288
TILE = 896
LOCAL_VMEM = 26 * 1024 * 1024
PADDED = EDGES + TILE
CHUNK = 512
NODE_CHUNK = 2048
PIECE = 1024
PROJECT = 2048
DENSE = 4096
RAW_ROWS = 1024
X_LOW, X_HIGH, Y_LOW, Y_HIGH, Z_LOW, Z_HIGH, FACES = 0, 128, 256, 320, 384, 896, 1408
SPANS = ((X_LOW, 128), (X_HIGH, 128), (Y_LOW, 64), (Y_HIGH, 64), (Z_LOW, 512), (Z_HIGH, 512))
MESH = pl.DeviceIdType.MESH

F32 = jnp.float32
BF16 = jnp.bfloat16


def dot(a, b):
    return jnp.dot(a, b, preferred_element_type=F32)


def dot_tn(a, b):
    return lax.dot_general(a, b, (((0,), (0,)), ((), ())), preferred_element_type=F32)


def pair_dot(rows, diagonal):
    half = rows.shape[0] // 2
    both = dot(jnp.concatenate([rows[:half], rows[half:]], axis=1), diagonal)
    return jnp.concatenate([both[:, :H], both[:, H:]], axis=0)


def block_diagonal(w):
    zero = jnp.zeros_like(w)
    return jnp.concatenate(
        [jnp.concatenate([w, zero], axis=1), jnp.concatenate([zero, w], axis=1)], axis=0
    )


def slope_and_value(z):
    sigma = 0.5 * jnp.tanh(0.5 * z) + 0.5
    value = z * sigma
    return value, sigma * (1.0 + (z - value))


def steps_of(send, recv):
    step = send - (((recv >> 7) + 1) * 204 + (((recv >> 2) & 31) + 1) * 6 + (recv & 3) + 1)
    size = jnp.abs(step)
    return step, jnp.where(size == 204, 0, jnp.where(size == 6, 1, 2))


def local_kernel(
    bounds,
    face_ref,
    key_col,
    kind_col,
    edge_hbm,
    cot_edge_hbm,
    *refs,
):
    small_hbm, refs = refs[:11], refs[11:]
    (
        grad_edge_hbm,
        base_ref,
        raw_ref,
        sums,
        edge,
        value,
        dz_all,
        cot,
        slope,
        grad,
        code_row,
        proj,
        proj_own,
        proj_face,
        wide,
        gathered,
        degree,
        tables,
        diag_w1,
        diag_w2t,
        diag_w1t,
        z_a,
        z_b,
        d_a,
        d_b,
        starts,
        planes,
        sems,
        small_sems,
    ) = refs[:29]
    small = refs[29:]
    (
        recv_ref,
        send_ref,
        w1e_ref,
        b1e_ref,
        w2e_ref,
        node_ref,
        cot_node_ref,
        b2e_ref,
        w1n_ref,
        b1n_ref,
        w2n_ref,
    ) = small
    small_copies = [
        pltpu.make_async_copy(source, target, small_sems.at[k])
        for k, (source, target) in enumerate(zip(small_hbm, small))
    ]
    copies = [
        pltpu.make_async_copy(edge_hbm, edge.at[pl.ds(0, EDGES), :], sems.at[0]),
        pltpu.make_async_copy(cot_edge_hbm, cot.at[pl.ds(0, EDGES), :], sems.at[1]),
    ]
    for item in small_copies[:6] + copies[:1] + small_copies[6:] + copies[1:]:
        item.start()

    tail = jnp.zeros((TILE, H), BF16)
    for ref in (edge, cot, value, slope):
        ref[EDGES:, :] = tail

    def list_plane(i, n):
        lo, hi = bounds[i], bounds[i + 1]
        first = (lo >> 4) << 4
        count = jnp.where(hi > lo, (hi - first + (TILE - 1)) // TILE, 0)

        def put(t, n):
            starts[n] = first + t * TILE
            planes[n] = i
            return n + 1

        return lax.fori_loop(0, count, put, n)

    starts[0] = EDGES
    planes[0] = 0
    last = lax.fori_loop(0, PLANES, list_plane, 1)
    rounds = last // 2
    for k in range(3):
        starts[last + k] = EDGES
        planes[last + k] = 0

    def clear(i, carry):
        sums[i] = jnp.zeros((256, 3 * H), F32)
        return carry

    lax.fori_loop(0, PLANES + 2, clear, 0)
    gathered[...] = jnp.zeros((CELLS, 2 * H), F32)
    degree[...] = jnp.zeros((CELLS, H), F32)
    wide[...] = jnp.zeros((2 * ROWS, H), F32)
    raw_ref[...] = jnp.zeros((RAW_ROWS, H), F32)

    for item in small_copies[:6]:
        item.wait()
    recv, step, axis = recv_ref[...], *steps_of(send_ref[...], recv_ref[...])
    code = recv * 8 + jnp.where(step < 0, 4, 0) + axis
    code_row[0:96, :] = code
    code_row[96:, :] = jnp.full((code_row.shape[0] - 96, 128), -8, jnp.int32)
    w1a = w1e_ref[0:H, :]
    w1b = w1e_ref[H : 2 * H, :]
    w1c = w1e_ref[2 * H :, :]
    diag_w1[...] = block_diagonal(w1a)
    diag_w2t[...] = block_diagonal(w2e_ref[...].T)
    diag_w1t[...] = block_diagonal(w1a.T)
    b1e = b1e_ref[...]

    proj_face[...] = dot(face_ref[...], w1b)
    proj[0:ROWS, :] = proj_face[X_LOW : X_LOW + ROWS, :]
    proj[ROWS * (PLANES + 1) :, :] = proj_face[X_HIGH : X_HIGH + ROWS, :]
    w1bc = jnp.concatenate([w1b, w1c], axis=1)

    def project(k, carry):
        rows = pl.ds(pl.multiple_of(k * PROJECT, PROJECT), PROJECT)
        both = dot(node_ref[rows, :], w1bc)
        proj[pl.ds(pl.multiple_of(k * PROJECT + ROWS, ROWS), PROJECT), :] = both[:, :H]
        proj_own[rows, :] = both[:, H:] + b1e
        return carry

    lax.fori_loop(0, CELLS // PROJECT, project, 0)

    row_id = lax.broadcasted_iota(jnp.int32, (ROWS, H), 0)
    low_z = (row_id & 3) == 0
    high_z = (row_id & 3) == 3
    low_y = row_id < 4
    high_y = row_id >= 124

    def plane_rows(i):
        return pl.ds(pl.multiple_of(i * ROWS, ROWS), ROWS)

    def build_table(i, carry):
        own = proj_own[plane_rows(i), :]
        mine = proj[plane_rows(i + 1), :]
        above = proj[plane_rows(i + 2), :]
        below = proj[plane_rows(i), :]
        wide[0:4, :] = proj_face[pl.ds(Y_LOW + 4 * i, 4), :]
        wide[124:128, :] = proj_face[pl.ds(Y_HIGH + 4 * i, 4), :]
        wide[pl.ds(ROWS, 32, stride=4), :] = proj_face[pl.ds(Z_LOW + 32 * i, 32), :]
        wide[pl.ds(ROWS + 3, 32, stride=4), :] = proj_face[pl.ds(Z_HIGH + 32 * i, 32), :]
        side_y = wide[:ROWS, :]
        side_z = wide[ROWS:, :]
        up_y = jnp.where(high_y, side_y, pltpu.roll(mine, 124, 0))
        down_y = jnp.where(low_y, side_y, pltpu.roll(mine, 4, 0))
        up_z = jnp.where(high_z, side_z, pltpu.roll(mine, 127, 0))
        down_z = jnp.where(low_z, side_z, pltpu.roll(mine, 1, 0))
        tables[i, 0:ROWS, :] = jnp.concatenate(
            [above + own, up_y + own, up_z + own], axis=1
        ).astype(BF16)
        tables[i, ROWS : 2 * ROWS, :] = jnp.concatenate(
            [below + own, down_y + own, down_z + own], axis=1
        ).astype(BF16)
        return carry

    lax.fori_loop(0, PLANES, build_table, 0)

    def tile_at(j):
        start = pl.multiple_of(starts[j], 16)
        return start, pl.ds(start, TILE), planes[j]

    lane = lax.broadcasted_iota(jnp.int32, (1, 128), 1).astype(F32)
    lane_low, lane_high = lane.astype(BF16), (lane + 128.0).astype(BF16)

    one, zero = jnp.ones((TILE, 128), BF16), jnp.zeros((TILE, 128), BF16)

    def kinds(i, count):
        first = jnp.full((1, 128), 4 * i, jnp.int32).astype(F32)
        return [first + float(k) for k in range(count)]

    def head_inside(start, i):
        kind = kind_col[pl.ds(start, 16), :].astype(F32)
        low, _, high = kinds(i, 3)
        return (kind >= low) & (kind <= high)

    def row_codes(start):
        q = start >> 7
        off = start & 127
        turn = (128 - off) & 127
        here = pltpu.roll(code_row[pl.ds(q, 8), :], turn, 1)
        there = pltpu.roll(code_row[pl.ds(q + 1, 8), :], turn, 1)
        spot = lax.broadcasted_iota(jnp.int32, (8, 128), 1)
        return jnp.where(spot < 128 - off, here, there)

    def one_hot_turned(keys, slots):
        slot = lax.broadcasted_iota(jnp.int32, (slots, 128), 0)
        return [
            jnp.where(jnp.broadcast_to(keys[k : k + 1, :], (slots, 128)) == slot, 1.0, 0.0)
            for k in range(TILE // 128)
        ]

    def keep_head(ref, start, new, inside):
        old = ref[pl.ds(start, 16), :].astype(F32)
        return jnp.concatenate([jnp.where(inside, new[:16], old), new[16:]], axis=0)

    def keep_rows(ref, start, new, inside):
        head = pl.ds(start, 16)
        old = ref[head, :].astype(F32)
        ref[head, :] = jnp.where(inside, new[:16].astype(F32), old).astype(BF16)
        ref[pl.ds(pl.multiple_of(start + 16, 16), TILE - 16), :] = new[16:]

    copies[0].wait()

    def forward_sums(j, z_buffer):
        start, span, i = tile_at(j)
        u, sp = slope_and_value(z_buffer[...])
        inside = head_inside(start, i)
        u = keep_head(value, start, u, inside).astype(BF16)
        value[span, :] = u
        slope[span, :] = keep_head(slope, start, sp, inside).astype(BF16)
        pieces = one_hot_turned((row_codes(start) >> 3) - 128 * i, ROWS)
        count = pieces[0]
        for piece in pieces[1:]:
            count = count + piece
        degree[plane_rows(i), :] += count
        spread = jnp.concatenate(pieces, axis=1).astype(BF16)
        gathered[plane_rows(i), :] += dot(spread, jnp.concatenate([edge[span, :], u], axis=1))

    def forward_values(j, z_buffer):
        start, span, i = tile_at(j)
        keys = key_col[span, :]
        hot = jnp.concatenate(
            [jnp.where(keys == lane_low, one, zero), jnp.where(keys == lane_high, one, zero)],
            axis=1,
        )
        picked = dot(hot, tables[i])
        kind = kind_col[span, :].astype(F32)
        first, second = kinds(i, 2)
        z_buffer[...] = pair_dot(edge[span, :], diag_w1[...]) + jnp.where(
            kind == first,
            picked[:, :H],
            jnp.where(kind == second, picked[:, H : 2 * H], picked[:, 2 * H :]),
        )

    def forward(m, carry):
        forward_values(2 * m + 1, z_a)
        forward_sums(2 * m, z_b)
        forward_values(2 * m + 2, z_b)
        forward_sums(2 * m + 1, z_a)
        return carry

    z_b[...] = jnp.zeros((TILE, H), F32)
    lax.fori_loop(0, rounds, forward, 0)
    forward_sums(2 * rounds, z_b)

    for item in small_copies[6:]:
        item.wait()
    w2nt = w2n_ref[...].T
    w1nt = w1n_ref[...].T

    def nodes(k, carry):
        rows = pl.ds(pl.multiple_of(k * NODE_CHUNK, NODE_CHUNK), NODE_CHUNK)
        packed = gathered[rows, :]
        count = jnp.sum(degree[rows, :], axis=1, keepdims=True)
        aggregate = (
            packed[:, :H]
            + dot(packed[:, H:].astype(BF16), w2e_ref[...])
            + count * b2e_ref[...]
        ).astype(BF16)
        x_node = jnp.concatenate([node_ref[rows, :], aggregate], axis=1)
        z_node = dot(x_node, w1n_ref[...]) + b1n_ref[...]
        u_node, sp_node = slope_and_value(z_node)
        cot_cells = cot_node_ref[rows, :]
        dz_node = (dot(cot_cells, w2nt) * sp_node).astype(BF16)
        dx_node = dot(dz_node, w1nt)
        base_ref[rows, :] = cot_cells.astype(F32) + dx_node[:, :H]
        gathered[rows, 0:H] = dx_node[:, H:]
        raw_ref[384:512, :] += dot_tn(packed[:, H:].astype(BF16), dx_node[:, H:].astype(BF16))
        raw_ref[897:898, :] += jnp.sum(count * dx_node[:, H:], axis=0, keepdims=True)
        raw_ref[512:768, :] += dot_tn(x_node, dz_node)
        raw_ref[768:896, :] += dot_tn(u_node.astype(BF16), cot_cells)
        raw_ref[898:899, :] += jnp.sum(dz_node.astype(F32), axis=0, keepdims=True)
        raw_ref[899:900, :] += jnp.sum(cot_cells.astype(F32), axis=0, keepdims=True)
        return carry

    lax.fori_loop(0, CELLS // NODE_CHUNK, nodes, 0)
    copies[1].wait()

    def backward_sums(j, d_buffer):
        start, span, i = tile_at(j)
        dz_edge = d_buffer[...]
        codes = row_codes(start)
        keys = (codes >> 3) - 128 * i + ((codes >> 2) & 1) * 128
        keys = jnp.where((codes >> 10) == i, keys, -1)
        spread = jnp.concatenate(one_hot_turned(keys, 2 * ROWS), axis=1).astype(BF16)
        kind = kind_col[span, :]
        first, second = (number.astype(BF16) for number in kinds(i, 2))
        parted = jnp.concatenate(
            [
                jnp.where(kind == first, dz_edge, zero),
                jnp.where(kind == second, dz_edge, zero),
                dz_edge,
            ],
            axis=1,
        )
        sums[i + 1] += dot(spread, parted)

    def backward_values(j, d_buffer):
        start, span, i = tile_at(j)
        keys = key_col[span, :]
        hot = jnp.where((keys == lane_low) | (keys == lane_high), one, zero)
        added = pair_dot(hot, block_diagonal(gathered[plane_rows(i), 0:H].astype(BF16)))
        d_wide = cot[span, :].astype(F32) + added
        d_edge = d_wide.astype(BF16)
        inside = head_inside(start, i)
        dz_edge = (pair_dot(d_edge, diag_w2t[...]) * slope[span, :].astype(F32)).astype(BF16)
        d_buffer[...] = dz_edge
        keep_rows(dz_all, start, dz_edge, inside)
        new = d_wide + pair_dot(dz_edge, diag_w1t[...])
        grad[span, :] = keep_head(grad, start, new, inside).astype(BF16)

    def piece(c):
        rows = pl.ds(pl.multiple_of(c * PIECE, PIECE), PIECE)
        return pltpu.make_async_copy(grad.at[rows, :], grad_edge_hbm.at[rows, :], sems.at[2])

    def send_pieces(done, final):
        upto = final // PIECE

        def send(c, carry):
            piece(c).start()
            return carry

        lax.fori_loop(done, upto, send, 0)
        return jnp.maximum(done, upto)

    def backward(m, carry):
        backward_values(2 * m + 1, d_a)
        backward_sums(2 * m, d_b)
        backward_values(2 * m + 2, d_b)
        backward_sums(2 * m + 1, d_a)
        return send_pieces(carry, starts[2 * m + 3])

    d_b[...] = jnp.zeros((TILE, H), BF16)
    sent = lax.fori_loop(0, rounds, backward, 0)
    send_pieces(sent, EDGES)
    backward_sums(2 * rounds, d_b)
    whole = pltpu.make_async_copy(grad.at[pl.ds(0, EDGES), :], grad_edge_hbm, sems.at[2])
    whole.wait()


def local_terms(bounds, faces, columns, edge_rows, cot_rows, small):
    vmem = pl.BlockSpec(memory_space=pltpu.VMEM)
    hbm = pl.BlockSpec(memory_space=pltpu.MemorySpace.HBM)
    return pl.pallas_call(
        local_kernel,
        out_shape=(
            jax.ShapeDtypeStruct((EDGES, H), BF16),
            pltpu.VMEM((CELLS, H), F32),
            pltpu.VMEM((RAW_ROWS, H), F32),
            pltpu.VMEM((PLANES + 2, 256, 3 * H), F32),
        )
        + (pltpu.VMEM((PADDED, H), BF16),) * 4,
        in_specs=[pl.BlockSpec(memory_space=pltpu.SMEM)] + [vmem] * 3 + [hbm] * 13,
        out_specs=(hbm,) + (vmem,) * 7,
        scratch_shapes=[pltpu.VMEM((PADDED, H), BF16)] * 2
        + [
            pltpu.VMEM((112, 128), jnp.int32),
            pltpu.VMEM((CELLS + 2 * ROWS, H), F32),
            pltpu.VMEM((CELLS, H), F32),
            pltpu.VMEM((FACES, H), F32),
            pltpu.VMEM((2 * ROWS, H), F32),
            pltpu.VMEM((CELLS, 2 * H), F32),
            pltpu.VMEM((CELLS, H), F32),
            pltpu.VMEM((PLANES, 256, 3 * H), BF16),
            pltpu.VMEM((256, 256), BF16),
            pltpu.VMEM((256, 256), BF16),
            pltpu.VMEM((256, 256), BF16),
            pltpu.VMEM((TILE, H), F32),
            pltpu.VMEM((TILE, H), F32),
            pltpu.VMEM((TILE, H), BF16),
            pltpu.VMEM((TILE, H), BF16),
            pltpu.SMEM((48,), jnp.int32),
            pltpu.SMEM((48,), jnp.int32),
            pltpu.SemaphoreType.DMA((3,)),
            pltpu.SemaphoreType.DMA((11,)),
        ]
        + [pltpu.VMEM(item.shape, item.dtype) for item in small],
        compiler_params=pltpu.CompilerParams(vmem_limit_bytes=LOCAL_VMEM),
        cost_estimate=pl.CostEstimate(
            flops=10_000_000_000, bytes_accessed=20_000_000, transcendentals=2_000_000
        ),
    )(bounds, faces, *columns, edge_rows, cot_rows, *small)


def place():
    return tuple(lax.axis_index(name) for name in ("gx", "gy", "gz"))


def sizes():
    return tuple(lax.axis_size(name) for name in ("gx", "gy", "gz"))


def across(side):
    dim, up = side // 2, side % 2
    here, count = place(), sizes()
    beyond = list(here)
    beyond[dim] = lax.rem(here[dim] + (1 if up else count[dim] - 1), count[dim])
    return tuple(beyond)


def face_copies(source, target, send_sems, recv_sems):
    copies = []
    for side, (first, rows) in enumerate(SPANS):
        opposite = SPANS[side ^ 1][0]
        copies.append(
            pltpu.make_async_remote_copy(
                src_ref=source.at[pl.ds(first, rows), :],
                dst_ref=target.at[pl.ds(opposite, rows), :],
                send_sem=send_sems.at[side],
                recv_sem=recv_sems.at[side],
                device_id=across(side),
                device_id_type=MESH,
            )
        )
    return copies


def halo_kernel(
    node_hbm,
    send_hbm,
    recv_hbm,
    face_ref,
    bounds_ref,
    key_col,
    kind_col,
    node_ref,
    send_ref,
    recv_ref,
    cells,
    packed,
    load_sems,
    send_sems,
    recv_sems,
):
    loads = [
        pltpu.make_async_copy(source, target, load_sems.at[k])
        for k, (source, target) in enumerate(
            ((node_hbm, node_ref), (send_hbm, send_ref), (recv_hbm, recv_ref))
        )
    ]
    for item in loads:
        item.start()
    barrier = pltpu.get_barrier_semaphore()
    for side in range(6):
        pl.semaphore_signal(barrier, inc=1, device_id=across(side), device_id_type=MESH)
    for item in loads:
        item.wait()
    cells[...] = node_ref[...].astype(F32)
    packed[X_LOW : X_LOW + ROWS, :] = node_ref[0:ROWS, :]
    packed[X_HIGH : X_HIGH + ROWS, :] = node_ref[CELLS - ROWS :, :]
    for first, at in ((Y_LOW, 0), (Y_HIGH, 124)):
        strips = [cells[ROWS * i + at : ROWS * i + at + 4, :] for i in range(PLANES)]
        packed[first : first + 64, :] = jnp.concatenate(strips, axis=0).astype(BF16)
    packed[Z_LOW : Z_LOW + 512, :] = cells[pl.ds(0, 512, stride=4), :].astype(BF16)
    packed[Z_HIGH : Z_HIGH + 512, :] = cells[pl.ds(3, 512, stride=4), :].astype(BF16)
    pl.semaphore_wait(barrier, 6)
    copies = face_copies(packed, face_ref, send_sems, recv_sems)
    for side in (5, 4, 1, 0, 3, 2):
        copies[side].start()
    recv = recv_ref[...]
    for i in range(PLANES + 1):
        below = jnp.where(recv < ROWS * i, 1.0, 0.0)
        bounds_ref[i] = jnp.sum(below).astype(jnp.int32)
    step, axis = steps_of(send_ref[...], recv)
    columns = (key_col, kind_col)
    zero = jnp.zeros((32, 128), F32)
    turned = jnp.concatenate(
        [
            jnp.concatenate([numbers.astype(F32), zero], axis=0).T
            for numbers in ((recv & 127) + jnp.where(step < 0, 128, 0), (recv >> 7) * 4 + axis)
        ],
        axis=0,
    ).astype(BF16)
    row = lax.broadcasted_iota(jnp.int32, (128, 256), 0)
    lane = lax.broadcasted_iota(jnp.int32, (128, 256), 1)
    for k in range(0, 96, 2):
        pick = jnp.where(row - (lane >> 7) == k, 1.0, 0.0).astype(BF16)
        both = dot(turned, pick).astype(BF16)
        for c, column in enumerate(columns):
            block = both[128 * c : 128 * c + 128]
            column[k * 128 : (k + 1) * 128, :] = block[:, :128]
            column[(k + 1) * 128 : (k + 2) * 128, :] = block[:, 128:]
    for column in columns:
        column[EDGES:, :] = jnp.full((TILE, 128), -4.0, BF16)
    for item in copies:
        item.wait()


def halo(node, send, recv):
    vmem = pl.BlockSpec(memory_space=pltpu.VMEM)
    return pl.pallas_call(
        halo_kernel,
        out_shape=(
            pltpu.VMEM((FACES, H), BF16),
            jax.ShapeDtypeStruct((PLANES + 1,), jnp.int32),
        )
        + (pltpu.VMEM((PADDED, 128), BF16),) * 2,
        in_specs=[pl.BlockSpec(memory_space=pltpu.MemorySpace.HBM)] * 3,
        out_specs=(vmem, pl.BlockSpec(memory_space=pltpu.SMEM)) + (vmem,) * 2,
        scratch_shapes=[
            pltpu.VMEM((CELLS, H), BF16),
            pltpu.VMEM((96, 128), jnp.int32),
            pltpu.VMEM((96, 128), jnp.int32),
            pltpu.VMEM((CELLS, H), F32),
            pltpu.VMEM((FACES, H), BF16),
            pltpu.SemaphoreType.DMA((3,)),
            pltpu.SemaphoreType.DMA((6,)),
            pltpu.SemaphoreType.DMA((6,)),
        ],
        compiler_params=pltpu.CompilerParams(
            collective_id=0, has_side_effects=True, vmem_limit_bytes=12 * 1024 * 1024
        ),
    )(node, send, recv)


def finish_kernel(
    base_ref,
    raw_in,
    sums,
    face_ref,
    edge,
    value,
    dz_all,
    cot,
    node_hbm,
    w1e_hbm,
    grad_ref,
    total_ref,
    node_ref,
    w1e_ref,
    raw_ref,
    edge_raw,
    dense_raw,
    leaving,
    moved,
    wide,
    out_ref,
    faces,
    cells,
    partner_part,
    half,
    parts,
    mine,
    full,
    send_sems,
    recv_sems,
    pair_send,
    pair_recv,
    all_send,
    all_recv,
    load_sems,
):
    (ga, gb, gc), (na, nb, nc) = place(), sizes()
    nz = nc // 2
    chips = na * nb * nz
    chip_z, core = lax.div(gc, 2), lax.rem(gc, 2)
    chip = (ga * nb + gb) * nz + chip_z
    partner = (ga, gb, 2 * chip_z + 1 - core)

    spots = (
        [lax.rem(ga + d, na) for d in range(na)],
        [lax.rem(gb + d, nb) for d in range(nb)],
        [lax.rem(chip_z + d, nz) for d in range(nz)],
    )
    rows_a = [spot * (nb * nz) for spot in spots[0]]
    rows_b = [spot * nz for spot in spots[1]]
    cores = [2 * spot + core for spot in spots[2]]

    def hops(d):
        da, db, dz = d
        return min(da, na - da) + min(db, nb - db) // 2 + db % 2 + 2 * dz

    offsets = sorted(
        ((da, db, dz) for da in range(na) for db in range(nb) for dz in range(nz)),
        key=lambda d: (-hops(d), d),
    )[:-1]

    def peer(d):
        da, db, dz = d
        where = (spots[0][da], spots[1][db], cores[dz])
        return where, rows_a[da] + rows_b[db] + spots[2][dz]

    barrier = pltpu.get_barrier_semaphore()
    for d in offsets:
        pl.semaphore_signal(barrier, inc=1, device_id=peer(d)[0], device_id_type=MESH)
    pl.semaphore_signal(barrier, inc=1, device_id=partner, device_id_type=MESH)
    for side in (4, 5):
        pl.semaphore_signal(barrier, inc=1, device_id=across(side), device_id_type=MESH)

    loads = [
        pltpu.make_async_copy(node_hbm, node_ref, load_sems.at[0]),
        pltpu.make_async_copy(w1e_hbm, w1e_ref, load_sems.at[1]),
    ]
    for item in loads:
        item.start()
    raw_ref[...] = raw_in[...]
    edge_raw[...] = jnp.zeros_like(edge_raw)
    for item in loads:
        item.wait()

    w1bt = w1e_ref[H : 2 * H, :].T
    w1bct = jnp.concatenate([w1bt, w1e_ref[2 * H :, :].T], axis=0)
    row_id = lax.broadcasted_iota(jnp.int32, (ROWS, H), 0)
    low_z = lax.rem(row_id, 4) == 0
    high_z = lax.rem(row_id, 4) == 3
    low_y = row_id < 4
    high_y = row_id >= 124

    def collect(i, carry):
        rows = pl.ds(pl.multiple_of(i * ROWS, ROWS), ROWS)
        here = sums[i + 1]
        third = here[:, 2 * H :] - here[:, :H] - here[:, H : 2 * H]
        arrived = here[:ROWS, 2 * H :] + here[ROWS:, 2 * H :]
        yp, ym = here[:ROWS, H : 2 * H], here[ROWS:, H : 2 * H]
        zp, zm = third[:ROWS], third[ROWS:]
        left = (
            sums[i, 0:ROWS, 0:H]
            + sums[i + 2, ROWS : 2 * ROWS, 0:H]
            + jnp.where(low_y, 0.0, pltpu.roll(yp, 4, 0))
            + jnp.where(high_y, 0.0, pltpu.roll(ym, 124, 0))
            + jnp.where(low_z, 0.0, pltpu.roll(zp, 1, 0))
            + jnp.where(high_z, 0.0, pltpu.roll(zm, 127, 0))
        )
        both_ways = jnp.concatenate([left, arrived], axis=1).astype(BF16)
        moved[rows, :] = both_ways
        leaving[pl.ds(Y_LOW + 4 * i, 4), :] = ym[:4]
        leaving[pl.ds(Y_HIGH + 4 * i, 4), :] = yp[124:]
        wide[0:ROWS, :] = zm
        wide[ROWS:, :] = zp
        leaving[pl.ds(Z_LOW + 32 * i, 32), :] = wide[pl.ds(0, 32, stride=4), :]
        leaving[pl.ds(Z_HIGH + 32 * i, 32), :] = wide[pl.ds(ROWS + 3, 32, stride=4), :]
        both = dot_tn(node_ref[rows, :], both_ways)
        edge_raw[0:H, :] += both[:, :H]
        edge_raw[H : 2 * H, :] += both[:, H:]
        edge_raw[2 * H : 2 * H + 1, :] += jnp.sum(arrived, axis=0, keepdims=True)
        return carry

    def collect_four(k, carry):
        for step in range(4):
            carry = collect(4 * k + step, carry)
        return carry

    lax.fori_loop(0, PLANES // 4, collect_four, 0)
    leaving[X_LOW : X_LOW + ROWS, :] = sums[1, ROWS : 2 * ROWS, 0:H]
    leaving[X_HIGH : X_HIGH + ROWS, :] = sums[PLANES, 0:ROWS, 0:H]
    edge_raw[0:H, :] += dot_tn(face_ref[...], leaving[...].astype(BF16))
    block = raw_ref.shape[1]
    raw_ref[H // block : 3 * H // block] = edge_raw[0 : 2 * H, :].reshape(2 * H // block, block, H)
    raw_ref[896 // block, 896 % block : 896 % block + 1, :] = edge_raw[2 * H : 2 * H + 1, :]

    dense_raw[...] = jnp.zeros_like(dense_raw)
    ones = jnp.ones((16, DENSE), BF16)

    def dense(k, carry):
        rows = pl.ds(pl.multiple_of(k * DENSE, DENSE), DENSE)
        dense_raw[...] += dot(
            jnp.concatenate([edge[rows, :].T, value[rows, :].T, ones], axis=0),
            jnp.concatenate([dz_all[rows, :], cot[rows, :]], axis=1),
        )
        return carry

    lax.fori_loop(0, EDGES // DENSE, dense, 0)
    per = H // block
    raw_ref[0:per] = dense_raw[0:H, :H].reshape(per, block, H)
    raw_ref[3 * per : 4 * per] += dense_raw[H : 2 * H, H:].reshape(per, block, H)
    raw_ref[897 // block, 897 % block : 897 % block + 1, :] += dense_raw[2 * H : 2 * H + 1, H:]
    pl.semaphore_wait(barrier, chips + 2)

    def to_partner(source, target, k):
        return pltpu.make_async_remote_copy(
            src_ref=source,
            dst_ref=target,
            send_sem=pair_send.at[k],
            recv_sem=pair_recv.at[k],
            device_id=partner,
            device_id_type=MESH,
        )

    first = to_partner(raw_ref.at[pl.ds((1 - core) * chips, chips)], partner_part, 0)
    first.start()
    first.wait()
    half[...] = raw_ref[pl.ds(core * chips, chips)] + partner_part[...]

    for d in offsets:
        where, other = peer(d)
        pltpu.make_async_remote_copy(
            src_ref=half.at[other],
            dst_ref=parts.at[chip],
            send_sem=all_send.at[0],
            recv_sem=all_recv.at[0],
            device_id=where,
            device_id_type=MESH,
        ).start()
    parts[chip] = half[chip]

    out_ref[...] = dot(leaving[...].astype(BF16), w1bt).astype(BF16)
    halos = face_copies(out_ref, faces, send_sems, recv_sems)
    for side in (0, 1, 2, 3):
        halos[side].start()

    def combine(k, carry):
        rows = pl.ds(pl.multiple_of(k * CHUNK, CHUNK), CHUNK)
        cells[rows, :] = base_ref[rows, :] + dot(moved[rows, :], w1bct)
        return carry

    lax.fori_loop(0, CELLS // CHUNK, combine, 0)

    def settle(buffer, sem):
        span = buffer.at[pl.ds(0, chips - 1)]
        pltpu.make_async_copy(span, span, sem).wait()

    settle(parts, all_recv.at[0])
    mine[...] = jnp.sum(parts[...], axis=0)

    slot = core * chips + chip
    for d in offsets:
        pltpu.make_async_remote_copy(
            src_ref=mine,
            dst_ref=full.at[slot],
            send_sem=all_send.at[1],
            recv_sem=all_recv.at[1],
            device_id=peer(d)[0],
            device_id_type=MESH,
        ).start()
    for side in (4, 5):
        halos[side].start()
    full[slot] = mine[...]
    settle(full, all_recv.at[1])
    held = pl.ds(core * chips, chips)
    last = to_partner(full.at[held], full.at[held], 1)
    last.start()
    for item in halos:
        item.wait()
    cells[0:ROWS, :] += faces[X_LOW : X_LOW + ROWS, :].astype(F32)
    cells[CELLS - ROWS :, :] += faces[X_HIGH : X_HIGH + ROWS, :].astype(F32)
    for start, at in ((Y_LOW, 0), (Y_HIGH, 124)):
        strip = faces[start : start + 64, :].astype(F32)
        for i in range(PLANES):
            cells[ROWS * i + at : ROWS * i + at + 4, :] += strip[4 * i : 4 * i + 4]
    cells[pl.ds(0, 512, stride=4), :] += faces[Z_LOW : Z_LOW + 512, :].astype(F32)
    cells[pl.ds(3, 512, stride=4), :] += faces[Z_HIGH : Z_HIGH + 512, :].astype(F32)
    grad_ref[...] = cells[...].astype(BF16)
    settle(half, all_send.at[0])
    settle(half, all_send.at[1])
    last.wait()
    total_ref[...] = full[...]


def write_kernel(grad_ref, total_ref, *refs):
    outs, scaled, sems = refs[:6], refs[6], refs[7]
    first = pltpu.make_async_copy(grad_ref, outs[0], sems.at[0])
    first.start()
    total = total_ref[...]
    squares = jnp.sum(total * total, axis=0, keepdims=True)
    squares = jnp.sum(squares, axis=1, keepdims=True)
    factor = 1.0 / jnp.maximum(1.0, jnp.sqrt(squares / (7 * H * H + 4 * H)))
    scaled[...] = total * factor
    copies = [first]
    at = 0
    for k, rows in enumerate((384, 128, 256, 128, 4)):
        copies.append(
            pltpu.make_async_copy(scaled.at[pl.ds(at, rows), :], outs[k + 1], sems.at[k + 1])
        )
        copies[-1].start()
        at += rows
    for item in copies:
        item.wait()


def write(grad, total):
    vmem = pl.BlockSpec(memory_space=pltpu.VMEM)
    return pl.pallas_call(
        write_kernel,
        out_shape=(jax.ShapeDtypeStruct((CELLS, H), BF16),)
        + tuple(jax.ShapeDtypeStruct((rows, H), F32) for rows in (384, 128, 256, 128, 4)),
        in_specs=[vmem] * 2,
        out_specs=(pl.BlockSpec(memory_space=pl.ANY),) * 6,
        scratch_shapes=[pltpu.VMEM((RAW_ROWS, H), F32), pltpu.SemaphoreType.DMA((6,))],
        compiler_params=pltpu.CompilerParams(vmem_limit_bytes=48 * 1024 * 1024),
    )(grad, total)


def finish(base, raw, sums, faces, slots, node, w1_edge):
    chips = lax.axis_size("gx") * lax.axis_size("gy") * lax.axis_size("gz") // 2
    block = RAW_ROWS // (2 * chips)
    vmem = pl.BlockSpec(memory_space=pltpu.VMEM)
    grad, total = pl.pallas_call(
        finish_kernel,
        out_shape=(
            jax.ShapeDtypeStruct((CELLS, H), BF16),
            jax.ShapeDtypeStruct((2 * chips, block, H), F32),
        ),
        in_specs=[vmem] * 8 + [pl.BlockSpec(memory_space=pltpu.MemorySpace.HBM)] * 2,
        out_specs=(vmem,) * 2,
        scratch_shapes=[
            pltpu.VMEM((CELLS, H), BF16),
            pltpu.VMEM((3 * H, H), BF16),
            pltpu.VMEM((2 * chips, block, H), F32),
            pltpu.VMEM((2 * H + 8, H), F32),
            pltpu.VMEM((2 * H + 16, 2 * H), F32),
            pltpu.VMEM((FACES, H), F32),
            pltpu.VMEM((CELLS, 2 * H), BF16),
            pltpu.VMEM((2 * ROWS, H), F32),
            pltpu.VMEM((FACES, H), BF16),
            pltpu.VMEM((FACES, H), BF16),
            pltpu.VMEM((CELLS, H), F32),
            pltpu.VMEM((chips, block, H), F32),
            pltpu.VMEM((chips, block, H), F32),
            pltpu.VMEM((chips, block, H), F32),
            pltpu.VMEM((block, H), F32),
            pltpu.VMEM((2 * chips, block, H), F32),
            pltpu.SemaphoreType.DMA((6,)),
            pltpu.SemaphoreType.DMA((6,)),
            pltpu.SemaphoreType.DMA((2,)),
            pltpu.SemaphoreType.DMA((2,)),
            pltpu.SemaphoreType.DMA((2,)),
            pltpu.SemaphoreType.DMA((2,)),
            pltpu.SemaphoreType.DMA((2,)),
        ],
        compiler_params=pltpu.CompilerParams(
            collective_id=1, has_side_effects=True, vmem_limit_bytes=24 * 1024 * 1024
        ),
    )(base, raw.reshape(2 * chips, block, H), sums, faces, *slots, node, w1_edge)
    return write(grad, total.reshape(RAW_ROWS, H))


def on_device(
    node_latent,
    edge_latent,
    senders,
    receivers,
    w1_edge,
    b1_edge,
    w2_edge,
    b2_edge,
    w1_node,
    b1_node,
    w2_node,
    cot_node,
    cot_edge,
):
    keep = functools.partial(
        pltpu.with_memory_space_constraint, memory_space=pltpu.MemorySpace.HBM
    )
    cells = keep(node_latent.reshape(CELLS, H))
    sender_ids = keep(senders.reshape(96, 128))
    receiver_ids = keep(receivers.reshape(96, 128))
    w1_edge = keep(w1_edge)
    faces, bounds, *columns = halo(cells, sender_ids, receiver_ids)
    grad_edge, base, raw, sums, *slots = local_terms(
        bounds,
        faces,
        columns,
        keep(edge_latent.reshape(EDGES, H)),
        keep(cot_edge.reshape(EDGES, H)),
        (
            receiver_ids,
            sender_ids,
            w1_edge,
            keep(b1_edge.reshape(1, H)),
            keep(w2_edge),
            cells,
            keep(cot_node.reshape(CELLS, H)),
            keep(b2_edge.reshape(1, H)),
            keep(w1_node),
            keep(b1_node.reshape(1, H)),
            keep(w2_node),
        ),
    )
    grad_node, *grads = finish(base, raw, sums, faces, slots, cells, w1_edge)
    return (grad_node.reshape(node_latent.shape), grad_edge.reshape(edge_latent.shape), *grads)


def solution(mesh):
    cell = P("gx", "gy", "gz", None)
    slots = P("gx", "gy", "gz", None, None)
    placed = (cell, slots, cell, cell, P(), P(), P(), P(), P(), P(), P(), cell, slots)
    return jax.shard_map(
        on_device,
        mesh=mesh,
        in_specs=placed,
        out_specs=(cell, slots, P(), P(), P(), P(), P()),
        check_vma=False,
    )
```
